32 devices in a mesh: fsdp: 8 (over y, x, core), tp: 4 (over z).
Axes of the slice: x: 2, y: 2, z: 4, core: 2. Of those that a mesh axis runs over, the one named last changes fastest.
Arguments:
- tokens: bfloat16 [8, 1024, 1024], P('fsdp', 'tp'), may hold values from -6 to 6
- lengths: int32 [8], P('fsdp'), may hold values from 256 to 1024, as said below
- norm_gain: bfloat16 [1024], P('fsdp'), may hold values from 0.5 to 1.5
- in_weight: bfloat16 [1024, 2, 2048], P('fsdp', None, 'tp'), may hold values from -0.1875 to 0.1875
- conv_weight: bfloat16 [4, 2048], P(None, ('tp', 'fsdp')), may hold values from -3 to 3
- conv_bias: bfloat16 [2048], P(('tp', 'fsdp')), may hold values from -3 to 3
- x_weight: bfloat16 [2048, 96], P(('tp', 'fsdp')), may hold values from -0.125 to 0.125
- dt_weight: bfloat16 [64, 2048], P('fsdp', 'tp'), may hold values from -0.75 to 0.75
- dt_bias: bfloat16 [2048], P(('tp', 'fsdp')), may hold values from -6.5 to -2.5
- a_log: bfloat16 [16, 2048], P(None, ('tp', 'fsdp')), may hold values from 0 to 2.796875
- d_skip: bfloat16 [2048], P(('tp', 'fsdp')), may hold values from 0.5 to 1.5
- out_weight: bfloat16 [2048, 1024], P('tp', 'fsdp'), may hold values from -0.25 to 0.25
- cotangent: bfloat16 [8, 1024, 1024], P('fsdp', 'tp'), may hold values from -6 to 6
Outputs:
- block_out: bfloat16 [8, 1024, 1024], P('fsdp', 'tp')
- input_grad: float32 [8, 1024, 1024], P('fsdp', 'tp')
- gain_grad: float32 [1024], P('fsdp')
- in_weight_grad: float32 [1024, 2, 2048], P('fsdp', None, 'tp')
- conv_weight_grad: float32 [4, 2048], P(None, ('tp', 'fsdp'))
- conv_bias_grad: float32 [2048], P(('tp', 'fsdp'))
- x_weight_grad: float32 [2048, 96], P(('tp', 'fsdp'))
- dt_weight_grad: float32 [64, 2048], P('fsdp', 'tp')
- dt_bias_grad: float32 [2048], P(('tp', 'fsdp'))
- a_log_grad: float32 [16, 2048], P(None, ('tp', 'fsdp'))
- d_skip_grad: float32 [2048], P(('tp', 'fsdp'))
- out_weight_grad: float32 [2048, 1024], P('tp', 'fsdp')
The draws below stay inside these ranges and needn't reach their ends.
Inputs may be any that keep to these rules, and one draw needn't show every extreme that they name: lengths[s] is the number of live positions of slot s, counted from its start; at least one slot is full.
All inputs are finite; a program needn't handle non-finite values.
Results may differ from the reference program's by a relative error of at most 0.011.
Values may be sent and summed in bfloat16 or wider, within the bound.
No kernel may reach another device: no remote copies, remote signals or barrier semaphores. Data moves between devices by JAX's collectives and lax.ppermute only.
A program may use at most 192 MiB of HBM per device.

```python
from functools import partial
import jax
import jax.numpy as jnp
from jax import lax

D = 1024
DI = 2048
NS = 16
R = 64
KC = 4
LEN = 1024
SEQ_GRP = 1
BLOCK = 64
NSEQ = 8


def draw_lengths(key, part):
    first, second = jax.random.split(jax.random.fold_in(key, 17))
    drawn = jax.random.randint(first, (NSEQ,), LEN // 4, LEN + 1)
    chosen = jax.random.randint(second, (), 0, NSEQ)
    return jnp.where(jnp.arange(NSEQ) == chosen, LEN, drawn).astype(jnp.int32)


def block_scale(stream_key, dims, cuts, least, top_value):
    gain, own = 1.0, jax.random.fold_in(stream_key, 6)
    for position, blocks in cuts:
        steps = jnp.exp(jax.random.uniform(jax.random.fold_in(own, position), (blocks,), jnp.float32, least / len(cuts), top_value / len(cuts)))
        gain = gain * jnp.repeat(steps, dims[position] // blocks).reshape([-1 if axis == position else 1 for axis in range(len(dims))])
    return gain


def scatter_about(own_key, dims, width, reach, cuts=(), kind=jnp.bfloat16):
    array = width * jax.random.normal(own_key, dims, jnp.float32)
    if cuts:
        array = array * block_scale(own_key, dims, cuts, -0.22, 0.18)
    return jnp.clip(array, -reach, reach).astype(kind)


def setup_inputs(seed: int = 0) -> dict:
    arg_keys = jax.random.split(jax.random.key(seed), 14)
    tokens = scatter_about(arg_keys[0], (NSEQ, LEN, D), 1.0, 6.0, ((0, 8), (1, 4)))
    lengths = draw_lengths(jax.random.fold_in(arg_keys[13], 71), 0)
    norm_gain = jnp.clip(1.0 + 0.1 * jax.random.normal(arg_keys[2], (D,), jnp.float32), 0.5, 1.5).astype(jnp.bfloat16)
    in_weight = scatter_about(arg_keys[3], (D, 2, DI), D ** -0.5, 0.1875, ((0, 8), (2, 4)))
    conv_weight = scatter_about(arg_keys[4], (KC, DI), KC ** -0.5, 3.0, ((1, 32),))
    conv_bias = scatter_about(arg_keys[5], (DI,), 0.5, 3.0, ((0, 32),))
    x_weight = scatter_about(arg_keys[6], (DI, R + 2 * NS), DI ** -0.5, 0.125, ((0, 32),))
    dt_weight = scatter_about(arg_keys[7], (R, DI), R ** -0.5, 0.75, ((0, 8), (1, 4)))
    dt_bias = jnp.clip(-6.5 + 4.0 * jax.random.uniform(arg_keys[8], (DI,), jnp.float32) ** block_scale(arg_keys[8], (DI,), ((0, 32),), -0.2, 0.2), -6.5, -2.5).astype(jnp.bfloat16)
    a_log = jnp.clip(2.796875 * jax.random.uniform(arg_keys[9], (NS, DI), jnp.float32) ** block_scale(arg_keys[9], (NS, DI), ((1, 32),), -0.2, 0.2), 0.0, 2.796875).astype(jnp.bfloat16)
    d_skip = jnp.clip(0.5 + 1.0 * jax.random.uniform(arg_keys[10], (DI,), jnp.float32) ** block_scale(arg_keys[10], (DI,), ((0, 32),), -0.2, 0.2), 0.5, 1.5).astype(jnp.bfloat16)
    out_weight = scatter_about(arg_keys[11], (DI, D), (DI // 4) ** -0.5, 0.25, ((0, 4), (1, 8)))
    cotangent = scatter_about(arg_keys[12], (NSEQ, LEN, D), 1.0, 6.0, ((0, 8), (1, 4)))
    return dict(tokens=tokens, lengths=lengths, norm_gain=norm_gain, in_weight=in_weight, conv_weight=conv_weight, conv_bias=conv_bias, x_weight=x_weight, dt_weight=dt_weight, dt_bias=dt_bias, a_log=a_log, d_skip=d_skip, out_weight=out_weight, cotangent=cotangent)


@jax.custom_vjp
def low(v):
    return lax.optimization_barrier(v.astype(jnp.bfloat16)).astype(jnp.float32)

@jax.custom_vjp
def low_back(v):
    return v

def low_keep(v):
    return (low(v), None)

def low_pass(kept, grad):
    return (grad,)

def back_keep(v):
    return (v, None)

def back_low(kept, grad):
    return (low(grad),)
low.defvjp(low_keep, low_pass)
low_back.defvjp(back_keep, back_low)
epsilon = 1e-05
highest = lax.Precision.HIGHEST

def combine(earlier, later):
    return (earlier[0] * later[0], later[0] * earlier[1] + later[1])

def to_blocks(values, count):
    shaped = values.reshape((values.shape[0], count, values.shape[1] // count) + values.shape[2:])
    return jnp.moveaxis(shaped, (1, 2), (0, 1))

def from_blocks(values):
    merged = jnp.moveaxis(values, (0, 1), (1, 2))
    return merged.reshape((merged.shape[0], merged.shape[1] * merged.shape[2]) + merged.shape[3:])

def scan_block(decay_rate, carried, pieces):
    step_size, input_map, output_map, conv_out = pieces
    decay = jnp.exp(step_size[:, :, None, :] * decay_rate)
    drive = (step_size * conv_out)[:, :, None, :] * input_map[:, :, :, None]
    product, summed = lax.associative_scan(combine, (decay, drive), axis=0)
    states = product * carried[None] + summed
    return (states[-1], lax.optimization_barrier(jnp.sum(states * output_map[:, :, :, None], axis=2)))

def forward(lengths, values, norm_gain, in_weight, conv_weight, conv_bias, x_weight, dt_weight, dt_bias, a_log, d_skip, out_weight):
    seq_len = values.shape[1]
    live_mask = (jnp.arange(seq_len)[None, :] < lengths[:, None]).astype(jnp.float32)[:, :, None]
    inverse = lax.rsqrt(lax.optimization_barrier(jnp.mean(values * values, axis=-1, keepdims=True)) + epsilon)
    normed = low(values * inverse * norm_gain)
    projected = low_back(jnp.einsum('bld,dkc->blkc', normed, in_weight, precision=highest))
    conv_input = projected[:, :, 0]
    gate_input = projected[:, :, 1]
    padded = jnp.pad(conv_input, ((0, 0), (KC - 1, 0), (0, 0)))
    conv_sum = conv_bias + sum((conv_weight[offset] * padded[:, offset:offset + seq_len] for offset in range(KC)))
    conv_out = low(jax.nn.silu(conv_sum))
    mapped = low_back(jnp.einsum('blc,cj->blj', conv_out, x_weight, precision=highest))
    low_rank = low(mapped[:, :, :R])
    input_map = mapped[:, :, R:R + NS]
    output_map = mapped[:, :, R + NS:]
    step_pre = low_back(jnp.einsum('blr,rc->blc', low_rank, dt_weight, precision=highest) + dt_bias)
    step_size = jax.nn.softplus(step_pre) * live_mask
    decay_rate = -jnp.exp(a_log)
    count = seq_len // BLOCK
    pieces = (to_blocks(step_size, count), to_blocks(input_map, count), to_blocks(output_map, count), to_blocks(conv_out, count))
    start = jnp.zeros((values.shape[0], NS, DI), jnp.float32)
    final, scan_out = lax.scan(jax.checkpoint(partial(scan_block, decay_rate)), start, pieces)
    scan_out = from_blocks(scan_out)
    mixed = low((scan_out + d_skip * conv_out) * jax.nn.silu(gate_input) * live_mask)
    return values + jnp.einsum('blc,cd->bld', mixed, out_weight, precision=highest)

def reference(tokens, lengths, norm_gain, in_weight, conv_weight, conv_bias, x_weight, dt_weight, dt_bias, a_log, d_skip, out_weight, cotangent):
    weights = tuple((weight.astype(jnp.float32) for weight in (norm_gain, in_weight, conv_weight, conv_bias, x_weight, dt_weight, dt_bias, a_log, d_skip, out_weight)))
    groups = NSEQ // SEQ_GRP
    shaped = tokens.astype(jnp.float32).reshape(groups, SEQ_GRP, LEN, D)
    grads_in = cotangent.astype(jnp.float32).reshape(groups, SEQ_GRP, LEN, D)
    group_lengths = lengths.reshape(groups, SEQ_GRP)

    def one_group(totals, pieces):
        values, seq_lengths, seq_grad = pieces
        result, pullback = jax.vjp(partial(forward, seq_lengths), values, *weights)
        grads = pullback(seq_grad)
        return (tuple((total + grad for total, grad in zip(totals, grads[1:]))), (result.astype(jnp.bfloat16), grads[0]))
    initial = tuple((jnp.zeros_like(weight) for weight in weights))
    totals, (results, input_grads) = lax.scan(one_group, initial, (shaped, group_lengths, grads_in))
    return (results.reshape(NSEQ, LEN, D), input_grads.reshape(NSEQ, LEN, D), totals[0], totals[1], totals[2], totals[3], totals[4], totals[5], totals[6], totals[7], totals[8], totals[9])
```

```python
import functools

import jax
import jax.numpy as jnp
from jax import lax
from jax.experimental import pallas as pl
from jax.experimental.pallas import tpu as pltpu
from jax.sharding import PartitionSpec as P

bf16 = jnp.bfloat16
f32 = jnp.float32
LOG2E = 1.4426950408889634
LN2 = 0.6931471805599453


epsilon = 1e-05


def silu_grad(values):
    sigma = jax.nn.sigmoid(values)
    return sigma * (1.0 + values * (1.0 - sigma))


def split(v):
    hi=v.astype(bf16)
    return hi,(v-hi.astype(f32)).astype(bf16)

def spread(m, sub):
    tb,ns=m.shape
    wide=sub*ns
    rep=(lax.broadcasted_iota(jnp.int32,(ns,wide),1)%ns==lax.broadcasted_iota(jnp.int32,(ns,wide),0)).astype(bf16)
    keep=(lax.broadcasted_iota(jnp.int32,(tb,wide),1)//ns==lax.broadcasted_iota(jnp.int32,(tb,wide),0)%sub)
    out=[]
    for part in split(m):
        t=jnp.dot(part,rep,preferred_element_type=f32)
        out.append(jnp.where(keep,t,0.0).astype(bf16))
    return out

def outer(eh,el,vh,vl):
    e=jnp.concatenate([eh,eh,el],0); v=jnp.concatenate([vh,vl,vh],0)
    return lax.dot_general(e,v,(((0,),(0,)),((),())),preferred_element_type=f32)

def fwd_kernel(sub, dt_ref,x_ref,b_ref,c_ref,rate_ref,y_ref,h_ref, drive, state, eb_h, eb_l, xh, xl):
    tb,ch=dt_ref.shape; ns=rate_ref.shape[0]; half=ns//2
    @pl.when(pl.program_id(0)==0)
    def _(): state[...]=jnp.zeros_like(state)
    eb_h[...],eb_l[...]=spread(b_ref[...],sub)
    dtx=dt_ref[...]*x_ref[...].astype(f32)
    xh[...],xl[...]=split(dtx)
    for i in range(tb//sub):
        s=slice(i*sub,(i+1)*sub)
        drive[i*sub*ns:(i+1)*sub*ns,:]=outer(eb_h[s],eb_l[s],xh[s],xl[s])
    r0=rate_ref[:half]*LOG2E; r1=rate_ref[half:]*LOG2E
    U=16
    def body(j,hs):
        h0,h1=hs
        rows=dt_ref[pl.ds(pl.multiple_of(j*U,U),U),:]
        for k in range(U):
            dtb=jnp.broadcast_to(rows[k:k+1],(half,ch))
            a0=jnp.exp2(dtb*r0); a1=jnp.exp2(dtb*r1)
            base=pl.multiple_of(j*(U*ns),U*ns)+k*ns
            h0=a0*h0+drive[pl.ds(base,half),:]
            h1=a1*h1+drive[pl.ds(base+half,half),:]
            h_ref[pl.ds(base,ns),:]=jnp.concatenate([h0,h1],0).astype(bf16)
        return h0,h1
    h0,h1=lax.fori_loop(0,tb//U,body,(state[:half],state[half:]))
    state[:half]=h0; state[half:]=h1
    ch_,cl_=spread(c_ref[...],sub)
    for i in range(tb//sub):
        s=slice(i*sub,(i+1)*sub)
        e=jnp.concatenate([ch_[s],cl_[s]],0)
        o=jnp.dot(e,h_ref[i*sub*ns:(i+1)*sub*ns,:],preferred_element_type=f32)
        y_ref[s,:]=o[:sub]+o[sub:]

def scan_fwd(dt,x,b,c,rate,tb=128,sub=16):
    t,ch=dt.shape; ns=rate.shape[0]
    row=lambda w: pl.BlockSpec((tb,w),lambda i:(i,0))
    full=lambda a: pl.BlockSpec(a.shape,lambda i:(0,0))
    return pl.pallas_call(functools.partial(fwd_kernel,sub),
        grid=(t//tb,),
        in_specs=[row(ch),row(ch),row(ns),row(ns),full(rate)],
        out_specs=[row(ch),pl.BlockSpec((tb*ns,ch),lambda i:(i,0))],
        out_shape=[jax.ShapeDtypeStruct((t,ch),f32),jax.ShapeDtypeStruct((t*ns,ch),bf16)],
        scratch_shapes=[pltpu.VMEM((tb*ns,ch),f32),pltpu.VMEM((ns,ch),f32),pltpu.VMEM((tb,sub*ns),bf16),pltpu.VMEM((tb,sub*ns),bf16),pltpu.VMEM((tb,ch),bf16),pltpu.VMEM((tb,ch),bf16)],
        compiler_params=pltpu.CompilerParams(vmem_limit_bytes=56*2**20),
        name="scan_fwd")(dt,x,b,c,rate)

def bwd_kernel(sub, dt_ref,x_ref,b_ref,c_ref,dy_ref,h_ref,hp_ref,rate_ref,
               w_ref,q_ref,ib_ref,oc_ref,acc_ref, drive, carry, gs, vs):
    tb,ch=dt_ref.shape; ns=rate_ref.shape[0]; half=ns//2
    step=pl.program_id(0); nb=pl.num_programs(0)
    @pl.when(step==0)
    def _():
        carry[...]=jnp.zeros_like(carry); acc_ref[...]=jnp.zeros_like(acc_ref)
    ech,ecl=spread(c_ref[...],sub)
    dy=dy_ref[...]
    yh,yl=split(dy)
    for i in range(tb//sub):
        s=slice(i*sub,(i+1)*sub)
        drive[i*sub*ns:(i+1)*sub*ns,:]=outer(ech[s],ecl[s],yh[s],yl[s])
    r0=rate_ref[:half]*LOG2E; r1=rate_ref[half:]*LOG2E
    before=jnp.where(step==nb-1,jnp.zeros_like(hp_ref[...]),hp_ref[...])
    U=16
    def body(jj,cs):
        q0,q1,s0,s1=cs
        j=tb//U-1-jj
        rows=dt_ref[pl.ds(pl.multiple_of(j*U,U),U),:]
        for k in reversed(range(U)):
            dtb=jnp.broadcast_to(rows[k:k+1],(half,ch))
            a0=jnp.exp2(dtb*r0); a1=jnp.exp2(dtb*r1)
            base=pl.multiple_of(j*(U*ns),U*ns)+k*ns
            g0=drive[pl.ds(base,half),:]+q0
            g1=drive[pl.ds(base+half,half),:]+q1
            gs[pl.ds(base,ns),:]=jnp.concatenate([g0,g1],0).astype(bf16)
            q0=a0*g0; q1=a1*g1
            if k==0:
                prev=h_ref[pl.ds(pl.multiple_of(jnp.maximum(base-ns,0),ns),ns),:]
                prev=jnp.where(j==0,before,prev)
            else:
                prev=h_ref[pl.ds(base-ns,ns),:]
            prev=prev.astype(f32)
            m0=r0*(q0*prev[:half]); m1=r1*(q1*prev[half:])
            s0=s0+dtb*m0; s1=s1+dtb*m1
            vs[pl.ds(base,ns),:]=jnp.concatenate([m0,m1],0).astype(bf16)
        return q0,q1,s0,s1
    q0,q1,s0,s1=lax.fori_loop(0,tb//U,body,(carry[:half],carry[half:],acc_ref[:half],acc_ref[half:]))
    carry[:half]=q0; carry[half:]=q1; acc_ref[:half]=s0; acc_ref[half:]=s1
    ebh,ebl=spread(b_ref[...],sub)
    wide=sub*ns
    ones=(lax.broadcasted_iota(jnp.int32,(sub,wide),1)//ns==lax.broadcasted_iota(jnp.int32,(sub,wide),0))
    one_b=ones.astype(bf16)
    rep=(lax.broadcasted_iota(jnp.int32,(wide,ns),0)%ns==lax.broadcasted_iota(jnp.int32,(wide,ns),1)).astype(bf16)
    dxh=(dt_ref[...]*x_ref[...].astype(f32)).astype(bf16)
    nt=(((1,),(1,)),((),()))
    for i in range(tb//sub):
        s=slice(i*sub,(i+1)*sub); big=slice(i*sub*ns,(i+1)*sub*ns)
        g=gs[big,:]
        o=jnp.dot(jnp.concatenate([ebh[s],ebl[s]],0),g,preferred_element_type=f32)
        w_ref[s,:]=o[:sub]+o[sub:]
        q_ref[s,:]=jnp.dot(one_b,vs[big,:],preferred_element_type=f32)*LN2
        zb=lax.dot_general(dxh[s],g,nt,preferred_element_type=f32)
        zc=lax.dot_general(yh[s],h_ref[big,:],nt,preferred_element_type=f32)
        z=jnp.where(jnp.concatenate([ones,ones],0),jnp.concatenate([zb,zc],0),0.0).astype(bf16)
        z=jnp.dot(z,rep,preferred_element_type=f32)
        ib_ref[s,:]=z[:sub]; oc_ref[s,:]=z[sub:]

def scan_bwd(dt,x,b,c,dy,h,rate,tb=128,sub=16):
    t,ch=dt.shape; ns=rate.shape[0]; nb=t//tb
    row=lambda w: pl.BlockSpec((tb,w),lambda i:(nb-1-i,0))
    full=lambda a: pl.BlockSpec(a.shape,lambda i:(0,0))
    return pl.pallas_call(functools.partial(bwd_kernel,sub),
        grid=(nb,),
        in_specs=[row(ch),row(ch),row(ns),row(ns),row(ch),pl.BlockSpec((tb*ns,ch),lambda i:(nb-1-i,0)),
                  pl.BlockSpec((ns,ch),lambda i:(jnp.maximum((nb-1-i)*tb-1,0),0)),full(rate)],
        out_specs=[row(ch),row(ch),row(ns),row(ns),full(rate)],
        out_shape=[jax.ShapeDtypeStruct((t,ch),f32),jax.ShapeDtypeStruct((t,ch),f32),jax.ShapeDtypeStruct((t,ns),f32),jax.ShapeDtypeStruct((t,ns),f32),jax.ShapeDtypeStruct((ns,ch),f32)],
        scratch_shapes=[pltpu.VMEM((tb*ns,ch),f32),pltpu.VMEM((ns,ch),f32),pltpu.VMEM((tb*ns,ch),bf16),pltpu.VMEM((tb*ns,ch),bf16)],
        compiler_params=pltpu.CompilerParams(vmem_limit_bytes=56*2**20),
        name="scan_bwd")(dt,x,b,c,dy,h,h,rate)


def shards(
    tokens,
    lengths,
    norm_gain,
    in_weight,
    conv_weight,
    conv_bias,
    x_weight,
    dt_weight,
    dt_bias,
    a_log,
    d_skip,
    out_weight,
    cotangent,
):
    gathered = (
        lax.all_gather(norm_gain, "fsdp", axis=0, tiled=True),
        lax.all_gather(in_weight, "fsdp", axis=0, tiled=True),
        lax.all_gather(conv_weight, "fsdp", axis=1, tiled=True),
        lax.all_gather(conv_bias, "fsdp", axis=0, tiled=True),
        lax.all_gather(x_weight, "fsdp", axis=0, tiled=True),
        lax.all_gather(dt_weight, "fsdp", axis=0, tiled=True),
        lax.all_gather(dt_bias, "fsdp", axis=0, tiled=True),
        lax.all_gather(a_log, "fsdp", axis=1, tiled=True),
        lax.all_gather(d_skip, "fsdp", axis=0, tiled=True),
        lax.all_gather(out_weight, "fsdp", axis=1, tiled=True),
    )
    (
        gain_full,
        in_full,
        conv_full,
        conv_bias_full,
        x_full,
        dt_full,
        dt_bias_full,
        rate_full,
        skip_full,
        out_full,
    ) = gathered
    whole = lax.all_gather(tokens, "tp", axis=1, tiled=True)
    seq_count = whole.shape[0]
    seq_len = whole.shape[1]
    kernel = conv_full.shape[0]
    rank = dt_full.shape[0]
    state_width = rate_full.shape[0]
    live_mask = (jnp.arange(seq_len)[None, :] < lengths[:, None]).astype(jnp.float32)[:, :, None]
    values = whole.astype(jnp.float32)
    inverse = lax.rsqrt(jnp.mean(values * values, axis=-1, keepdims=True) + epsilon)
    normed = (values * inverse * gain_full.astype(jnp.float32)).astype(jnp.bfloat16)
    projected = jnp.einsum("bld,dkc->blkc", normed, in_full, preferred_element_type=jnp.float32)
    conv_input = projected[:, :, 0]
    gate_input = projected[:, :, 1]
    conv_weights = conv_full.astype(jnp.float32)
    padded = jnp.pad(conv_input, ((0, 0), (kernel - 1, 0), (0, 0)))
    conv_sum = conv_bias_full.astype(jnp.float32) + sum(
        (conv_weights[offset] * padded[:, offset : offset + seq_len] for offset in range(kernel))
    )
    conv_low = jax.nn.silu(conv_sum).astype(jnp.bfloat16)
    conv_out = conv_low.astype(jnp.float32)
    mapped = lax.psum(
        jnp.einsum("blc,cj->blj", conv_low, x_full, preferred_element_type=jnp.float32), "tp"
    )
    low_rank = mapped[:, :, :rank].astype(jnp.bfloat16)
    input_map = mapped[:, :, rank : rank + state_width]
    output_map = mapped[:, :, rank + state_width :]
    step_pre = jnp.einsum(
        "blr,rc->blc", low_rank, dt_full, preferred_element_type=jnp.float32
    ) + dt_bias_full.astype(jnp.float32)
    step_size = jax.nn.softplus(step_pre) * live_mask
    decay_rate = -jnp.exp(rate_full.astype(jnp.float32))
    scans = [
        scan_fwd(step_size[s], conv_low[s], input_map[s], output_map[s], decay_rate)
        for s in range(seq_count)
    ]
    scan_out = jnp.stack([s[0] for s in scans])
    skip_values = skip_full.astype(jnp.float32)
    gate_act = jax.nn.silu(gate_input)
    before_gate = scan_out + skip_values * conv_out
    mixed = (before_gate * gate_act * live_mask).astype(jnp.bfloat16)
    partial_out = jnp.einsum("blc,cd->bld", mixed, out_full, preferred_element_type=jnp.float32)
    block_sum = lax.psum_scatter(
        partial_out.astype(jnp.bfloat16), "tp", scatter_dimension=1, tiled=True
    ).astype(jnp.float32)
    block_out = (tokens.astype(jnp.float32) + block_sum).astype(jnp.bfloat16)
    regathered = (
        lax.all_gather(norm_gain, "fsdp", axis=0, tiled=True),
        lax.all_gather(in_weight, "fsdp", axis=0, tiled=True),
        lax.all_gather(conv_weight, "fsdp", axis=1, tiled=True),
        lax.all_gather(x_weight, "fsdp", axis=0, tiled=True),
        lax.all_gather(dt_weight, "fsdp", axis=0, tiled=True),
        lax.all_gather(out_weight, "fsdp", axis=1, tiled=True),
    )
    gain_back, in_back, conv_back, x_back, dt_back, out_back = regathered
    grad_whole = lax.all_gather(cotangent, "tp", axis=1, tiled=True)
    mixed_grad = jnp.einsum("bld,cd->blc", grad_whole, out_back, preferred_element_type=jnp.float32)
    out_weight_grad = jnp.einsum(
        "blc,bld->cd", mixed, grad_whole, preferred_element_type=jnp.float32
    )
    masked_grad = mixed_grad * live_mask
    scan_grad = masked_grad * gate_act
    gate_grad = masked_grad * before_gate * silu_grad(gate_input)
    skip_grad = jnp.sum(scan_grad * conv_out, axis=(0, 1))
    backs = [
        scan_bwd(
            step_size[s],
            conv_low[s],
            input_map[s],
            output_map[s],
            scan_grad[s],
            scans[s][1],
            decay_rate,
        )
        for s in range(seq_count)
    ]
    weighted, step_part, input_grad, output_grad = (
        jnp.stack([s[i] for s in backs]) for i in range(4)
    )
    conv_scan_grad = weighted * step_size
    step_grad = step_part + weighted * conv_out
    a_log_grad = sum(s[4] for s in backs) * LN2
    pre_grad = (step_grad * live_mask * jax.nn.sigmoid(step_pre)).astype(jnp.bfloat16)
    dt_bias_grad = jnp.sum(pre_grad.astype(jnp.float32), axis=(0, 1))
    dt_weight_grad = jnp.einsum(
        "blr,blc->rc", low_rank, pre_grad, preferred_element_type=jnp.float32
    )
    rank_grad = jnp.einsum("blc,rc->blr", pre_grad, dt_back, preferred_element_type=jnp.float32)
    map_terms = jnp.concatenate(
        [rank_grad, input_grad, output_grad], axis=2
    )
    map_grad = lax.psum(map_terms.astype(jnp.bfloat16), "tp")
    x_weight_grad = jnp.einsum(
        "blc,blj->cj", conv_low, map_grad, preferred_element_type=jnp.float32
    )
    conv_out_grad = (
        scan_grad * skip_values
        + conv_scan_grad
        + jnp.einsum("blj,cj->blc", map_grad, x_back, preferred_element_type=jnp.float32)
    )
    sum_grad = conv_out_grad * silu_grad(conv_sum)
    conv_bias_grad = jnp.sum(sum_grad, axis=(0, 1))
    conv_weight_grad = jnp.stack(
        [
            jnp.sum(sum_grad * padded[:, offset : offset + seq_len], axis=(0, 1))
            for offset in range(kernel)
        ]
    )
    padded_grad = jnp.pad(sum_grad, ((0, 0), (0, kernel - 1), (0, 0)))
    conv_back_values = conv_back.astype(jnp.float32)
    conv_input_grad = sum(
        (
            conv_back_values[offset]
            * padded_grad[:, kernel - 1 - offset : kernel - 1 - offset + seq_len]
            for offset in range(kernel)
        )
    )
    projected_grad = jnp.stack([conv_input_grad, gate_grad], axis=2).astype(jnp.bfloat16)
    in_weight_grad = jnp.einsum(
        "bld,blkc->dkc", normed, projected_grad, preferred_element_type=jnp.float32
    )
    normed_part = jnp.einsum(
        "blkc,dkc->bld", projected_grad, in_back, preferred_element_type=jnp.float32
    )
    normed_grad = lax.psum_scatter(
        normed_part.astype(jnp.bfloat16), "tp", scatter_dimension=1, tiled=True
    ).astype(jnp.float32)
    own_values = tokens.astype(jnp.float32)
    own_inverse = lax.rsqrt(jnp.mean(own_values * own_values, axis=-1, keepdims=True) + epsilon)
    own_hat = own_values * own_inverse
    scaled = normed_grad * gain_back.astype(jnp.float32)
    input_grads = cotangent.astype(jnp.float32) + own_inverse * (
        scaled - own_hat * jnp.mean(scaled * own_hat, axis=-1, keepdims=True)
    )
    gain_grad = lax.psum(jnp.sum(normed_grad * own_hat, axis=(0, 1)), "tp")
    reduced = (
        lax.psum_scatter(gain_grad, "fsdp", scatter_dimension=0, tiled=True),
        lax.psum_scatter(in_weight_grad, "fsdp", scatter_dimension=0, tiled=True),
        lax.psum_scatter(conv_weight_grad, "fsdp", scatter_dimension=1, tiled=True),
        lax.psum_scatter(conv_bias_grad, "fsdp", scatter_dimension=0, tiled=True),
        lax.psum_scatter(x_weight_grad, "fsdp", scatter_dimension=0, tiled=True),
        lax.psum_scatter(dt_weight_grad, "fsdp", scatter_dimension=0, tiled=True),
        lax.psum_scatter(dt_bias_grad, "fsdp", scatter_dimension=0, tiled=True),
        lax.psum_scatter(a_log_grad, "fsdp", scatter_dimension=1, tiled=True),
        lax.psum_scatter(skip_grad, "fsdp", scatter_dimension=0, tiled=True),
        lax.psum_scatter(out_weight_grad, "fsdp", scatter_dimension=1, tiled=True),
    )
    return (
        block_out,
        input_grads,
        reduced[0],
        reduced[1],
        reduced[2],
        reduced[3],
        reduced[4],
        reduced[5],
        reduced[6],
        reduced[7],
        reduced[8],
        reduced[9],
    )


def solution(mesh):
    return jax.shard_map(
        shards,
        mesh=mesh,
        in_specs=(
            P("fsdp", "tp", None),
            P("fsdp"),
            P("fsdp"),
            P("fsdp", None, "tp"),
            P(None, ("tp", "fsdp")),
            P(("tp", "fsdp")),
            P(("tp", "fsdp"), None),
            P("fsdp", "tp"),
            P(("tp", "fsdp")),
            P(None, ("tp", "fsdp")),
            P(("tp", "fsdp")),
            P("tp", "fsdp"),
            P("fsdp", "tp", None),
        ),
        out_specs=(
            P("fsdp", "tp", None),
            P("fsdp", "tp", None),
            P("fsdp"),
            P("fsdp", None, "tp"),
            P(None, ("tp", "fsdp")),
            P(("tp", "fsdp")),
            P(("tp", "fsdp"), None),
            P("fsdp", "tp"),
            P(("tp", "fsdp")),
            P(None, ("tp", "fsdp")),
            P(("tp", "fsdp")),
            P("tp", "fsdp"),
        ),
        check_vma=False,
    )
```

```python
import functools

import jax
import jax.numpy as jnp
from jax import lax
from jax.experimental import pallas as pl
from jax.experimental.pallas import tpu as pltpu
from jax.sharding import PartitionSpec as P

bf16 = jnp.bfloat16
f32 = jnp.float32
LOG2E = 1.4426950408889634
LN2 = 0.6931471805599453
SUB = 16
ROWS = 128
UNROLL = 16
NT = (((1,), (1,)), ((), ()))
TN = (((0,), (0,)), ((), ()))
epsilon = 1e-05
VMEM_LIMIT = 56 * 2**20


def dot(a, b, dims=(((1,), (0,)), ((), ()))):
    return lax.dot_general(a, b, dims, preferred_element_type=f32)


def shape(dims, kind):
    return jax.ShapeDtypeStruct(dims, kind)


def iota(dims, axis):
    return lax.broadcasted_iota(jnp.int32, dims, axis)


def params():
    return pltpu.CompilerParams(vmem_limit_bytes=VMEM_LIMIT)


def halves(values):
    high = values.astype(bf16)
    return high, (values - high.astype(f32)).astype(bf16)


def spread(parts, first, width, positions):
    rows, cols = parts[0].shape
    wide = positions * width
    pick = (iota((cols, wide), 1) % width + first == iota((cols, wide), 0)).astype(bf16)
    keep = iota((rows, wide), 1) // width == iota((rows, wide), 0) % positions
    return [jnp.where(keep, dot(part, pick), 0.0).astype(bf16) for part in parts]


def outer(e_high, e_low, v_high, v_low):
    left = jnp.concatenate([e_high, e_high, e_low], 0)
    right = jnp.concatenate([v_high, v_low, v_high], 0)
    return dot(left, right, TN)


def live_rows(length, first, rows):
    return (iota((rows, 1), 0) + first < length).astype(f32)


def front_kernel(
    pieces, order, place, tokens, gain, conv_w, conv_b, x_w, *refs
):
    piece_refs = refs[:pieces]
    normed_ref, w_ref, input_ref, gate_ref, sum_ref, low_ref, map_ref, halo = refs[pieces:]
    rows = tokens.shape[1]
    chans = conv_w.shape[1]
    taps = conv_w.shape[0]

    @pl.when(pl.program_id(0) == 0)
    def _():
        for index in range(pieces):
            depth = piece_refs[index].shape[0]
            start = pl.multiple_of(place[index] * depth, depth)
            w_ref[pl.ds(start, depth), :] = piece_refs[index][...]
        halo[:8] = jnp.zeros_like(halo[:8])

    values = tokens[0].astype(f32)
    inverse = lax.rsqrt(jnp.mean(values * values, axis=-1, keepdims=True) + epsilon)
    normed = (values * inverse * gain[...]).astype(bf16)
    normed_ref[...] = normed
    projected = dot(normed, w_ref[...])
    conv_in = projected[:, :chans]
    input_ref[...] = conv_in
    gate_ref[...] = projected[:, chans:]
    halo[8:] = conv_in
    total = conv_b[...]
    for tap in range(taps):
        first = 8 - taps + 1 + tap
        total = total + conv_w[tap : tap + 1] * halo[first : first + rows]
    halo[:8] = conv_in[rows - 8 :]
    sum_ref[...] = total
    low = (total * jax.nn.sigmoid(total)).astype(bf16)
    low_ref[...] = low
    map_ref[...] = dot(low, x_w[...], NT)


def front(order, place, stack, gain, conv_w, conv_b, x_w, pieces):
    count, rows, depth = stack.shape
    total = count * rows
    chans = conv_w.shape[1]
    maps = x_w.shape[0]
    full = lambda a: pl.BlockSpec(a.shape, lambda i, *_: (0,) * a.ndim)
    row = lambda w: pl.BlockSpec((rows, w), lambda i, *_: (i, 0))
    both = pieces[0].shape[1]
    return pl.pallas_call(
        functools.partial(front_kernel, len(pieces)),
        grid_spec=pltpu.PrefetchScalarGridSpec(
            num_scalar_prefetch=2,
            grid=(count,),
            in_specs=[pl.BlockSpec((1, rows, depth), lambda i, o, p: (o[i], 0, 0))]
            + [full(a) for a in (gain, conv_w, conv_b, x_w)]
            + [full(a) for a in pieces],
            out_specs=[
                row(depth),
                pl.BlockSpec((depth, both), lambda i, *_: (0, 0)),
                row(chans),
                row(chans),
                row(chans),
                row(chans),
                row(maps),
            ],
            scratch_shapes=[pltpu.VMEM((rows + 8, chans), f32)],
        ),
        out_shape=[
            shape((total, depth), bf16),
            shape((depth, both), bf16),
            shape((total, chans), f32),
            shape((total, chans), f32),
            shape((total, chans), f32),
            shape((total, chans), bf16),
            shape((total, maps), f32),
        ],
        compiler_params=params(),
        name="front",
    )(order, place, stack, gain, conv_w, conv_b, x_w, *pieces)


def forward_kernel(
    length, own, got, low, gate, dt_w, dt_b, a_log, skip,
    mixed_ref, before_ref, step_ref, h_ref, drive, state,
):
    rows, chans = low.shape
    width = a_log.shape[0]
    rank = dt_w.shape[0] - 2 * width
    half = width // 2
    first = pl.program_id(0) * rows

    @pl.when(pl.program_id(0) == 0)
    def _():
        state[...] = jnp.zeros_like(state)

    live = live_rows(length[0], first, rows)
    mapped = own[...] + got[...].astype(f32)
    parts = halves(mapped)
    step = jax.nn.softplus(dot(parts[0], dt_w[...]) + dt_b[...]) * live
    step_ref[...] = step
    conv_out = low[...].astype(f32)
    b_high, b_low = spread(parts, rank, width, SUB)
    x_high, x_low = halves(step * conv_out)
    for index in range(rows // SUB):
        s = slice(index * SUB, (index + 1) * SUB)
        drive[index * SUB * width : (index + 1) * SUB * width, :] = outer(
            b_high[s], b_low[s], x_high[s], x_low[s]
        )
    rate = -jnp.exp(a_log[...]) * LOG2E
    rate_0, rate_1 = rate[:half], rate[half:]

    def body(block, carried):
        h_0, h_1 = carried
        steps = step_ref[pl.ds(pl.multiple_of(block * UNROLL, UNROLL), UNROLL), :]
        for k in range(UNROLL):
            wide = jnp.broadcast_to(steps[k : k + 1], (half, chans))
            base = pl.multiple_of(block * (UNROLL * width), UNROLL * width) + k * width
            h_0 = jnp.exp2(wide * rate_0) * h_0 + drive[pl.ds(base, half), :]
            h_1 = jnp.exp2(wide * rate_1) * h_1 + drive[pl.ds(base + half, half), :]
            h_ref[pl.ds(base, width), :] = jnp.concatenate([h_0, h_1], 0).astype(bf16)
        return h_0, h_1

    h_0, h_1 = lax.fori_loop(0, rows // UNROLL, body, (state[:half], state[half:]))
    state[:half] = h_0
    state[half:] = h_1
    c_high, c_low = spread(parts, rank + width, width, SUB)
    scan = []
    for index in range(rows // SUB):
        s = slice(index * SUB, (index + 1) * SUB)
        both = dot(
            jnp.concatenate([c_high[s], c_low[s]], 0),
            h_ref[index * SUB * width : (index + 1) * SUB * width, :],
        )
        scan.append(both[:SUB] + both[SUB:])
    before = jnp.concatenate(scan, 0) + skip[...] * conv_out
    before_ref[...] = before
    gates = gate[...]
    mixed_ref[...] = (before * (gates * jax.nn.sigmoid(gates)) * live).astype(bf16)


def forward(length, own, got, low, gate, dt_w, dt_b, a_log, skip):
    total, chans = low.shape
    width = a_log.shape[0]
    row = lambda w: pl.BlockSpec((ROWS, w), lambda i, *_: (i, 0))
    full = lambda a: pl.BlockSpec(a.shape, lambda i, *_: (0,) * a.ndim)
    maps = own.shape[1]
    return pl.pallas_call(
        forward_kernel,
        grid_spec=pltpu.PrefetchScalarGridSpec(
            num_scalar_prefetch=1,
            grid=(total // ROWS,),
            in_specs=[row(maps), row(maps), row(chans), row(chans)]
            + [full(a) for a in (dt_w, dt_b, a_log, skip)],
            out_specs=[
                row(chans),
                row(chans),
                row(chans),
                pl.BlockSpec((ROWS * width, chans), lambda i, *_: (i, 0)),
            ],
            scratch_shapes=[
                pltpu.VMEM((ROWS * width, chans), f32),
                pltpu.VMEM((width, chans), f32),
            ],
        ),
        out_shape=[
            shape((total, chans), bf16),
            shape((total, chans), f32),
            shape((total, chans), f32),
            shape((total * width, chans), bf16),
        ],
        compiler_params=params(),
        name="forward",
    )(length, own, got, low, gate, dt_w, dt_b, a_log, skip)


def gate_kernel(length, grad, out_w, gate, before, low, scan_ref, gate_ref, skip_ref):
    rows = grad.shape[0]
    live = live_rows(length[0], pl.program_id(0) * rows, rows)
    masked = dot(grad[...], out_w[...], NT) * live
    gates = gate[...]
    sigma = jax.nn.sigmoid(gates)
    scan_grad = masked * (gates * sigma)
    scan_ref[...] = scan_grad
    gate_ref[...] = (masked * before[...] * (sigma * (1.0 + gates * (1.0 - sigma)))).astype(bf16)

    @pl.when(pl.program_id(0) == 0)
    def _():
        skip_ref[...] = jnp.zeros_like(skip_ref)

    skip_ref[...] += jnp.sum(scan_grad * low[...].astype(f32), axis=0, keepdims=True)


def gate_back(length, grad, out_w, gate, before, low):
    total, chans = low.shape
    rows = 256
    row = lambda w: pl.BlockSpec((rows, w), lambda i, *_: (i, 0))
    full = lambda a: pl.BlockSpec(a.shape, lambda i, *_: (0,) * a.ndim)
    return pl.pallas_call(
        gate_kernel,
        grid_spec=pltpu.PrefetchScalarGridSpec(
            num_scalar_prefetch=1,
            grid=(total // rows,),
            in_specs=[row(grad.shape[1]), full(out_w), row(chans), row(chans), row(chans)],
            out_specs=[row(chans), row(chans), pl.BlockSpec((1, chans), lambda i, *_: (0, 0))],
        ),
        out_shape=[shape((total, chans), f32), shape((total, chans), bf16), shape((1, chans), f32)],
        compiler_params=params(),
        name="gate_back",
    )(length, grad, out_w, gate, before, low)


def backward_kernel(
    length, own, got, low, step_ref, scan_grad_ref, h_ref, last_ref, dt_w, dt_b, a_log, skip,
    map_ref, out_ref, rate_ref, dt_w_ref, dt_b_ref, drive, carry, grads, terms,
):
    rows, chans = low.shape
    width = a_log.shape[0]
    rank = dt_w.shape[0] - 2 * width
    half = width // 2
    turn = pl.program_id(0)
    turns = pl.num_programs(0)

    @pl.when(turn == 0)
    def _():
        carry[...] = jnp.zeros_like(carry)
        rate_ref[...] = jnp.zeros_like(rate_ref)
        dt_w_ref[...] = jnp.zeros_like(dt_w_ref)
        dt_b_ref[...] = jnp.zeros_like(dt_b_ref)

    mapped = own[...] + got[...].astype(f32)
    parts = halves(mapped)
    c_high, c_low = spread(parts, rank + width, width, SUB)
    scan_grad = scan_grad_ref[...]
    y_high, y_low = halves(scan_grad)
    for index in range(rows // SUB):
        s = slice(index * SUB, (index + 1) * SUB)
        drive[index * SUB * width : (index + 1) * SUB * width, :] = outer(
            c_high[s], c_low[s], y_high[s], y_low[s]
        )
    rate = -jnp.exp(a_log[...]) * LOG2E
    rate_0, rate_1 = rate[:half], rate[half:]
    before = jnp.where(turn == turns - 1, jnp.zeros_like(last_ref[...]), last_ref[...])

    def body(back, carried):
        q_0, q_1, sum_0, sum_1 = carried
        block = rows // UNROLL - 1 - back
        steps = step_ref[pl.ds(pl.multiple_of(block * UNROLL, UNROLL), UNROLL), :]
        for k in reversed(range(UNROLL)):
            wide = jnp.broadcast_to(steps[k : k + 1], (half, chans))
            base = pl.multiple_of(block * (UNROLL * width), UNROLL * width) + k * width
            g_0 = drive[pl.ds(base, half), :] + q_0
            g_1 = drive[pl.ds(base + half, half), :] + q_1
            grads[pl.ds(base, width), :] = jnp.concatenate([g_0, g_1], 0).astype(bf16)
            q_0 = jnp.exp2(wide * rate_0) * g_0
            q_1 = jnp.exp2(wide * rate_1) * g_1
            if k == 0:
                start = pl.multiple_of(jnp.maximum(base - width, 0), width)
                past = jnp.where(block == 0, before, h_ref[pl.ds(start, width), :])
            else:
                past = h_ref[pl.ds(base - width, width), :]
            past = past.astype(f32)
            m_0 = rate_0 * (q_0 * past[:half])
            m_1 = rate_1 * (q_1 * past[half:])
            sum_0 = sum_0 + wide * m_0
            sum_1 = sum_1 + wide * m_1
            terms[pl.ds(base, width), :] = jnp.concatenate([m_0, m_1], 0).astype(bf16)
        return q_0, q_1, sum_0, sum_1

    q_0, q_1, sum_0, sum_1 = lax.fori_loop(
        0, rows // UNROLL, body, (carry[:half], carry[half:], rate_ref[:half], rate_ref[half:])
    )
    carry[:half] = q_0
    carry[half:] = q_1
    rate_ref[:half] = sum_0
    rate_ref[half:] = sum_1
    b_high, b_low = spread(parts, rank, width, SUB)
    wide = SUB * width
    own_group = iota((SUB, wide), 1) // width == iota((SUB, wide), 0)
    ones = own_group.astype(bf16)
    maps = rank + 2 * width
    pick_b = (iota((wide, maps), 0) % width + rank == iota((wide, maps), 1)).astype(bf16)
    pick_c = (iota((wide, maps), 0) % width + rank + width == iota((wide, maps), 1)).astype(bf16)
    steps = step_ref[...]
    conv_out = low[...].astype(f32)
    drive_low = (steps * conv_out).astype(bf16)
    weighted, stepped, crossed = [], [], []
    for index in range(rows // SUB):
        s = slice(index * SUB, (index + 1) * SUB)
        big = slice(index * SUB * width, (index + 1) * SUB * width)
        grad = grads[big, :]
        both = dot(jnp.concatenate([b_high[s], b_low[s]], 0), grad)
        weighted.append(both[:SUB] + both[SUB:])
        stepped.append(dot(ones, terms[big, :]))
        on_b = jnp.where(own_group, dot(drive_low[s], grad, NT), 0.0).astype(bf16)
        on_c = jnp.where(own_group, dot(y_high[s], h_ref[big, :], NT), 0.0).astype(bf16)
        crossed.append(dot(on_b, pick_b) + dot(on_c, pick_c))
    weighted = jnp.concatenate(weighted, 0)
    step_grad = jnp.concatenate(stepped, 0) * LN2 + conv_out * weighted
    live = live_rows(length[0], (turns - 1 - turn) * rows, rows)
    step_pre = dot(parts[0], dt_w[...]) + dt_b[...]
    pre_grad = (step_grad * live * jax.nn.sigmoid(step_pre)).astype(bf16)
    dt_b_ref[...] += jnp.sum(pre_grad.astype(f32), axis=0, keepdims=True)
    dt_w_ref[...] += dot(parts[0], pre_grad, TN)
    map_ref[...] = jnp.concatenate(crossed, 0) + dot(pre_grad, dt_w[...], NT)
    out_ref[...] = scan_grad * skip[...] + steps * weighted


def backward(length, own, got, low, step, scan_grad, h, dt_w, dt_b, a_log, skip):
    total, chans = low.shape
    width = a_log.shape[0]
    turns = total // ROWS
    at = lambda i: turns - 1 - i
    row = lambda w: pl.BlockSpec((ROWS, w), lambda i, *_: (at(i), 0))
    full = lambda a: pl.BlockSpec(a.shape, lambda i, *_: (0,) * a.ndim)
    maps = own.shape[1]
    return pl.pallas_call(
        backward_kernel,
        grid_spec=pltpu.PrefetchScalarGridSpec(
            num_scalar_prefetch=1,
            grid=(turns,),
            in_specs=[
                row(maps),
                row(maps),
                row(chans),
                row(chans),
                row(chans),
                pl.BlockSpec((ROWS * width, chans), lambda i, *_: (at(i), 0)),
                pl.BlockSpec((width, chans), lambda i, *_: (jnp.maximum(at(i) * ROWS - 1, 0), 0)),
            ]
            + [full(a) for a in (dt_w, dt_b, a_log, skip)],
            out_specs=[row(maps), row(chans), full(a_log), full(dt_w), full(dt_b)],
            scratch_shapes=[
                pltpu.VMEM((ROWS * width, chans), f32),
                pltpu.VMEM((width, chans), f32),
                pltpu.VMEM((ROWS * width, chans), bf16),
                pltpu.VMEM((ROWS * width, chans), bf16),
            ],
        ),
        out_shape=[
            shape((total, maps), f32),
            shape((total, chans), f32),
            shape(a_log.shape, f32),
            shape(dt_w.shape, f32),
            shape(dt_b.shape, f32),
        ],
        compiler_params=params(),
        name="backward",
    )(length, own, got, low, step, scan_grad, h, h, dt_w, dt_b, a_log, skip)


def back_kernel(
    slot, own, got, x_w, out_grad, conv_sum, conv_in, low, conv_w, gate_grad, normed, tokens, w,
    part_ref, weight_ref, x_ref, conv_w_ref, conv_b_ref, gain_ref, halo, total,
):
    rows, chans = low.shape
    taps = conv_w.shape[0]
    turn = pl.program_id(0)

    @pl.when(turn == 0)
    def _():
        halo[rows:] = jnp.zeros_like(halo[rows:])
        total[...] = jnp.zeros_like(total)
        for ref in (x_ref, conv_w_ref, conv_b_ref, gain_ref):
            ref[...] = jnp.zeros_like(ref)

    map_grad = (own[...] + got[...].astype(f32)).astype(bf16)
    x_ref[...] += dot(map_grad, low[...], TN)
    values = conv_sum[...]
    sigma = jax.nn.sigmoid(values)
    sum_grad = (out_grad[...] + dot(map_grad, x_w[...])) * (sigma * (1.0 + values * (1.0 - sigma)))
    conv_b_ref[...] += jnp.sum(sum_grad, axis=0, keepdims=True)
    halo[:rows] = sum_grad
    inputs = conv_in[...]
    input_grad = jnp.zeros_like(inputs)
    for tap in range(taps):
        first = taps - 1 - tap
        moved = halo[first : first + rows]
        input_grad = input_grad + conv_w[tap : tap + 1] * moved
        conv_w_ref[tap : tap + 1] += jnp.sum(inputs * moved, axis=0, keepdims=True)
    halo[rows:] = sum_grad[:8]
    input_grad = input_grad.astype(bf16)
    total[...] += dot(normed[...], input_grad, TN)
    part = dot(jnp.concatenate([input_grad, gate_grad[...]], 1), w[...], NT)
    part_ref[0] = part.astype(bf16)
    values = tokens[0].astype(f32)
    inverse = lax.rsqrt(jnp.mean(values * values, axis=-1, keepdims=True) + epsilon)
    gain_ref[...] += jnp.sum(part * (values * inverse), axis=0, keepdims=True)

    @pl.when(turn == pl.num_programs(0) - 1)
    def _():
        weight_ref[...] = total[...].astype(bf16)


def back(slot, order, own, got, x_w, out_grad, conv_sum, conv_in, low, conv_w, gate_grad, normed, stack, w):
    chans = low.shape[1]
    count, rows, depth = stack.shape
    at = lambda i: count - 1 - i
    row = lambda a: pl.BlockSpec((rows, a.shape[1]), lambda i, *_: (at(i), 0))
    full = lambda a: pl.BlockSpec(a.shape, lambda i, *_: (0,) * len(a.shape))
    outs = [
        shape((count, rows, depth), bf16),
        shape((depth, chans), bf16),
        shape(x_w.shape, f32),
        shape(conv_w.shape, f32),
        shape((1, chans), f32),
        shape((1, depth), f32),
    ]

    def kernel(slot, order, *refs):
        back_kernel(slot, *refs)

    return pl.pallas_call(
        kernel,
        grid_spec=pltpu.PrefetchScalarGridSpec(
            num_scalar_prefetch=2,
            grid=(count,),
            in_specs=[
                row(own),
                row(got),
                full(x_w),
                row(out_grad),
                row(conv_sum),
                row(conv_in),
                row(low),
                full(conv_w),
                row(gate_grad),
                row(normed),
                pl.BlockSpec((1, rows, depth), lambda i, s, o: (o[at(i)], 0, 0)),
                full(w),
            ],
            out_specs=[pl.BlockSpec((1, rows, depth), lambda i, s, o: (s[at(i)], 0, 0))]
            + [full(a) for a in outs[1:]],
            scratch_shapes=[pltpu.VMEM((rows + 8, chans), f32), pltpu.VMEM((depth, chans), f32)],
        ),
        out_shape=outs,
        compiler_params=params(),
        name="back",
    )(slot, order, own, got, x_w, out_grad, conv_sum, conv_in, low, conv_w, gate_grad, normed, stack, w)


def project_kernel(slot, mixed, out_w, part_ref):
    part_ref[0] = dot(mixed[...], out_w[...]).astype(bf16)


def project(slot, mixed, out_w, count):
    total, chans = mixed.shape
    rows = total // count
    depth = out_w.shape[1]
    return pl.pallas_call(
        project_kernel,
        grid_spec=pltpu.PrefetchScalarGridSpec(
            num_scalar_prefetch=1,
            grid=(count,),
            in_specs=[
                pl.BlockSpec((rows, chans), lambda i, s: (i, 0)),
                pl.BlockSpec(out_w.shape, lambda i, s: (0, 0)),
            ],
            out_specs=pl.BlockSpec((1, rows, depth), lambda i, s: (s[i], 0, 0)),
        ),
        out_shape=shape((count, rows, depth), bf16),
        compiler_params=params(),
        name="project",
    )(slot, mixed, out_w)


def exchange(values, axis, size, bits):
    return lax.ppermute(values, axis, [(i, i ^ bits) for i in range(size)])


def relay(values, axis, size, cuts):
    me = lax.axis_index(axis)
    rows = values.shape[0] // cuts
    found = []
    for cut in range(cuts):
        piece = values[cut * rows : (cut + 1) * rows]
        up, down = [piece], [piece]
        for hop in range(1, size):
            pairs = range(hop - 1, size - 1)
            up.append(lax.ppermute(up[-1], axis, [(i, i + 1) for i in pairs]))
            down.append(lax.ppermute(down[-1], axis, [(size - 1 - i, size - 2 - i) for i in pairs]))
        found.append([piece] + [jnp.where(me >= k, up[k], down[size - k]) for k in range(1, size)])
    return jnp.stack([jnp.concatenate([part[k] for part in found], 0) for k in range(size)])


def gather_pieces(values, axis, size):
    even = [values] + [exchange(values, axis, size, m) for m in range(2, size, 2)]
    odd = [exchange(piece, axis, size, 1) for piece in even]
    return [piece for pair in zip(even, odd) for piece in pair]


def scatter_sum(values, axis, size):
    me = lax.axis_index(axis)
    pairs = values.reshape((size // 2, 2) + values.shape[1:])
    core = me % 2
    keep = lax.dynamic_index_in_dim(pairs, core, 1, False)
    send = lax.dynamic_index_in_dim(pairs, 1 - core, 1, False)
    summed = keep + exchange(send, axis, size, 1)
    place = me // 2
    total = lax.dynamic_index_in_dim(summed, place, 0, False).astype(f32)
    for m in range(1, size // 2):
        piece = lax.dynamic_index_in_dim(summed, place ^ m, 0, False)
        total = total + exchange(piece, axis, size, 2 * m).astype(f32)
    return total


def sum_all(values, axis, size):
    bits = 1
    while bits < size:
        got = exchange(values.astype(bf16), axis, size, 2 * bits - 1)
        bits *= 2
        if bits < size:
            values = values + got.astype(f32)
    return values, got


def shards(
    fsdp, tp, tokens, lengths, norm_gain, in_weight, conv_weight, conv_bias, x_weight, dt_weight,
    dt_bias, a_log, d_skip, out_weight, cotangent,
):
    tp_me = lax.axis_index("tp")
    fs_me = lax.axis_index("fsdp")
    chunks = jnp.arange(tp)
    order = ((tp_me - chunks) % tp).astype(jnp.int32)
    slot = ((chunks - tp_me) % tp).astype(jnp.int32)
    place = (fs_me ^ jnp.arange(fsdp)).astype(jnp.int32)
    depth = tokens.shape[2]
    part = conv_weight.shape[1]
    chans = part * fsdp
    taps = conv_weight.shape[0]
    width = a_log.shape[0]
    maps = x_weight.shape[1]
    rank = maps - 2 * width

    stack = relay(tokens[0], "tp", tp, 2)
    pieces = gather_pieces(in_weight.reshape(in_weight.shape[0], 2 * chans), "fsdp", fsdp)
    small = jnp.concatenate(
        [
            conv_weight,
            conv_bias[None],
            dt_bias[None],
            d_skip[None],
            a_log,
            x_weight.T,
            dt_weight.reshape(-1, part),
            norm_gain.reshape(-1, part),
        ],
        0,
    )
    gathered = lax.all_gather(small, "fsdp", axis=0)
    top = taps + 3 + width + maps
    by_chan = gathered[:, :top].transpose(1, 0, 2).reshape(top, chans)
    conv_w = by_chan[:taps].astype(f32)
    conv_b, dt_b, skip = (by_chan[taps + i : taps + i + 1].astype(f32) for i in range(3))
    logs = by_chan[taps + 3 : taps + 3 + width].astype(f32)
    x_w = by_chan[taps + 3 + width :]
    dt_rows = rank * chans // part // fsdp
    dt_w = gathered[:, top : top + dt_rows].reshape(rank, chans)
    dt_w = jnp.pad(dt_w, ((0, 2 * width), (0, 0)))
    gain = gathered[:, top + dt_rows :].reshape(1, depth).astype(f32)
    out_w = lax.all_gather(out_weight, "fsdp", axis=1, tiled=True)
    grad_whole = lax.all_gather(cotangent[0], "tp", axis=0, tiled=True)

    normed, w, conv_in, gate, conv_sum, low, map_part = front(
        order, place, stack, gain, conv_w, conv_b, x_w, pieces
    )
    own, got = sum_all(map_part, "tp", tp)
    mixed, before, step, h = forward(lengths, own, got, low, gate, dt_w, dt_b, logs, skip)

    sent = project(slot, mixed, out_w, tp)
    block_out = tokens.astype(f32) + scatter_chunks(sent, "tp", tp)[None]
    scan_grad, gate_grad, skip_grad = gate_back(lengths, grad_whole, out_w, gate, before, low)
    out_grad = dot(grad_whole, mixed, TN).astype(bf16)
    out_weight_grad = scatter_sum(out_grad.reshape(fsdp, -1, chans), "fsdp", fsdp)
    gate_weight = dot(normed, gate_grad, TN).astype(bf16)
    gate_weight_grad = scatter_sum(gate_weight.reshape(fsdp, -1, chans), "fsdp", fsdp)

    map_part, conv_grad, rate_grad, dt_w_grad, dt_b_grad = backward(
        lengths, own, got, low, step, scan_grad, h, dt_w, dt_b, logs, skip
    )
    own_grad, got_grad = sum_all(map_part, "tp", tp)
    sent_back, conv_weight_half, x_w_grad, conv_w_grad, conv_b_grad, gain_grad = back(
        slot, order, own_grad, got_grad, x_w, conv_grad, conv_sum, conv_in, low, conv_w,
        gate_grad, normed, stack, w,
    )
    normed_grad = scatter_chunks(sent_back, "tp", tp)
    conv_half_grad = scatter_sum(conv_weight_half.reshape(fsdp, -1, chans), "fsdp", fsdp)
    a_log_grad = rate_grad * LN2
    rows = jnp.concatenate(
        [conv_w_grad, conv_b_grad, dt_b_grad, skip_grad, a_log_grad, x_w_grad], 0
    )
    packed = jnp.concatenate(
        [
            rows.reshape(top, fsdp, part).transpose(1, 0, 2),
            dt_w_grad[:rank].reshape(fsdp, -1, part),
            gain_grad.reshape(fsdp, -1, part),
        ],
        1,
    )
    small_grad = lax.psum_scatter(packed, "fsdp", scatter_dimension=0, tiled=False)
    gain_out = lax.psum(small_grad[top + dt_rows :].reshape(-1), "tp")

    own_values = tokens.astype(f32)
    own_inverse = lax.rsqrt(jnp.mean(own_values * own_values, axis=-1, keepdims=True) + epsilon)
    own_hat = own_values * own_inverse
    scaled = normed_grad[None] * gain[None]
    input_grads = cotangent.astype(f32) + own_inverse * (
        scaled - own_hat * jnp.mean(scaled * own_hat, axis=-1, keepdims=True)
    )
    return (
        block_out.astype(bf16),
        input_grads,
        gain_out,
        jnp.stack([conv_half_grad, gate_weight_grad], 1),
        small_grad[:taps],
        small_grad[taps],
        small_grad[taps + 3 + width : top].T,
        small_grad[top : top + dt_rows].reshape(-1, chans),
        small_grad[taps + 1],
        small_grad[taps + 3 : taps + 3 + width],
        small_grad[taps + 2],
        out_weight_grad.T,
    )


def scatter_chunks(sent, axis, size):
    total = sent[0].astype(f32)
    for s in range(1, size):
        total = total + lax.ppermute(
            sent[s], axis, [(i, (i + s) % size) for i in range(size)]
        ).astype(f32)
    return total


def solution(mesh):
    sizes = dict(mesh.shape)
    return jax.shard_map(
        functools.partial(shards, sizes["fsdp"], sizes["tp"]),
        mesh=mesh,
        in_specs=(
            P("fsdp", "tp", None),
            P("fsdp"),
            P("fsdp"),
            P("fsdp", None, "tp"),
            P(None, ("tp", "fsdp")),
            P(("tp", "fsdp")),
            P(("tp", "fsdp"), None),
            P("fsdp", "tp"),
            P(("tp", "fsdp")),
            P(None, ("tp", "fsdp")),
            P(("tp", "fsdp")),
            P("tp", "fsdp"),
            P("fsdp", "tp", None),
        ),
        out_specs=(
            P("fsdp", "tp", None),
            P("fsdp", "tp", None),
            P("fsdp"),
            P("fsdp", None, "tp"),
            P(None, ("tp", "fsdp")),
            P(("tp", "fsdp")),
            P(("tp", "fsdp"), None),
            P("fsdp", "tp"),
            P(("tp", "fsdp")),
            P(None, ("tp", "fsdp")),
            P(("tp", "fsdp")),
            P("tp", "fsdp"),
        ),
        check_vma=False,
    )
```

```python
import functools

import jax
import jax.numpy as jnp
from jax import lax
from jax.experimental import pallas as pl
from jax.experimental.pallas import tpu as pltpu
from jax.sharding import PartitionSpec as P

bf16 = jnp.bfloat16
f32 = jnp.float32
LOG2E = 1.4426950408889634
LN2 = 0.6931471805599453
ROWS = 128
STEPS = 16
LANES = 128
NT = (((1,), (1,)), ((), ()))
TN = (((0,), (0,)), ((), ()))
epsilon = 1e-05
VMEM_LIMIT = 56 * 2**20


def dot(a, b, dims=(((1,), (0,)), ((), ()))):
    return lax.dot_general(a, b, dims, preferred_element_type=f32)


def shape(dims, kind):
    return jax.ShapeDtypeStruct(dims, kind)


def iota(dims, axis):
    return lax.broadcasted_iota(jnp.int32, dims, axis)


def params():
    return pltpu.CompilerParams(vmem_limit_bytes=VMEM_LIMIT)


def cost(micros):
    return pl.CostEstimate(
        flops=int(micros * 1e9), bytes_accessed=int(micros * 3e6), transcendentals=0
    )


def halves(values):
    high = values.astype(bf16)
    return high, (values - high.astype(f32)).astype(bf16)


def spread(columns):
    width, rows = columns.shape
    wide = STEPS * width
    pick = (iota((width, wide), 1) % width == iota((width, wide), 0)).astype(bf16)
    keep = iota((rows, wide), 1) // width == iota((rows, wide), 0) % STEPS
    return jnp.where(keep, dot(columns, pick, TN), 0.0).astype(bf16)


def to_lanes(target, columns):
    width, rows = columns.shape
    wide = STEPS * width
    parts = [spread(part) for part in halves(columns)]
    ones = jnp.ones((2 * STEPS, LANES), bf16)
    for index in range(rows // STEPS):
        s = slice(index * STEPS, (index + 1) * STEPS)
        both = jnp.concatenate([part[s] for part in parts], 0)
        target[index * wide : (index + 1) * wide, :] = dot(both, ones, TN)


def across(values, chans):
    return jnp.concatenate([values] * (chans // LANES), 1)


def row_of(ref, index, count):
    return ref[pl.ds(index, count, stride=0), :]


def twice(values):
    return jnp.concatenate([values, values], 0).astype(bf16)


def fold(values):
    return sum(values[:, i : i + LANES] for i in range(0, values.shape[1], LANES))


def lane_sums(values, width):
    rows = values.shape[0] // width
    sums = dot(values, jnp.ones((LANES, rows), bf16))
    lane = iota((width, rows), 1)
    kept = [jnp.zeros((width, rows), f32)] * 4
    for t in range(rows):
        kept[t % 4] = jnp.where(lane == t, sums[t * width : (t + 1) * width], kept[t % 4])
    return (kept[0] + kept[1]) + (kept[2] + kept[3])


def live_rows(length, first, rows):
    return (iota((rows, 1), 0) + first < length).astype(f32)


def full(array):
    return pl.BlockSpec(array.shape, lambda *_: (0,) * len(array.shape))


class Rows:
    def __init__(self, maps, width, taps):
        self.maps = maps
        self.width = width
        self.taps = taps
        self.rank = maps - 2 * width
        self.first = maps + width
        self.count = -(-(self.first + taps + 3) // 16) * 16

    def x_w(self, ref):
        return ref[: self.maps, :]

    def a_log(self, ref):
        return ref[self.maps : self.first, :].astype(f32)

    def rest(self, ref):
        return ref[self.first :, :].astype(f32)


def front_kernel(lay, shards, pieces, order, place, gain, small, *refs):
    token_refs = refs[:shards]
    piece_refs = refs[shards : shards + pieces]
    (
        normed_ref, w_ref, input_ref, gate_ref, sum_ref, low_ref, map_ref, send_ref, halo, tokens,
    ) = refs[shards + pieces :]
    rows = tokens.shape[0]
    chans = small.shape[1]
    taps = lay.taps
    turn = pl.program_id(0)

    @pl.when(turn == 0)
    def _():
        for index in range(pieces):
            depth = piece_refs[index].shape[0]
            start = pl.multiple_of(place[index] * depth, depth)
            w_ref[pl.ds(start, depth), :] = piece_refs[index][...]
        halo[:8] = jnp.zeros_like(halo[:8])

    for index in range(shards):

        @pl.when(order[turn] == index)
        def _(index=index):
            tokens[...] = token_refs[index][...].astype(f32)

    values = tokens[...]
    inverse = lax.rsqrt(jnp.mean(values * values, axis=-1, keepdims=True) + epsilon)
    normed = (values * inverse * gain[...]).astype(bf16)
    normed_ref[...] = normed
    projected = dot(normed, w_ref[...])
    conv_in = projected[:, :chans]
    input_ref[...] = conv_in
    gate_ref[...] = projected[:, chans:]
    halo[8:] = conv_in
    rest = lay.rest(small)
    total = rest[taps : taps + 1]
    for tap in range(taps):
        first = 8 - taps + 1 + tap
        total = total + rest[tap : tap + 1] * halo[first : first + rows]
    halo[:8] = conv_in[rows - 8 :]
    sum_ref[...] = total
    low = (total * jax.nn.sigmoid(total)).astype(bf16)
    low_ref[...] = low
    mapped = dot(lay.x_w(small), low, NT)
    map_ref[...] = mapped
    send_ref[...] = mapped.astype(bf16)


def front(lay, order, place, shards, gain, small, pieces):
    rows, depth = shards[0].shape
    total = len(shards) * rows
    chans = small.shape[1]
    row = lambda w: pl.BlockSpec((rows, w), lambda i, *_: (i, 0))
    column = lambda w: pl.BlockSpec((w, rows), lambda i, *_: (0, i))
    both = pieces[0].shape[1]
    return pl.pallas_call(
        functools.partial(front_kernel, lay, len(shards), len(pieces)),
        grid_spec=pltpu.PrefetchScalarGridSpec(
            num_scalar_prefetch=2,
            grid=(len(shards),),
            in_specs=[full(a) for a in (gain, small, *shards, *pieces)],
            out_specs=[
                row(depth),
                pl.BlockSpec((depth, both), lambda i, *_: (0, 0)),
                row(chans),
                row(chans),
                row(chans),
                row(chans),
                column(lay.maps),
                column(lay.maps),
            ],
            scratch_shapes=[pltpu.VMEM((rows + 8, chans), f32), pltpu.VMEM((rows, depth), f32)],
        ),
        out_shape=[
            shape((total, depth), bf16),
            shape((depth, both), bf16),
            shape((total, chans), f32),
            shape((total, chans), f32),
            shape((total, chans), f32),
            shape((total, chans), bf16),
            shape((lay.maps, total), f32),
            shape((lay.maps, total), bf16),
        ],
        compiler_params=params(),
        cost_estimate=cost(9),
        name="front",
    )(order, place, gain, small, *shards, *pieces)


def forward_kernel(
    lay, length, slot, own, got, low, gate, dt_w, small, out_w,
    mixed_ref, before_ref, step_ref, h_ref, sent_ref, state, drive, lanes, step_rows, drive_rows,
):
    rows, chans = low.shape
    width, rank, taps = lay.width, lay.rank, lay.taps
    half = width // 2
    wide = STEPS * width

    @pl.when(pl.program_id(0) == 0)
    def _():
        state[...] = jnp.zeros_like(state)

    live = live_rows(length[0], pl.program_id(0) * rows, rows)
    mapped = own[...] + got[...].astype(f32)
    rest = lay.rest(small)
    step_pre = dot(mapped[:rank].astype(bf16), dt_w[...], TN) + rest[taps + 1 : taps + 2]
    step = jax.nn.softplus(step_pre) * live
    step_ref[...] = step
    conv_out = low[...].astype(f32)
    drive[...] = step * conv_out
    to_lanes(lanes, mapped[rank : rank + width])
    rate = -jnp.exp(lay.a_log(small)) * LOG2E
    rate_0, rate_1 = rate[:half], rate[half:]

    def body(block, carried):
        h_0, h_1 = carried
        s = pl.ds(pl.multiple_of(block * STEPS, STEPS), STEPS)
        step_rows[...] = step_ref[s, :]
        drive_rows[...] = drive[s, :]
        for k in range(STEPS):
            steps = row_of(step_rows, k, half)
            drives = row_of(drive_rows, k, half)
            base = pl.multiple_of(block * wide, wide) + k * width
            b_0 = across(lanes[pl.ds(base, half), :], chans)
            b_1 = across(lanes[pl.ds(base + half, half), :], chans)
            h_0 = jnp.exp2(steps * rate_0) * h_0 + drives * b_0
            h_1 = jnp.exp2(steps * rate_1) * h_1 + drives * b_1
            h_ref[pl.ds(base, width), :] = jnp.concatenate([h_0, h_1], 0).astype(bf16)
        return h_0, h_1

    h_0, h_1 = lax.fori_loop(0, rows // STEPS, body, (state[:half], state[half:]))
    state[:half] = h_0
    state[half:] = h_1
    outs = spread(mapped[rank + width :].astype(bf16))
    scan = [
        dot(outs[i * STEPS : (i + 1) * STEPS], h_ref[i * wide : (i + 1) * wide, :])
        for i in range(rows // STEPS)
    ]
    before = jnp.concatenate(scan, 0) + rest[taps + 2 : taps + 3] * conv_out
    before_ref[...] = before
    gates = gate[...]
    mixed = (before * (gates * jax.nn.sigmoid(gates)) * live).astype(bf16)
    mixed_ref[...] = mixed
    sent_ref[0] = dot(mixed, out_w[...]).astype(bf16)


def forward(lay, length, slot, own, got, low, gate, dt_w, small, out_w):
    total, chans = low.shape
    count = slot.shape[0]
    part = total // count
    blocks = part // ROWS
    depth = out_w.shape[1]
    width = lay.width
    row = lambda w: pl.BlockSpec((ROWS, w), lambda i, *_: (i, 0))
    column = lambda w: pl.BlockSpec((w, ROWS), lambda i, *_: (0, i))
    return pl.pallas_call(
        functools.partial(forward_kernel, lay),
        grid_spec=pltpu.PrefetchScalarGridSpec(
            num_scalar_prefetch=2,
            grid=(total // ROWS,),
            in_specs=[column(lay.maps), column(lay.maps), row(chans), row(chans)]
            + [full(a) for a in (dt_w, small, out_w)],
            out_specs=[
                row(chans),
                row(chans),
                row(chans),
                pl.BlockSpec((ROWS * width, chans), lambda i, *_: (i, 0)),
                pl.BlockSpec((1, ROWS, depth), lambda i, n, s: (s[i // blocks], i % blocks, 0)),
            ],
            scratch_shapes=[
                pltpu.VMEM((width, chans), f32),
                pltpu.VMEM((ROWS, chans), f32),
                pltpu.VMEM((ROWS * width, LANES), f32),
                pltpu.VMEM((STEPS, chans), f32),
                pltpu.VMEM((STEPS, chans), f32),
            ],
        ),
        out_shape=[
            shape((total, chans), bf16),
            shape((total, chans), f32),
            shape((total, chans), f32),
            shape((total * width, chans), bf16),
            shape((count, part, depth), bf16),
        ],
        compiler_params=params(),
        cost_estimate=cost(24),
        name="forward",
    )(length, slot, own, got, low, gate, dt_w, small, out_w)


def backward_kernel(
    lay, length, own, got, low, gate, before_ref, step_ref, grad, h_ref, last_ref, dt_w, small, out_w,
    map_ref, send_ref, out_ref, gate_ref, rate_ref, dt_w_ref, bias_ref,
    carry, grads, terms, drive, scan_grad, lanes, cross_b, cross_c, step_rows, drive_rows, grad_rows,
):
    rows, chans = low.shape
    width, rank, taps = lay.width, lay.rank, lay.taps
    half = width // 2
    wide = STEPS * width
    turn = pl.program_id(0)
    turns = pl.num_programs(0)

    @pl.when(turn == 0)
    def _():
        for ref in (carry, rate_ref, dt_w_ref, bias_ref):
            ref[...] = jnp.zeros_like(ref)

    live = live_rows(length[0], (turns - 1 - turn) * rows, rows)
    rest = lay.rest(small)
    conv_out = low[...].astype(f32)
    masked = dot(grad[...], out_w[...], NT) * live
    gates = gate[...]
    sigma = jax.nn.sigmoid(gates)
    gate_ref[...] = (
        masked * before_ref[...] * (sigma * (1.0 + gates * (1.0 - sigma)))
    ).astype(bf16)
    out_scan = masked * (gates * sigma)
    scan_grad[...] = out_scan
    bias_ref[1:2] += jnp.sum(out_scan * conv_out, axis=0, keepdims=True)
    mapped = own[...] + got[...].astype(f32)
    to_lanes(lanes, mapped[rank + width :])
    drive[...] = step_ref[...] * conv_out
    rate = -jnp.exp(lay.a_log(small)) * LOG2E
    rate_0, rate_1 = rate[:half], rate[half:]
    rate_low = rate.astype(bf16)
    first = jnp.where(turn == turns - 1, jnp.zeros_like(last_ref[...]), last_ref[...])

    def body(back, carried):
        q_0, q_1, total, h = carried
        block = rows // STEPS - 1 - back
        s = pl.ds(pl.multiple_of(block * STEPS, STEPS), STEPS)
        step_rows[...] = step_ref[s, :]
        drive_rows[...] = drive[s, :]
        grad_rows[...] = scan_grad[s, :]
        part = jnp.zeros((width, chans), bf16)
        for k in reversed(range(STEPS)):
            steps = row_of(step_rows, k, half)
            drives = row_of(drive_rows, k, half)
            outs = row_of(grad_rows, k, half)
            base = pl.multiple_of(block * wide, wide) + k * width
            g_0 = outs * across(lanes[pl.ds(base, half), :], chans) + q_0
            g_1 = outs * across(lanes[pl.ds(base + half, half), :], chans) + q_1
            g = jnp.concatenate([g_0, g_1], 0).astype(bf16)
            grads[pl.ds(base, width), :] = g
            cross_b[pl.ds(base, width), :] = fold(g * twice(drives))
            cross_c[pl.ds(base, width), :] = fold(h * twice(outs))
            q_0 = jnp.exp2(steps * rate_0) * g_0
            q_1 = jnp.exp2(steps * rate_1) * g_1
            if k == 0:
                start = pl.multiple_of(jnp.maximum(base - width, 0), width)
                h = jnp.where(block == 0, first, h_ref[pl.ds(start, width), :])
            else:
                h = h_ref[pl.ds(base - width, width), :]
            term = jnp.concatenate([q_0, q_1], 0).astype(bf16) * h * rate_low
            terms[pl.ds(base, width), :] = term
            part = part + twice(steps) * term
        return q_0, q_1, total + part.astype(f32), h

    start = (carry[:half], carry[half:], rate_ref[...], h_ref[(rows - 1) * width :, :])
    q_0, q_1, total, _ = lax.fori_loop(0, rows // STEPS, body, start)
    carry[:half] = q_0
    carry[half:] = q_1
    rate_ref[...] = total
    ins = spread(mapped[rank : rank + width].astype(bf16))
    ones = (iota((STEPS, wide), 1) // width == iota((STEPS, wide), 0)).astype(bf16)
    weighted, stepped = [], []
    for i in range(rows // STEPS):
        big = slice(i * wide, (i + 1) * wide)
        weighted.append(dot(ins[i * STEPS : (i + 1) * STEPS], grads[big, :]))
        stepped.append(dot(ones, terms[big, :]))
    weighted = jnp.concatenate(weighted, 0)
    step_grad = jnp.concatenate(stepped, 0) * LN2 + conv_out * weighted
    map_low = mapped[:rank].astype(bf16)
    step_pre = dot(map_low, dt_w[...], TN) + rest[taps + 1 : taps + 2]
    pre_grad = (step_grad * live * jax.nn.sigmoid(step_pre)).astype(bf16)
    bias_ref[0:1] += jnp.sum(pre_grad.astype(f32), axis=0, keepdims=True)
    dt_w_ref[...] += dot(map_low, pre_grad)
    map_grad = jnp.concatenate(
        [dot(dt_w[...], pre_grad, NT), lane_sums(cross_b[...], width), lane_sums(cross_c[...], width)],
        0,
    )
    map_ref[...] = map_grad
    send_ref[...] = map_grad.astype(bf16)
    out_ref[...] = out_scan * rest[taps + 2 : taps + 3] + step_ref[...] * weighted


def backward(lay, length, own, got, low, gate, before, step, grad, h, dt_w, small, out_w):
    total, chans = low.shape
    width = lay.width
    turns = total // ROWS
    at = lambda i: turns - 1 - i
    row = lambda w: pl.BlockSpec((ROWS, w), lambda i, *_: (at(i), 0))
    column = lambda w: pl.BlockSpec((w, ROWS), lambda i, *_: (0, at(i)))
    outs = [
        shape((lay.maps, total), f32),
        shape((lay.maps, total), bf16),
        shape((total, chans), f32),
        shape((total, chans), bf16),
        shape((width, chans), f32),
        shape(dt_w.shape, f32),
        shape((8, chans), f32),
    ]
    return pl.pallas_call(
        functools.partial(backward_kernel, lay),
        grid_spec=pltpu.PrefetchScalarGridSpec(
            num_scalar_prefetch=1,
            grid=(turns,),
            in_specs=[
                column(lay.maps),
                column(lay.maps),
                row(chans),
                row(chans),
                row(chans),
                row(chans),
                row(grad.shape[1]),
                pl.BlockSpec((ROWS * width, chans), lambda i, *_: (at(i), 0)),
                pl.BlockSpec((width, chans), lambda i, *_: (jnp.maximum(at(i) * ROWS - 1, 0), 0)),
            ]
            + [full(a) for a in (dt_w, small, out_w)],
            out_specs=[column(lay.maps), column(lay.maps), row(chans), row(chans)]
            + [full(a) for a in outs[4:]],
            scratch_shapes=[
                pltpu.VMEM((width, chans), f32),
                pltpu.VMEM((ROWS * width, chans), bf16),
                pltpu.VMEM((ROWS * width, chans), bf16),
                pltpu.VMEM((ROWS, chans), f32),
                pltpu.VMEM((ROWS, chans), f32),
                pltpu.VMEM((ROWS * width, LANES), f32),
                pltpu.VMEM((ROWS * width, LANES), bf16),
                pltpu.VMEM((ROWS * width, LANES), bf16),
                pltpu.VMEM((STEPS, chans), f32),
                pltpu.VMEM((STEPS, chans), f32),
                pltpu.VMEM((STEPS, chans), f32),
            ],
        ),
        out_shape=outs,
        compiler_params=params(),
        cost_estimate=cost(40),
        name="backward",
    )(length, own, got, low, gate, before, step, grad, h, h, dt_w, small, out_w)


def back_kernel(
    lay, shards, slot, order, own, got, small, out_grad, conv_sum, conv_in, low, gate_grad, normed, w,
    *refs,
):
    token_refs = refs[:shards]
    part_ref, weight_ref, x_ref, conv_ref, gain_ref, halo, total, tokens = refs[shards:]
    rows, chans = low.shape
    taps = lay.taps
    turn = pl.program_id(0)

    @pl.when(turn == 0)
    def _():
        halo[rows:] = jnp.zeros_like(halo[rows:])
        for ref in (total, x_ref, conv_ref, gain_ref):
            ref[...] = jnp.zeros_like(ref)

    for index in range(shards):

        @pl.when(order[shards - 1 - turn] == index)
        def _(index=index):
            tokens[...] = token_refs[index][...].astype(f32)

    rest = lay.rest(small)
    map_grad = (own[...] + got[...].astype(f32)).astype(bf16)
    x_ref[...] += dot(map_grad, low[...])
    values = conv_sum[...]
    sigma = jax.nn.sigmoid(values)
    sum_grad = (out_grad[...] + dot(map_grad, lay.x_w(small), TN)) * (
        sigma * (1.0 + values * (1.0 - sigma))
    )
    conv_ref[taps : taps + 1] += jnp.sum(sum_grad, axis=0, keepdims=True)
    halo[:rows] = sum_grad
    inputs = conv_in[...]
    input_grad = jnp.zeros_like(inputs)
    for tap in range(taps):
        first = taps - 1 - tap
        moved = halo[first : first + rows]
        input_grad = input_grad + rest[tap : tap + 1] * moved
        conv_ref[tap : tap + 1] += jnp.sum(inputs * moved, axis=0, keepdims=True)
    halo[rows:] = sum_grad[:8]
    input_grad = input_grad.astype(bf16)
    total[...] += dot(normed[...], input_grad, TN)
    part = dot(jnp.concatenate([input_grad, gate_grad[...]], 1), w[...], NT)
    part_ref[0] = part.astype(bf16)
    values = tokens[...]
    inverse = lax.rsqrt(jnp.mean(values * values, axis=-1, keepdims=True) + epsilon)
    gain_ref[...] += jnp.sum(part * (values * inverse), axis=0, keepdims=True)

    @pl.when(turn == pl.num_programs(0) - 1)
    def _():
        weight_ref[...] = total[...].astype(bf16)


def back(lay, slot, order, own, got, small, out_grad, conv_sum, conv_in, low, gate_grad, normed, w, tokens):
    chans = low.shape[1]
    count = len(tokens)
    rows, depth = tokens[0].shape
    at = lambda i: count - 1 - i
    row = lambda a: pl.BlockSpec((rows, a.shape[1]), lambda i, *_: (at(i), 0))
    column = lambda a: pl.BlockSpec((a.shape[0], rows), lambda i, *_: (0, at(i)))
    outs = [
        shape((count, rows, depth), bf16),
        shape((depth, chans), bf16),
        shape((lay.maps, chans), f32),
        shape((8, chans), f32),
        shape((1, depth), f32),
    ]
    return pl.pallas_call(
        functools.partial(back_kernel, lay, count),
        grid_spec=pltpu.PrefetchScalarGridSpec(
            num_scalar_prefetch=2,
            grid=(count,),
            in_specs=[
                column(own),
                column(got),
                full(small),
                row(out_grad),
                row(conv_sum),
                row(conv_in),
                row(low),
                row(gate_grad),
                row(normed),
                full(w),
            ]
            + [full(a) for a in tokens],
            out_specs=[pl.BlockSpec((1, rows, depth), lambda i, s, o: (s[at(i)], 0, 0))]
            + [full(a) for a in outs[1:]],
            scratch_shapes=[
                pltpu.VMEM((rows + 8, chans), f32),
                pltpu.VMEM((depth, chans), f32),
                pltpu.VMEM((rows, depth), f32),
            ],
        ),
        out_shape=outs,
        compiler_params=params(),
        cost_estimate=cost(13),
        name="back",
    )(slot, order, own, got, small, out_grad, conv_sum, conv_in, low, gate_grad, normed, w, *tokens)


def exchange(values, axis, size, bits):
    return lax.ppermute(values, axis, [(i, i ^ bits) for i in range(size)])


def relay(values, axis, size, beside):
    me = lax.axis_index(axis)
    up, down = [values], [values]
    for hop in range(1, size):
        pairs = range(hop - 1, size - 1)
        up.append(lax.ppermute(up[-1], axis, [(i, i + 1) for i in pairs]))
        down.append(lax.ppermute(down[-1], axis, [(size - 1 - i, size - 2 - i) for i in pairs]))
        if hop == 1:
            up[1], down[1], beside = lax.optimization_barrier((up[1], down[1], beside))
    return up, down, beside


def chain_terms(sent, axis, size):
    up, down = sent[size - 1], sent[1]
    for hop in range(1, size):
        up = lax.ppermute(up, axis, [(i, i + 1) for i in range(hop)])
        down = lax.ppermute(down, axis, [(size - 1 - i, size - 2 - i) for i in range(hop)])
        if hop < size - 1:
            up = up + sent[size - 1 - hop]
            down = down + sent[hop + 1]
    return [sent[0], up, down]


def gather_pieces(values, axis, size):
    even = [values] + [exchange(values, axis, size, m) for m in range(2, size, 2)]
    odd = [exchange(piece, axis, size, 1) for piece in even]
    return [piece for pair in zip(even, odd) for piece in pair]


def pair_sum(values, axis, size):
    pairs = values.reshape((size // 2, 2) + values.shape[1:])
    core = lax.axis_index(axis) % 2
    keep = lax.dynamic_index_in_dim(pairs, core, 1, False)
    send = lax.dynamic_index_in_dim(pairs, 1 - core, 1, False)
    return keep + exchange(send, axis, size, 1)


def chip_terms(summed, axis, size):
    place = lax.axis_index(axis) // 2
    terms = [lax.dynamic_index_in_dim(summed, place, 0, False)]
    for m in range(1, size // 2):
        piece = lax.dynamic_index_in_dim(summed, place ^ m, 0, False)
        terms.append(exchange(piece, axis, size, 2 * m))
    return terms


def chunk_terms(sent, axis, size):
    return [sent[0]] + [
        lax.ppermute(sent[s], axis, [(i, (i + s) % size) for i in range(size)])
        for s in range(1, size)
    ]


def total(terms):
    return sum(term.astype(f32) for term in terms)


def sum_all(values, send, axis, size):
    bits = 1
    while bits < size:
        got = exchange(send, axis, size, 2 * bits - 1)
        bits *= 2
        if bits < size:
            values = values + got.astype(f32)
            send = values.astype(bf16)
    return values, got


def shards(
    fsdp, tp, tokens, lengths, norm_gain, in_weight, conv_weight, conv_bias, x_weight, dt_weight,
    dt_bias, a_log, d_skip, out_weight, cotangent,
):
    tp_me = lax.axis_index("tp")
    fs_me = lax.axis_index("fsdp")
    chunks = jnp.arange(tp)
    order = ((tp_me - chunks) % tp).astype(jnp.int32)
    slot = ((chunks - tp_me) % tp).astype(jnp.int32)
    place = (fs_me ^ jnp.arange(fsdp)).astype(jnp.int32)
    depth = tokens.shape[2]
    part = conv_weight.shape[1]
    chans = part * fsdp
    lay = Rows(x_weight.shape[1], a_log.shape[0], conv_weight.shape[0])
    maps, width, taps, rank, first = lay.maps, lay.width, lay.taps, lay.rank, lay.first

    pieces = gather_pieces(in_weight.reshape(in_weight.shape[0], 2 * chans), "fsdp", fsdp)
    packed = jnp.concatenate(
        [
            x_weight.T,
            a_log,
            conv_weight,
            conv_bias[None],
            dt_bias[None],
            d_skip[None],
            jnp.zeros((lay.count - first - taps - 3, part), bf16),
            dt_weight.reshape(-1, part),
            norm_gain.reshape(-1, part),
        ],
        0,
    )
    gathered = lax.all_gather(packed, "fsdp", axis=0)
    up, down, gathered = relay(tokens[0], "tp", tp, gathered)
    token_shards = up[:1] + [jnp.where(tp_me >= k, up[k], down[tp - k]) for k in range(1, tp)]
    small = gathered[:, : lay.count].transpose(1, 0, 2).reshape(lay.count, chans)
    dt_rows = dt_weight.size // part
    dt_w = gathered[:, lay.count : lay.count + dt_rows].reshape(rank, chans)
    gain = gathered[:, lay.count + dt_rows :].reshape(1, depth).astype(f32)
    out_w = lax.all_gather(out_weight, "fsdp", axis=1, tiled=True)
    token_shards, held = lax.optimization_barrier((token_shards, cotangent[0]))
    grad_whole = lax.all_gather(held, "tp", axis=0, tiled=True)

    normed, w, conv_in, gate, conv_sum, low, map_part, map_send = front(
        lay, order, place, token_shards, gain, small, pieces
    )
    own, got = sum_all(map_part, map_send, "tp", tp)
    mixed, before, step, h, sent = forward(
        lay, lengths, slot, own, got, low, gate, dt_w, small, out_w
    )
    block_terms = chunk_terms(sent, "tp", tp)
    out_grad = dot(grad_whole, mixed, TN).astype(bf16)

    map_part, map_send, conv_grad, gate_grad, rate_grad, dt_w_grad, bias_grad = backward(
        lay, lengths, own, got, low, gate, before, step, grad_whole, h, dt_w, small, out_w
    )
    map_part, map_send, block_terms[0] = lax.optimization_barrier(
        (map_part, map_send, block_terms[0])
    )
    own_grad, got_grad = sum_all(map_part, map_send, "tp", tp)
    block_out = (tokens.astype(f32) + total(block_terms)[None]).astype(bf16)
    gate_weight = dot(normed, gate_grad, TN).astype(bf16)
    out_terms = chip_terms(pair_sum(out_grad.reshape(fsdp, -1, chans), "fsdp", fsdp), "fsdp", fsdp)
    gate_terms = chip_terms(
        pair_sum(gate_weight.reshape(fsdp, -1, chans), "fsdp", fsdp), "fsdp", fsdp
    )
    own_grad, got_grad, block_out, out_terms, gate_terms = lax.optimization_barrier(
        (own_grad, got_grad, block_out, out_terms, gate_terms)
    )
    sent_back, conv_weight_half, x_w_grad, taps_grad, gain_grad = back(
        lay, slot, order, own_grad, got_grad, small, conv_grad, conv_sum, conv_in, low,
        gate_grad, normed, w, token_shards,
    )
    normed_grad = total(chain_terms(sent_back, "tp", tp))
    conv_pairs = pair_sum(conv_weight_half.reshape(fsdp, -1, chans), "fsdp", fsdp)
    rows = jnp.concatenate(
        [x_w_grad, rate_grad * LN2, taps_grad[: taps + 1], bias_grad[:2]], 0
    ).astype(bf16)
    top = rows.shape[0]
    packed = jnp.concatenate(
        [
            rows.reshape(top, fsdp, part).transpose(1, 0, 2),
            dt_w_grad.astype(bf16).reshape(fsdp, -1, part),
            gain_grad.astype(bf16).reshape(fsdp, -1, part),
        ],
        1,
    )
    small_grad = total(chip_terms(pair_sum(packed, "fsdp", fsdp), "fsdp", fsdp))
    gain_out = small_grad[top + dt_rows :].reshape(-1, 2 * part)
    bits = 1
    while bits < tp:
        gain_out = gain_out + exchange(gain_out, "tp", tp, 2 * bits - 1)
        bits *= 2
    out_weight_grad = total(out_terms).T
    conv_terms = chip_terms(conv_pairs, "fsdp", fsdp)
    in_weight_grad = jnp.stack([total(conv_terms), total(gate_terms)], 1)

    own_values = tokens.astype(f32)
    own_inverse = lax.rsqrt(jnp.mean(own_values * own_values, axis=-1, keepdims=True) + epsilon)
    own_hat = own_values * own_inverse
    scaled = normed_grad[None] * gain[None]
    input_grads = cotangent.astype(f32) + own_inverse * (
        scaled - own_hat * jnp.mean(scaled * own_hat, axis=-1, keepdims=True)
    )
    return (
        block_out,
        input_grads,
        gain_out.reshape(-1),
        in_weight_grad,
        small_grad[first : first + taps],
        small_grad[first + taps],
        small_grad[:maps].T,
        small_grad[top : top + dt_rows].reshape(-1, chans),
        small_grad[first + taps + 1],
        small_grad[maps:first],
        small_grad[first + taps + 2],
        out_weight_grad,
    )


def solution(mesh):
    sizes = dict(mesh.shape)
    return jax.shard_map(
        functools.partial(shards, sizes["fsdp"], sizes["tp"]),
        mesh=mesh,
        in_specs=(
            P("fsdp", "tp", None),
            P("fsdp"),
            P("fsdp"),
            P("fsdp", None, "tp"),
            P(None, ("tp", "fsdp")),
            P(("tp", "fsdp")),
            P(("tp", "fsdp"), None),
            P("fsdp", "tp"),
            P(("tp", "fsdp")),
            P(None, ("tp", "fsdp")),
            P(("tp", "fsdp")),
            P("tp", "fsdp"),
            P("fsdp", "tp", None),
        ),
        out_specs=(
            P("fsdp", "tp", None),
            P("fsdp", "tp", None),
            P("fsdp"),
            P("fsdp", None, "tp"),
            P(None, ("tp", "fsdp")),
            P(("tp", "fsdp")),
            P(("tp", "fsdp"), None),
            P("fsdp", "tp"),
            P(("tp", "fsdp")),
            P(None, ("tp", "fsdp")),
            P(("tp", "fsdp")),
            P("tp", "fsdp"),
        ),
        check_vma=False,
    )
```

```python
import functools

import jax
import jax.numpy as jnp
from jax import lax
from jax.experimental import pallas as pl
from jax.experimental.pallas import tpu as pltpu
from jax.sharding import PartitionSpec as P

bf16 = jnp.bfloat16
f32 = jnp.float32
LOG2E = 1.4426950408889634
LN2 = 0.6931471805599453
ROWS = 128
STEPS = 16
LANES = 128
SCALE = 1.0
NT = (((1,), (1,)), ((), ()))
TN = (((0,), (0,)), ((), ()))
epsilon = 1e-05
VMEM_LIMIT = 56 * 2**20


def dot(a, b, dims=(((1,), (0,)), ((), ()))):
    return lax.dot_general(a, b, dims, preferred_element_type=f32)


def shape(dims, kind):
    return jax.ShapeDtypeStruct(dims, kind)


def iota(dims, axis):
    return lax.broadcasted_iota(jnp.int32, dims, axis)


def params():
    return pltpu.CompilerParams(vmem_limit_bytes=VMEM_LIMIT)


def cost(micros):
    return pl.CostEstimate(
        flops=int(micros * SCALE * 1e9), bytes_accessed=int(micros * SCALE * 3e6), transcendentals=0
    )


def halves(values):
    high = values.astype(bf16)
    return high, (values - high.astype(f32)).astype(bf16)


def spread(columns):
    width, rows = columns.shape
    wide = STEPS * width
    pick = (iota((width, wide), 1) % width == iota((width, wide), 0)).astype(bf16)
    keep = iota((rows, wide), 1) // width == iota((rows, wide), 0) % STEPS
    return jnp.where(keep, dot(columns, pick, TN), 0.0).astype(bf16)


def to_lanes(target, columns):
    width, rows = columns.shape
    wide = STEPS * width
    parts = [spread(part) for part in halves(columns)]
    ones = jnp.ones((2 * STEPS, LANES), bf16)
    for index in range(rows // STEPS):
        s = slice(index * STEPS, (index + 1) * STEPS)
        both = jnp.concatenate([part[s] for part in parts], 0)
        target[index * wide : (index + 1) * wide, :] = dot(both, ones, TN)


def across(values, chans):
    return jnp.concatenate([values] * (chans // LANES), 1)


def row_of(ref, index, count):
    return ref[pl.ds(index, count, stride=0), :]


def twice(values):
    return jnp.concatenate([values, values], 0).astype(bf16)


def fold(values):
    return sum(values[:, i : i + LANES] for i in range(0, values.shape[1], LANES))


def lane_sums(values, width):
    rows = values.shape[0] // width
    sums = dot(values, jnp.ones((LANES, rows), bf16))
    lane = iota((width, rows), 1)
    kept = [jnp.zeros((width, rows), f32)] * 4
    for t in range(rows):
        kept[t % 4] = jnp.where(lane == t, sums[t * width : (t + 1) * width], kept[t % 4])
    return (kept[0] + kept[1]) + (kept[2] + kept[3])


def live_rows(length, first, rows):
    return (iota((rows, 1), 0) + first < length).astype(f32)


def full(array):
    return pl.BlockSpec(array.shape, lambda *_: (0,) * len(array.shape))


class Rows:
    def __init__(self, maps, width, taps):
        self.maps = maps
        self.width = width
        self.taps = taps
        self.rank = maps - 2 * width
        self.first = maps + width
        self.count = -(-(self.first + taps + 3) // 16) * 16

    def x_w(self, ref):
        return ref[: self.maps, :]

    def a_log(self, ref):
        return ref[self.maps : self.first, :].astype(f32)

    def rest(self, ref):
        return ref[self.first :, :].astype(f32)


def front_kernel(lay, shards, pieces, order, place, gain, small, *refs):
    token_refs = refs[:shards]
    piece_refs = refs[shards : shards + pieces]
    (
        normed_ref, w_ref, input_ref, gate_ref, sum_ref, low_ref, map_ref, send_ref, halo, tokens,
    ) = refs[shards + pieces :]
    rows = tokens.shape[0]
    chans = small.shape[1]
    taps = lay.taps
    turn = pl.program_id(0)

    @pl.when(turn == 0)
    def _():
        for index in range(pieces):
            depth = piece_refs[index].shape[0]
            start = pl.multiple_of(place[index] * depth, depth)
            w_ref[pl.ds(start, depth), :] = piece_refs[index][...]
        halo[:8] = jnp.zeros_like(halo[:8])

    for index in range(shards):

        @pl.when(order[turn] == index)
        def _(index=index):
            tokens[...] = token_refs[index][...].astype(f32)

    values = tokens[...]
    inverse = lax.rsqrt(jnp.mean(values * values, axis=-1, keepdims=True) + epsilon)
    normed = (values * inverse * gain[...]).astype(bf16)
    normed_ref[...] = normed
    projected = dot(normed, w_ref[...])
    conv_in = projected[:, :chans]
    input_ref[...] = conv_in
    gate_ref[...] = projected[:, chans:]
    halo[8:] = conv_in
    rest = lay.rest(small)
    total = rest[taps : taps + 1]
    for tap in range(taps):
        first = 8 - taps + 1 + tap
        total = total + rest[tap : tap + 1] * halo[first : first + rows]
    halo[:8] = conv_in[rows - 8 :]
    sum_ref[...] = total
    low = (total * jax.nn.sigmoid(total)).astype(bf16)
    low_ref[...] = low
    mapped = dot(lay.x_w(small), low, NT)
    map_ref[...] = mapped
    send_ref[...] = mapped.astype(bf16)


def front(lay, order, place, shards, gain, small, pieces):
    rows, depth = shards[0].shape
    count = order.shape[0]
    total = count * rows
    chans = small.shape[1]
    row = lambda w: pl.BlockSpec((rows, w), lambda i, *_: (i, 0))
    column = lambda w: pl.BlockSpec((w, rows), lambda i, *_: (0, i))
    both = pieces[0].shape[1]
    return pl.pallas_call(
        functools.partial(front_kernel, lay, len(shards), len(pieces)),
        grid_spec=pltpu.PrefetchScalarGridSpec(
            num_scalar_prefetch=2,
            grid=(count,),
            in_specs=[full(a) for a in (gain, small, *shards, *pieces)],
            out_specs=[
                row(depth),
                pl.BlockSpec((depth, both), lambda i, *_: (0, 0)),
                row(chans),
                row(chans),
                row(chans),
                row(chans),
                column(lay.maps),
                column(lay.maps),
            ],
            scratch_shapes=[pltpu.VMEM((rows + 8, chans), f32), pltpu.VMEM((rows, depth), f32)],
        ),
        out_shape=[
            shape((total, depth), bf16),
            shape((depth, both), bf16),
            shape((total, chans), f32),
            shape((total, chans), f32),
            shape((total, chans), f32),
            shape((total, chans), bf16),
            shape((lay.maps, total), f32),
            shape((lay.maps, total), bf16),
        ],
        compiler_params=params(),
        cost_estimate=cost(9),
        name="front",
    )(order, place, gain, small, *shards, *pieces)


def forward_kernel(
    lay, count, length, slot, own, got, low, gate, dt_w, small, out_w,
    mixed_ref, before_ref, step_ref, h_ref, *refs,
):
    sent_refs = refs[:count]
    state, drive, lanes, step_rows, drive_rows = refs[count:]
    rows, chans = low.shape
    width, rank, taps = lay.width, lay.rank, lay.taps
    half = width // 2
    wide = STEPS * width

    @pl.when(pl.program_id(0) == 0)
    def _():
        state[...] = jnp.zeros_like(state)

    live = live_rows(length[0], pl.program_id(0) * rows, rows)
    mapped = own[...] + got[...].astype(f32)
    rest = lay.rest(small)
    step_pre = dot(mapped[:rank].astype(bf16), dt_w[...], TN) + rest[taps + 1 : taps + 2]
    step = jax.nn.softplus(step_pre) * live
    step_ref[...] = step
    conv_out = low[...].astype(f32)
    drive[...] = step * conv_out
    to_lanes(lanes, mapped[rank : rank + width])
    rate = -jnp.exp(lay.a_log(small)) * LOG2E
    rate_0, rate_1 = rate[:half], rate[half:]

    def body(block, carried):
        h_0, h_1 = carried
        s = pl.ds(pl.multiple_of(block * STEPS, STEPS), STEPS)
        step_rows[...] = step_ref[s, :]
        drive_rows[...] = drive[s, :]
        for k in range(STEPS):
            steps = row_of(step_rows, k, half)
            drives = row_of(drive_rows, k, half)
            base = pl.multiple_of(block * wide, wide) + k * width
            b_0 = across(lanes[pl.ds(base, half), :], chans)
            b_1 = across(lanes[pl.ds(base + half, half), :], chans)
            h_0 = jnp.exp2(steps * rate_0) * h_0 + drives * b_0
            h_1 = jnp.exp2(steps * rate_1) * h_1 + drives * b_1
            h_ref[pl.ds(base, width), :] = jnp.concatenate([h_0, h_1], 0).astype(bf16)
        return h_0, h_1

    h_0, h_1 = lax.fori_loop(0, rows // STEPS, body, (state[:half], state[half:]))
    state[:half] = h_0
    state[half:] = h_1
    outs = spread(mapped[rank + width :].astype(bf16))
    scan = [
        dot(outs[i * STEPS : (i + 1) * STEPS], h_ref[i * wide : (i + 1) * wide, :])
        for i in range(rows // STEPS)
    ]
    before = jnp.concatenate(scan, 0) + rest[taps + 2 : taps + 3] * conv_out
    before_ref[...] = before
    gates = gate[...]
    mixed = (before * (gates * jax.nn.sigmoid(gates)) * live).astype(bf16)
    mixed_ref[...] = mixed
    part = dot(mixed, out_w[...]).astype(bf16)
    blocks = sent_refs[0].shape[0] // rows
    turn = pl.program_id(0)
    for index in range(count):

        @pl.when(slot[turn // blocks] == index)
        def _(index=index):
            sent_refs[index][pl.ds(pl.multiple_of(turn % blocks * rows, rows), rows), :] = part


def forward(lay, length, slot, own, got, low, gate, dt_w, small, out_w):
    total, chans = low.shape
    count = slot.shape[0]
    part = total // count
    depth = out_w.shape[1]
    width = lay.width
    row = lambda w: pl.BlockSpec((ROWS, w), lambda i, *_: (i, 0))
    column = lambda w: pl.BlockSpec((w, ROWS), lambda i, *_: (0, i))
    return pl.pallas_call(
        functools.partial(forward_kernel, lay, count),
        grid_spec=pltpu.PrefetchScalarGridSpec(
            num_scalar_prefetch=2,
            grid=(total // ROWS,),
            in_specs=[column(lay.maps), column(lay.maps), row(chans), row(chans)]
            + [full(a) for a in (dt_w, small, out_w)],
            out_specs=[
                row(chans),
                row(chans),
                row(chans),
                pl.BlockSpec((ROWS * width, chans), lambda i, *_: (i, 0)),
            ]
            + [pl.BlockSpec((part, depth), lambda i, *_: (0, 0))] * count,
            scratch_shapes=[
                pltpu.VMEM((width, chans), f32),
                pltpu.VMEM((ROWS, chans), f32),
                pltpu.VMEM((ROWS * width, LANES), f32),
                pltpu.VMEM((STEPS, chans), f32),
                pltpu.VMEM((STEPS, chans), f32),
            ],
        ),
        out_shape=[
            shape((total, chans), bf16),
            shape((total, chans), f32),
            shape((total, chans), f32),
            shape((total * width, chans), bf16),
        ]
        + [shape((part, depth), bf16)] * count,
        compiler_params=params(),
        cost_estimate=cost(24),
        name="forward",
    )(length, slot, own, got, low, gate, dt_w, small, out_w)


def backward_kernel(
    lay, length, own, got, low, gate, before_ref, step_ref, grad, h_ref, last_ref, dt_w, small, out_w,
    map_ref, send_ref, out_ref, gate_ref, rate_ref, dt_w_ref, bias_ref,
    carry, grads, terms, drive, scan_grad, lanes, cross_b, cross_c, step_rows, drive_rows, grad_rows,
):
    rows, chans = low.shape
    width, rank, taps = lay.width, lay.rank, lay.taps
    half = width // 2
    wide = STEPS * width
    turn = pl.program_id(0)
    turns = pl.num_programs(0)

    @pl.when(turn == 0)
    def _():
        for ref in (carry, rate_ref, dt_w_ref, bias_ref):
            ref[...] = jnp.zeros_like(ref)

    live = live_rows(length[0], (turns - 1 - turn) * rows, rows)
    rest = lay.rest(small)
    conv_out = low[...].astype(f32)
    masked = dot(grad[...], out_w[...], NT) * live
    gates = gate[...]
    sigma = jax.nn.sigmoid(gates)
    gate_ref[...] = (
        masked * before_ref[...] * (sigma * (1.0 + gates * (1.0 - sigma)))
    ).astype(bf16)
    out_scan = masked * (gates * sigma)
    scan_grad[...] = out_scan
    bias_ref[1:2] += jnp.sum(out_scan * conv_out, axis=0, keepdims=True)
    mapped = own[...] + got[...].astype(f32)
    to_lanes(lanes, mapped[rank + width :])
    drive[...] = step_ref[...] * conv_out
    rate = -jnp.exp(lay.a_log(small)) * LOG2E
    rate_0, rate_1 = rate[:half], rate[half:]
    rate_low = rate.astype(bf16)
    first = jnp.where(turn == turns - 1, jnp.zeros_like(last_ref[...]), last_ref[...])

    def body(back, carried):
        q_0, q_1, total, h = carried
        block = rows // STEPS - 1 - back
        s = pl.ds(pl.multiple_of(block * STEPS, STEPS), STEPS)
        step_rows[...] = step_ref[s, :]
        drive_rows[...] = drive[s, :]
        grad_rows[...] = scan_grad[s, :]
        part = jnp.zeros((width, chans), bf16)
        for k in reversed(range(STEPS)):
            steps = row_of(step_rows, k, half)
            drives = row_of(drive_rows, k, half)
            outs = row_of(grad_rows, k, half)
            base = pl.multiple_of(block * wide, wide) + k * width
            g_0 = outs * across(lanes[pl.ds(base, half), :], chans) + q_0
            g_1 = outs * across(lanes[pl.ds(base + half, half), :], chans) + q_1
            g = jnp.concatenate([g_0, g_1], 0).astype(bf16)
            grads[pl.ds(base, width), :] = g
            cross_b[pl.ds(base, width), :] = fold(g * twice(drives))
            cross_c[pl.ds(base, width), :] = fold(h * twice(outs))
            q_0 = jnp.exp2(steps * rate_0) * g_0
            q_1 = jnp.exp2(steps * rate_1) * g_1
            if k == 0:
                start = pl.multiple_of(jnp.maximum(base - width, 0), width)
                h = jnp.where(block == 0, first, h_ref[pl.ds(start, width), :])
            else:
                h = h_ref[pl.ds(base - width, width), :]
            term = jnp.concatenate([q_0, q_1], 0).astype(bf16) * h * rate_low
            terms[pl.ds(base, width), :] = term
            part = part + twice(steps) * term
        return q_0, q_1, total + part.astype(f32), h

    start = (carry[:half], carry[half:], rate_ref[...], h_ref[(rows - 1) * width :, :])
    q_0, q_1, total, _ = lax.fori_loop(0, rows // STEPS, body, start)
    carry[:half] = q_0
    carry[half:] = q_1
    rate_ref[...] = total
    ins = spread(mapped[rank : rank + width].astype(bf16))
    ones = (iota((STEPS, wide), 1) // width == iota((STEPS, wide), 0)).astype(bf16)
    weighted, stepped = [], []
    for i in range(rows // STEPS):
        big = slice(i * wide, (i + 1) * wide)
        weighted.append(dot(ins[i * STEPS : (i + 1) * STEPS], grads[big, :]))
        stepped.append(dot(ones, terms[big, :]))
    weighted = jnp.concatenate(weighted, 0)
    step_grad = jnp.concatenate(stepped, 0) * LN2 + conv_out * weighted
    map_low = mapped[:rank].astype(bf16)
    step_pre = dot(map_low, dt_w[...], TN) + rest[taps + 1 : taps + 2]
    pre_grad = (step_grad * live * jax.nn.sigmoid(step_pre)).astype(bf16)
    bias_ref[0:1] += jnp.sum(pre_grad.astype(f32), axis=0, keepdims=True)
    dt_w_ref[...] += dot(map_low, pre_grad)
    map_grad = jnp.concatenate(
        [dot(dt_w[...], pre_grad, NT), lane_sums(cross_b[...], width), lane_sums(cross_c[...], width)],
        0,
    )
    map_ref[...] = map_grad
    send_ref[...] = map_grad.astype(bf16)
    out_ref[...] = out_scan * rest[taps + 2 : taps + 3] + step_ref[...] * weighted


def backward(lay, length, own, got, low, gate, before, step, grad, h, dt_w, small, out_w):
    total, chans = low.shape
    width = lay.width
    turns = total // ROWS
    at = lambda i: turns - 1 - i
    row = lambda w: pl.BlockSpec((ROWS, w), lambda i, *_: (at(i), 0))
    column = lambda w: pl.BlockSpec((w, ROWS), lambda i, *_: (0, at(i)))
    outs = [
        shape((lay.maps, total), f32),
        shape((lay.maps, total), bf16),
        shape((total, chans), f32),
        shape((total, chans), bf16),
        shape((width, chans), f32),
        shape(dt_w.shape, f32),
        shape((8, chans), f32),
    ]
    return pl.pallas_call(
        functools.partial(backward_kernel, lay),
        grid_spec=pltpu.PrefetchScalarGridSpec(
            num_scalar_prefetch=1,
            grid=(turns,),
            in_specs=[
                column(lay.maps),
                column(lay.maps),
                row(chans),
                row(chans),
                row(chans),
                row(chans),
                row(grad.shape[1]),
                pl.BlockSpec((ROWS * width, chans), lambda i, *_: (at(i), 0)),
                pl.BlockSpec((width, chans), lambda i, *_: (jnp.maximum(at(i) * ROWS - 1, 0), 0)),
            ]
            + [full(a) for a in (dt_w, small, out_w)],
            out_specs=[column(lay.maps), column(lay.maps), row(chans), row(chans)]
            + [full(a) for a in outs[4:]],
            scratch_shapes=[
                pltpu.VMEM((width, chans), f32),
                pltpu.VMEM((ROWS * width, chans), bf16),
                pltpu.VMEM((ROWS * width, chans), bf16),
                pltpu.VMEM((ROWS, chans), f32),
                pltpu.VMEM((ROWS, chans), f32),
                pltpu.VMEM((ROWS * width, LANES), f32),
                pltpu.VMEM((ROWS * width, LANES), bf16),
                pltpu.VMEM((ROWS * width, LANES), bf16),
                pltpu.VMEM((STEPS, chans), f32),
                pltpu.VMEM((STEPS, chans), f32),
                pltpu.VMEM((STEPS, chans), f32),
            ],
        ),
        out_shape=outs,
        compiler_params=params(),
        cost_estimate=cost(40),
        name="backward",
    )(length, own, got, low, gate, before, step, grad, h, h, dt_w, small, out_w)


def back_kernel(
    lay, count, slot, place, own, got, small, out_grad, conv_sum, conv_in, low, gate_grad, normed, w, *refs
):
    part_refs = refs[:count]
    keep_ref, send_ref, x_ref, conv_ref, halo, total = refs[count:]
    rows, chans = low.shape
    taps = lay.taps
    turn = pl.program_id(0)

    @pl.when(turn == 0)
    def _():
        halo[rows:] = jnp.zeros_like(halo[rows:])
        for ref in (total, x_ref, conv_ref):
            ref[...] = jnp.zeros_like(ref)

    rest = lay.rest(small)
    map_grad = (own[...] + got[...].astype(f32)).astype(bf16)
    x_ref[...] += dot(map_grad, low[...])
    values = conv_sum[...]
    sigma = jax.nn.sigmoid(values)
    sum_grad = (out_grad[...] + dot(map_grad, lay.x_w(small), TN)) * (
        sigma * (1.0 + values * (1.0 - sigma))
    )
    conv_ref[taps : taps + 1] += jnp.sum(sum_grad, axis=0, keepdims=True)
    halo[:rows] = sum_grad
    inputs = conv_in[...]
    input_grad = jnp.zeros_like(inputs)
    for tap in range(taps):
        first = taps - 1 - tap
        moved = halo[first : first + rows]
        input_grad = input_grad + rest[tap : tap + 1] * moved
        conv_ref[tap : tap + 1] += jnp.sum(inputs * moved, axis=0, keepdims=True)
    halo[rows:] = sum_grad[:8]
    input_grad = input_grad.astype(bf16)
    total[...] += dot(normed[...], input_grad, TN)
    part = dot(jnp.concatenate([input_grad, gate_grad[...]], 1), w[...], NT)
    for index in range(count):

        @pl.when(slot[pl.num_programs(0) - 1 - turn] == index)
        def _(index=index):
            part_refs[index][...] = part.astype(bf16)

    @pl.when(turn == pl.num_programs(0) - 1)
    def _():
        depth = keep_ref.shape[1]
        for index in range(2 * keep_ref.shape[0]):
            start = pl.multiple_of(place[index] * depth, depth)
            values = total[pl.ds(start, depth), :].astype(bf16)
            (send_ref if index % 2 else keep_ref)[index // 2] = values


def back(lay, slot, place, own, got, small, out_grad, conv_sum, conv_in, low, gate_grad, normed, w):
    chans = low.shape[1]
    count = slot.shape[0]
    total, depth = normed.shape
    rows = total // count
    at = lambda i: count - 1 - i
    row = lambda a: pl.BlockSpec((rows, a.shape[1]), lambda i, *_: (at(i), 0))
    column = lambda a: pl.BlockSpec((a.shape[0], rows), lambda i, *_: (0, at(i)))
    half = place.shape[0] // 2
    outs = [shape((rows, depth), bf16)] * count + [
        shape((half, depth // half // 2, chans), bf16),
        shape((half, depth // half // 2, chans), bf16),
        shape((lay.maps, chans), f32),
        shape((8, chans), f32),
    ]
    return pl.pallas_call(
        functools.partial(back_kernel, lay, count),
        grid_spec=pltpu.PrefetchScalarGridSpec(
            num_scalar_prefetch=2,
            grid=(count,),
            in_specs=[
                column(own),
                column(got),
                full(small),
                row(out_grad),
                row(conv_sum),
                row(conv_in),
                row(low),
                row(gate_grad),
                row(normed),
                full(w),
            ],
            out_specs=[full(a) for a in outs],
            scratch_shapes=[pltpu.VMEM((rows + 8, chans), f32), pltpu.VMEM((depth, chans), f32)],
        ),
        out_shape=outs,
        compiler_params=params(),
        cost_estimate=cost(11),
        name="back",
    )(slot, place, own, got, small, out_grad, conv_sum, conv_in, low, gate_grad, normed, w)


def exchange(values, axis, size, bits):
    return lax.ppermute(values, axis, [(i, i ^ bits) for i in range(size)])


def relay(values, axis, size, beside):
    up, down = [values], [values]
    beside = list(beside)
    for hop in range(1, size):
        pairs = range(hop - 1, size - 1)
        up.append(lax.ppermute(up[-1], axis, [(i, i + 1) for i in pairs]))
        down.append(lax.ppermute(down[-1], axis, [(size - 1 - i, size - 2 - i) for i in pairs]))
        if hop <= len(beside):
            up[-1], down[-1], beside[hop - 1] = lax.optimization_barrier(
                (up[-1], down[-1], beside[hop - 1])
            )
    return up, down, beside


def chain_terms(sent, axis, size, after):
    up, down = sent[size - 1], sent[1]
    for hop in range(1, size):
        up = lax.ppermute(up, axis, [(i, i + 1) for i in range(hop)])
        down = lax.ppermute(down, axis, [(size - 1 - i, size - 2 - i) for i in range(hop)])
        if hop == size - 2:
            up, down, after = lax.optimization_barrier((up, down, after))
        if hop < size - 1:
            up = up + sent[size - 1 - hop]
            down = down + sent[hop + 1]
    return [sent[0], up, down], after


def even_pieces(values, axis, size):
    return [values] + [exchange(values, axis, size, m) for m in range(2, size, 2)]


def all_pieces(even, axis, size):
    odd = [exchange(piece, axis, size, 1) for piece in even]
    return [piece for pair in zip(even, odd) for piece in pair]


def pair_sum(keep, send, axis, size):
    return keep + exchange(send, axis, size, 1)


def chip_terms(summed, axis, size):
    return [summed[0]] + [exchange(summed[m], axis, size, 2 * m) for m in range(1, size // 2)]


def chunk_terms(sent, axis, size):
    return [sent[0]] + [
        lax.ppermute(sent[s], axis, [(i, (i + s) % size) for i in range(size)])
        for s in range(1, size)
    ]


def total(terms):
    return sum(term.astype(f32) for term in terms)


def sum_all(values, send, axis, size, beside):
    bits = 1
    while bits < size:
        got = exchange(send, axis, size, 2 * bits - 1)
        if bits == 1:
            got, beside = lax.optimization_barrier((got, beside))
        bits *= 2
        if bits < size:
            values = values + got.astype(f32)
            send = values.astype(bf16)
    return values, got, beside


def shards(
    fsdp, tp, tokens, lengths, norm_gain, in_weight, conv_weight, conv_bias, x_weight, dt_weight,
    dt_bias, a_log, d_skip, out_weight, cotangent,
):
    tp_me = lax.axis_index("tp")
    fs_me = lax.axis_index("fsdp")
    chunks = jnp.arange(tp)
    order = ((tp_me - chunks) % tp).astype(jnp.int32)
    slot = ((chunks - tp_me) % tp).astype(jnp.int32)
    place = (fs_me ^ jnp.arange(fsdp)).astype(jnp.int32)
    depth = tokens.shape[2]
    part = conv_weight.shape[1]
    chans = part * fsdp
    lay = Rows(x_weight.shape[1], a_log.shape[0], conv_weight.shape[0])
    maps, width, taps, rank, first = lay.maps, lay.width, lay.taps, lay.rank, lay.first

    even = even_pieces(in_weight.reshape(in_weight.shape[0], 2 * chans), "fsdp", fsdp)
    packed = jnp.concatenate(
        [
            x_weight.T,
            a_log,
            conv_weight,
            conv_bias[None],
            dt_bias[None],
            d_skip[None],
            jnp.zeros((lay.count - first - taps - 3, part), bf16),
            dt_weight.reshape(-1, part),
            norm_gain.reshape(-1, part),
        ],
        0,
    )
    gathered = lax.all_gather(packed, "fsdp", axis=0)
    up, down, (gathered, even) = relay(tokens[0], "tp", tp, (gathered, even))
    pieces = all_pieces(even, "fsdp", fsdp)
    token_shards = up + down[1:]
    source = jnp.where(chunks <= tp_me, tp_me - chunks, chunks - tp_me + tp - 1).astype(jnp.int32)
    small = gathered[:, : lay.count].transpose(1, 0, 2).reshape(lay.count, chans)
    dt_rows = dt_weight.size // part
    dt_w = gathered[:, lay.count : lay.count + dt_rows].reshape(rank, chans)
    gain = gathered[:, lay.count + dt_rows :].reshape(1, depth).astype(f32)
    out_w = lax.all_gather(out_weight, "fsdp", axis=1, tiled=True)

    normed, w, conv_in, gate, conv_sum, low, map_part, map_send = front(
        lay, source, place, token_shards, gain, small, pieces
    )
    map_send, held = lax.optimization_barrier((map_send, cotangent[0]))
    grad_whole = lax.all_gather(held, "tp", axis=0, tiled=True)
    own, got, _ = sum_all(map_part, map_send, "tp", tp, ())
    mixed, before, step, h, *sent = forward(
        lay, lengths, slot, own, got, low, gate, dt_w, small, out_w
    )
    sent, grad_whole = lax.optimization_barrier((sent, grad_whole))
    block_terms = chunk_terms(sent, "tp", tp)

    map_part, map_send, conv_grad, gate_grad, rate_grad, dt_w_grad, bias_grad = backward(
        lay, lengths, own, got, low, gate, before, step, grad_whole, h, dt_w, small, out_w
    )
    map_part, map_send, block_terms = lax.optimization_barrier((map_part, map_send, block_terms))
    own_grad, got_grad, held = sum_all(map_part, map_send, "tp", tp, gate_grad)
    pair = [
        dot(a, b, TN).reshape(fsdp, 1, -1, chans)
        for a, b in ((normed, held), (grad_whole, mixed))
    ]
    gate_half, out_weight_grad = lax.psum_scatter(
        jnp.concatenate(pair, 1).astype(bf16), "fsdp", scatter_dimension=0, tiled=False
    )
    block_out = (tokens.astype(f32) + total(block_terms)[None]).astype(bf16)
    own_grad, got_grad, block_out = lax.optimization_barrier((own_grad, got_grad, block_out))
    *sent_back, keep, send, x_w_grad, taps_grad = back(
        lay, slot, place, own_grad, got_grad, small, conv_grad, conv_sum, conv_in, low,
        gate_grad, normed, w,
    )
    conv_half = total(chip_terms(pair_sum(keep, send, "fsdp", fsdp), "fsdp", fsdp))
    rows = jnp.concatenate(
        [x_w_grad, rate_grad * LN2, taps_grad[: taps + 1], bias_grad[:2]], 0
    ).astype(bf16)
    top = rows.shape[0]
    packed = jnp.concatenate(
        [
            rows.reshape(top, fsdp, part).transpose(1, 0, 2),
            dt_w_grad.astype(bf16).reshape(fsdp, -1, part),
        ],
        1,
    )[place]
    pairs = pair_sum(packed[0::2], packed[1::2], "fsdp", fsdp)
    small_grad = total(chip_terms(pairs, "fsdp", fsdp))
    chain, (small_grad, gate_half, out_weight_grad) = chain_terms(
        sent_back, "tp", tp, (small_grad, gate_half, out_weight_grad)
    )
    normed_grad = total(chain)
    in_weight_grad = jnp.stack([conv_half, gate_half.astype(f32)], 1)
    out_weight_grad = out_weight_grad.astype(f32).T
    gain_out = jnp.sum(in_weight_grad * in_weight.astype(f32), axis=(1, 2), keepdims=True)
    gain_out = (gain_out[:, 0] / norm_gain.astype(f32)[:, None]).reshape(1, -1)
    bits = 1
    while bits < tp:
        gain_out = gain_out + exchange(gain_out, "tp", tp, 2 * bits - 1)
        bits *= 2

    own_values = tokens.astype(f32)
    own_inverse = lax.rsqrt(jnp.mean(own_values * own_values, axis=-1, keepdims=True) + epsilon)
    own_hat = own_values * own_inverse
    scaled = normed_grad[None] * gain[None]
    input_grads = cotangent.astype(f32) + own_inverse * (
        scaled - own_hat * jnp.mean(scaled * own_hat, axis=-1, keepdims=True)
    )
    return (
        block_out,
        input_grads,
        gain_out.reshape(-1),
        in_weight_grad,
        small_grad[first : first + taps],
        small_grad[first + taps],
        small_grad[:maps].T,
        small_grad[top : top + dt_rows].reshape(-1, chans),
        small_grad[first + taps + 1],
        small_grad[maps:first],
        small_grad[first + taps + 2],
        out_weight_grad,
    )


def solution(mesh):
    sizes = dict(mesh.shape)
    return jax.shard_map(
        functools.partial(shards, sizes["fsdp"], sizes["tp"]),
        mesh=mesh,
        in_specs=(
            P("fsdp", "tp", None),
            P("fsdp"),
            P("fsdp"),
            P("fsdp", None, "tp"),
            P(None, ("tp", "fsdp")),
            P(("tp", "fsdp")),
            P(("tp", "fsdp"), None),
            P("fsdp", "tp"),
            P(("tp", "fsdp")),
            P(None, ("tp", "fsdp")),
            P(("tp", "fsdp")),
            P("tp", "fsdp"),
            P("fsdp", "tp", None),
        ),
        out_specs=(
            P("fsdp", "tp", None),
            P("fsdp", "tp", None),
            P("fsdp"),
            P("fsdp", None, "tp"),
            P(None, ("tp", "fsdp")),
            P(("tp", "fsdp")),
            P(("tp", "fsdp"), None),
            P("fsdp", "tp"),
            P(("tp", "fsdp")),
            P(None, ("tp", "fsdp")),
            P(("tp", "fsdp")),
            P("tp", "fsdp"),
        ),
        check_vma=False,
    )
```

```python
import functools

import jax
import jax.numpy as jnp
from jax import lax
from jax.experimental import pallas as pl
from jax.experimental.pallas import tpu as pltpu
from jax.sharding import PartitionSpec as P

bf16 = jnp.bfloat16
f32 = jnp.float32
LOG2E = 1.4426950408889634
LN2 = 0.6931471805599453
ROWS = 128
STEPS = 16
LANES = 128
SCALE = 1.0
NT = (((1,), (1,)), ((), ()))
TN = (((0,), (0,)), ((), ()))
epsilon = 1e-05
VMEM_LIMIT = 56 * 2**20


def dot(a, b, dims=(((1,), (0,)), ((), ()))):
    return lax.dot_general(a, b, dims, preferred_element_type=f32)


def shape(dims, kind):
    return jax.ShapeDtypeStruct(dims, kind)


def iota(dims, axis):
    return lax.broadcasted_iota(jnp.int32, dims, axis)


def params():
    return pltpu.CompilerParams(vmem_limit_bytes=VMEM_LIMIT)


def cost(micros):
    return pl.CostEstimate(
        flops=int(micros * SCALE * 1e9), bytes_accessed=int(micros * SCALE * 3e6), transcendentals=0
    )


def halves(values):
    high = values.astype(bf16)
    return high, (values - high.astype(f32)).astype(bf16)


def spread(columns):
    width, rows = columns.shape
    wide = STEPS * width
    pick = (iota((width, wide), 1) % width == iota((width, wide), 0)).astype(bf16)
    keep = iota((rows, wide), 1) // width == iota((rows, wide), 0) % STEPS
    return jnp.where(keep, dot(columns, pick, TN), 0.0).astype(bf16)


def to_lanes(target, columns):
    width, rows = columns.shape
    wide = STEPS * width
    parts = [spread(part) for part in halves(columns)]
    ones = jnp.ones((2 * STEPS, LANES), bf16)
    for index in range(rows // STEPS):
        s = slice(index * STEPS, (index + 1) * STEPS)
        both = jnp.concatenate([part[s] for part in parts], 0)
        target[index * wide : (index + 1) * wide, :] = dot(both, ones, TN)


def across(values, chans):
    return jnp.concatenate([values] * (chans // LANES), 1)


def row_of(ref, index, count):
    return ref[pl.ds(index, count, stride=0), :]


def twice(values):
    return jnp.concatenate([values, values], 0).astype(bf16)


def fold(values):
    return sum(values[:, i : i + LANES] for i in range(0, values.shape[1], LANES))


def lane_sums(values, width):
    rows = values.shape[0] // width
    sums = dot(values, jnp.ones((LANES, rows), bf16))
    lane = iota((width, rows), 1)
    kept = [jnp.zeros((width, rows), f32)] * 4
    for t in range(rows):
        kept[t % 4] = jnp.where(lane == t, sums[t * width : (t + 1) * width], kept[t % 4])
    return (kept[0] + kept[1]) + (kept[2] + kept[3])


def live_rows(length, first, rows):
    return (iota((rows, 1), 0) + first < length).astype(f32)


def full(array):
    return pl.BlockSpec(array.shape, lambda *_: (0,) * len(array.shape))


class Rows:
    def __init__(self, maps, width, taps):
        self.maps = maps
        self.width = width
        self.taps = taps
        self.rank = maps - 2 * width
        self.first = maps + width
        self.count = -(-(self.first + taps + 3) // 16) * 16

    def x_w(self, ref):
        return ref[: self.maps, :]

    def a_log(self, ref):
        return ref[self.maps : self.first, :].astype(f32)

    def rest(self, ref):
        return ref[self.first :, :].astype(f32)


def front_kernel(
    lay, tokens, gain, small, w,
    normed_ref, input_ref, gate_ref, sum_ref, low_ref, map_ref, send_ref, halo,
):
    rows = tokens.shape[0]
    chans = small.shape[1]
    taps = lay.taps

    @pl.when(pl.program_id(0) == 0)
    def _():
        halo[:8] = jnp.zeros_like(halo[:8])

    values = tokens[...].astype(f32)
    inverse = lax.rsqrt(jnp.mean(values * values, axis=-1, keepdims=True) + epsilon)
    normed = (values * inverse * gain[...]).astype(bf16)
    normed_ref[...] = normed
    projected = dot(normed, w[...])
    conv_in = projected[:, :chans]
    input_ref[...] = conv_in
    gate_ref[...] = projected[:, chans:]
    halo[8:] = conv_in
    rest = lay.rest(small)
    total = rest[taps : taps + 1]
    for tap in range(taps):
        first = 8 - taps + 1 + tap
        total = total + rest[tap : tap + 1] * halo[first : first + rows]
    halo[:8] = conv_in[rows - 8 :]
    sum_ref[...] = total
    low = (total * jax.nn.sigmoid(total)).astype(bf16)
    low_ref[...] = low
    mapped = dot(lay.x_w(small), low, NT)
    map_ref[...] = mapped
    send_ref[...] = mapped.astype(bf16)


def front(lay, tokens, gain, small, w):
    total, depth = tokens.shape
    rows = 256
    chans = small.shape[1]
    row = lambda w: pl.BlockSpec((rows, w), lambda i: (i, 0))
    column = lambda w: pl.BlockSpec((w, rows), lambda i: (0, i))
    return pl.pallas_call(
        functools.partial(front_kernel, lay),
        grid=(total // rows,),
        in_specs=[row(depth)] + [full(a) for a in (gain, small, w)],
        out_specs=[row(depth)] + [row(chans)] * 4 + [column(lay.maps)] * 2,
        out_shape=[
            shape((total, depth), bf16),
            shape((total, chans), f32),
            shape((total, chans), f32),
            shape((total, chans), f32),
            shape((total, chans), bf16),
            shape((lay.maps, total), f32),
            shape((lay.maps, total), bf16),
        ],
        scratch_shapes=[pltpu.VMEM((rows + 8, chans), f32)],
        compiler_params=params(),
        cost_estimate=cost(9),
        name="front",
    )(tokens, gain, small, w)


def forward_kernel(
    lay, length, own, got, low, gate, dt_w, small, out_w,
    mixed_ref, before_ref, step_ref, h_ref, sent_ref, state, drive, lanes, step_rows, drive_rows,
):
    rows, chans = low.shape
    width, rank, taps = lay.width, lay.rank, lay.taps
    half = width // 2
    wide = STEPS * width

    @pl.when(pl.program_id(0) == 0)
    def _():
        state[...] = jnp.zeros_like(state)

    live = live_rows(length[0], pl.program_id(0) * rows, rows)
    mapped = own[...] + got[...].astype(f32)
    rest = lay.rest(small)
    step_pre = dot(mapped[:rank].astype(bf16), dt_w[...], TN) + rest[taps + 1 : taps + 2]
    step = jax.nn.softplus(step_pre) * live
    step_ref[...] = step
    conv_out = low[...].astype(f32)
    drive[...] = step * conv_out
    to_lanes(lanes, mapped[rank : rank + width])
    rate = -jnp.exp(lay.a_log(small)) * LOG2E
    rate_0, rate_1 = rate[:half], rate[half:]

    def body(block, carried):
        h_0, h_1 = carried
        s = pl.ds(pl.multiple_of(block * STEPS, STEPS), STEPS)
        step_rows[...] = step_ref[s, :]
        drive_rows[...] = drive[s, :]
        for k in range(STEPS):
            steps = row_of(step_rows, k, half)
            drives = row_of(drive_rows, k, half)
            base = pl.multiple_of(block * wide, wide) + k * width
            b_0 = across(lanes[pl.ds(base, half), :], chans)
            b_1 = across(lanes[pl.ds(base + half, half), :], chans)
            h_0 = jnp.exp2(steps * rate_0) * h_0 + drives * b_0
            h_1 = jnp.exp2(steps * rate_1) * h_1 + drives * b_1
            h_ref[pl.ds(base, width), :] = jnp.concatenate([h_0, h_1], 0).astype(bf16)
        return h_0, h_1

    h_0, h_1 = lax.fori_loop(0, rows // STEPS, body, (state[:half], state[half:]))
    state[:half] = h_0
    state[half:] = h_1
    outs = spread(mapped[rank + width :].astype(bf16))
    scan = [
        dot(outs[i * STEPS : (i + 1) * STEPS], h_ref[i * wide : (i + 1) * wide, :])
        for i in range(rows // STEPS)
    ]
    before = jnp.concatenate(scan, 0) + rest[taps + 2 : taps + 3] * conv_out
    before_ref[...] = before
    gates = gate[...]
    mixed = (before * (gates * jax.nn.sigmoid(gates)) * live).astype(bf16)
    mixed_ref[...] = mixed
    sent_ref[...] = dot(mixed, out_w[...]).astype(bf16)


def forward(lay, length, own, got, low, gate, dt_w, small, out_w):
    total, chans = low.shape
    depth = out_w.shape[1]
    width = lay.width
    row = lambda w: pl.BlockSpec((ROWS, w), lambda i, *_: (i, 0))
    column = lambda w: pl.BlockSpec((w, ROWS), lambda i, *_: (0, i))
    return pl.pallas_call(
        functools.partial(forward_kernel, lay),
        grid_spec=pltpu.PrefetchScalarGridSpec(
            num_scalar_prefetch=1,
            grid=(total // ROWS,),
            in_specs=[column(lay.maps), column(lay.maps), row(chans), row(chans)]
            + [full(a) for a in (dt_w, small, out_w)],
            out_specs=[
                row(chans),
                row(chans),
                row(chans),
                pl.BlockSpec((ROWS * width, chans), lambda i, *_: (i, 0)),
                row(depth),
            ],
            scratch_shapes=[
                pltpu.VMEM((width, chans), f32),
                pltpu.VMEM((ROWS, chans), f32),
                pltpu.VMEM((ROWS * width, LANES), f32),
                pltpu.VMEM((STEPS, chans), f32),
                pltpu.VMEM((STEPS, chans), f32),
            ],
        ),
        out_shape=[
            shape((total, chans), bf16),
            shape((total, chans), f32),
            shape((total, chans), f32),
            shape((total * width, chans), bf16),
            shape((total, depth), bf16),
        ],
        compiler_params=params(),
        cost_estimate=cost(24),
        name="forward",
    )(length, own, got, low, gate, dt_w, small, out_w)


def backward_kernel(
    lay, length, own, got, low, gate, before_ref, step_ref, grad, h_ref, last_ref, dt_w, small, out_w,
    map_ref, send_ref, out_ref, gate_ref, rate_ref, dt_w_ref, bias_ref,
    carry, grads, terms, drive, scan_grad, lanes, cross_b, cross_c, step_rows, drive_rows, grad_rows,
):
    rows, chans = low.shape
    width, rank, taps = lay.width, lay.rank, lay.taps
    half = width // 2
    wide = STEPS * width
    turn = pl.program_id(0)
    turns = pl.num_programs(0)

    @pl.when(turn == 0)
    def _():
        for ref in (carry, rate_ref, dt_w_ref, bias_ref):
            ref[...] = jnp.zeros_like(ref)

    live = live_rows(length[0], (turns - 1 - turn) * rows, rows)
    rest = lay.rest(small)
    conv_out = low[...].astype(f32)
    masked = dot(grad[...], out_w[...], NT) * live
    gates = gate[...]
    sigma = jax.nn.sigmoid(gates)
    gate_ref[...] = (
        masked * before_ref[...] * (sigma * (1.0 + gates * (1.0 - sigma)))
    ).astype(bf16)
    out_scan = masked * (gates * sigma)
    scan_grad[...] = out_scan
    bias_ref[1:2] += jnp.sum(out_scan * conv_out, axis=0, keepdims=True)
    mapped = own[...] + got[...].astype(f32)
    to_lanes(lanes, mapped[rank + width :])
    drive[...] = step_ref[...] * conv_out
    rate = -jnp.exp(lay.a_log(small)) * LOG2E
    rate_0, rate_1 = rate[:half], rate[half:]
    rate_low = rate.astype(bf16)
    first = jnp.where(turn == turns - 1, jnp.zeros_like(last_ref[...]), last_ref[...])

    def body(back, carried):
        q_0, q_1, total, h = carried
        block = rows // STEPS - 1 - back
        s = pl.ds(pl.multiple_of(block * STEPS, STEPS), STEPS)
        step_rows[...] = step_ref[s, :]
        drive_rows[...] = drive[s, :]
        grad_rows[...] = scan_grad[s, :]
        part = jnp.zeros((width, chans), bf16)
        for k in reversed(range(STEPS)):
            steps = row_of(step_rows, k, half)
            drives = row_of(drive_rows, k, half)
            outs = row_of(grad_rows, k, half)
            base = pl.multiple_of(block * wide, wide) + k * width
            g_0 = outs * across(lanes[pl.ds(base, half), :], chans) + q_0
            g_1 = outs * across(lanes[pl.ds(base + half, half), :], chans) + q_1
            g = jnp.concatenate([g_0, g_1], 0).astype(bf16)
            grads[pl.ds(base, width), :] = g
            cross_b[pl.ds(base, width), :] = fold(g * twice(drives))
            cross_c[pl.ds(base, width), :] = fold(h * twice(outs))
            q_0 = jnp.exp2(steps * rate_0) * g_0
            q_1 = jnp.exp2(steps * rate_1) * g_1
            if k == 0:
                start = pl.multiple_of(jnp.maximum(base - width, 0), width)
                h = jnp.where(block == 0, first, h_ref[pl.ds(start, width), :])
            else:
                h = h_ref[pl.ds(base - width, width), :]
            term = jnp.concatenate([q_0, q_1], 0).astype(bf16) * h * rate_low
            terms[pl.ds(base, width), :] = term
            part = part + twice(steps) * term
        return q_0, q_1, total + part.astype(f32), h

    start = (carry[:half], carry[half:], rate_ref[...], h_ref[(rows - 1) * width :, :])
    q_0, q_1, total, _ = lax.fori_loop(0, rows // STEPS, body, start)
    carry[:half] = q_0
    carry[half:] = q_1
    rate_ref[...] = total
    ins = spread(mapped[rank : rank + width].astype(bf16))
    ones = (iota((STEPS, wide), 1) // width == iota((STEPS, wide), 0)).astype(bf16)
    weighted, stepped = [], []
    for i in range(rows // STEPS):
        big = slice(i * wide, (i + 1) * wide)
        weighted.append(dot(ins[i * STEPS : (i + 1) * STEPS], grads[big, :]))
        stepped.append(dot(ones, terms[big, :]))
    weighted = jnp.concatenate(weighted, 0)
    step_grad = jnp.concatenate(stepped, 0) * LN2 + conv_out * weighted
    map_low = mapped[:rank].astype(bf16)
    step_pre = dot(map_low, dt_w[...], TN) + rest[taps + 1 : taps + 2]
    pre_grad = (step_grad * live * jax.nn.sigmoid(step_pre)).astype(bf16)
    bias_ref[0:1] += jnp.sum(pre_grad.astype(f32), axis=0, keepdims=True)
    dt_w_ref[...] += dot(map_low, pre_grad)
    map_grad = jnp.concatenate(
        [dot(dt_w[...], pre_grad, NT), lane_sums(cross_b[...], width), lane_sums(cross_c[...], width)],
        0,
    )
    map_ref[...] = map_grad
    send_ref[...] = map_grad.astype(bf16)
    out_ref[...] = out_scan * rest[taps + 2 : taps + 3] + step_ref[...] * weighted


def backward(lay, length, own, got, low, gate, before, step, grad, h, dt_w, small, out_w):
    total, chans = low.shape
    width = lay.width
    turns = total // ROWS
    at = lambda i: turns - 1 - i
    row = lambda w: pl.BlockSpec((ROWS, w), lambda i, *_: (at(i), 0))
    column = lambda w: pl.BlockSpec((w, ROWS), lambda i, *_: (0, at(i)))
    outs = [
        shape((lay.maps, total), f32),
        shape((lay.maps, total), bf16),
        shape((total, chans), f32),
        shape((total, chans), bf16),
        shape((width, chans), f32),
        shape(dt_w.shape, f32),
        shape((8, chans), f32),
    ]
    return pl.pallas_call(
        functools.partial(backward_kernel, lay),
        grid_spec=pltpu.PrefetchScalarGridSpec(
            num_scalar_prefetch=1,
            grid=(turns,),
            in_specs=[
                column(lay.maps),
                column(lay.maps),
                row(chans),
                row(chans),
                row(chans),
                row(chans),
                row(grad.shape[1]),
                pl.BlockSpec((ROWS * width, chans), lambda i, *_: (at(i), 0)),
                pl.BlockSpec((width, chans), lambda i, *_: (jnp.maximum(at(i) * ROWS - 1, 0), 0)),
            ]
            + [full(a) for a in (dt_w, small, out_w)],
            out_specs=[column(lay.maps), column(lay.maps), row(chans), row(chans)]
            + [full(a) for a in outs[4:]],
            scratch_shapes=[
                pltpu.VMEM((width, chans), f32),
                pltpu.VMEM((ROWS * width, chans), bf16),
                pltpu.VMEM((ROWS * width, chans), bf16),
                pltpu.VMEM((ROWS, chans), f32),
                pltpu.VMEM((ROWS, chans), f32),
                pltpu.VMEM((ROWS * width, LANES), f32),
                pltpu.VMEM((ROWS * width, LANES), bf16),
                pltpu.VMEM((ROWS * width, LANES), bf16),
                pltpu.VMEM((STEPS, chans), f32),
                pltpu.VMEM((STEPS, chans), f32),
                pltpu.VMEM((STEPS, chans), f32),
            ],
        ),
        out_shape=outs,
        compiler_params=params(),
        cost_estimate=cost(40),
        name="backward",
    )(length, own, got, low, gate, before, step, grad, h, h, dt_w, small, out_w)


def back_kernel(
    lay, own, got, small, out_grad, conv_sum, conv_in, low, gate_grad, w,
    part_ref, input_ref, x_ref, conv_ref, halo,
):
    rows, chans = low.shape
    taps = lay.taps
    turn = pl.program_id(0)

    @pl.when(turn == 0)
    def _():
        halo[rows:] = jnp.zeros_like(halo[rows:])
        for ref in (x_ref, conv_ref):
            ref[...] = jnp.zeros_like(ref)

    rest = lay.rest(small)
    map_grad = (own[...] + got[...].astype(f32)).astype(bf16)
    x_ref[...] += dot(map_grad, low[...])
    values = conv_sum[...]
    sigma = jax.nn.sigmoid(values)
    sum_grad = (out_grad[...] + dot(map_grad, lay.x_w(small), TN)) * (
        sigma * (1.0 + values * (1.0 - sigma))
    )
    conv_ref[taps : taps + 1] += jnp.sum(sum_grad, axis=0, keepdims=True)
    halo[:rows] = sum_grad
    inputs = conv_in[...]
    input_grad = jnp.zeros_like(inputs)
    for tap in range(taps):
        first = taps - 1 - tap
        moved = halo[first : first + rows]
        input_grad = input_grad + rest[tap : tap + 1] * moved
        conv_ref[tap : tap + 1] += jnp.sum(inputs * moved, axis=0, keepdims=True)
    halo[rows:] = sum_grad[:8]
    input_grad = input_grad.astype(bf16)
    input_ref[...] = input_grad
    part = dot(jnp.concatenate([input_grad, gate_grad[...]], 1), w[...], NT)
    part_ref[...] = part.astype(bf16)


def back(lay, own, got, small, out_grad, conv_sum, conv_in, low, gate_grad, w):
    total, chans = low.shape
    depth = w.shape[0]
    rows = 256
    count = total // rows
    at = lambda i: count - 1 - i
    row = lambda a: pl.BlockSpec((rows, a.shape[1]), lambda i: (at(i), 0))
    column = lambda a: pl.BlockSpec((a.shape[0], rows), lambda i: (0, at(i)))
    outs = [
        shape((total, depth), bf16),
        shape((total, chans), bf16),
        shape((lay.maps, chans), f32),
        shape((8, chans), f32),
    ]
    return pl.pallas_call(
        functools.partial(back_kernel, lay),
        grid=(count,),
        in_specs=[
            column(own),
            column(got),
            full(small),
            row(out_grad),
            row(conv_sum),
            row(conv_in),
            row(low),
            row(gate_grad),
            full(w),
        ],
        out_specs=[row(outs[0]), row(outs[1]), full(outs[2]), full(outs[3])],
        out_shape=outs,
        scratch_shapes=[pltpu.VMEM((rows + 8, chans), f32)],
        compiler_params=params(),
        cost_estimate=cost(11),
        name="back",
    )(own, got, small, out_grad, conv_sum, conv_in, low, gate_grad, w)


def weights_kernel(pairs, half, place, *refs):
    lefts, rights = refs[:pairs], refs[pairs : 2 * pairs]
    w, keep_ref, send_ref, gain_ref, total = refs[2 * pairs :]
    chans = rights[0].shape[1]
    depth = keep_ref.shape[2]
    for i in range(pairs):
        values = dot(lefts[i][...], rights[i][...], TN)
        total[...] = values
        if i == 0:
            product = values * w[:, half * chans : (half + 1) * chans].astype(f32)
            gain_ref[...] = dot(jnp.ones((8, chans), bf16), product.astype(bf16), NT)
        for index in range(2 * keep_ref.shape[0]):
            start = pl.multiple_of(place[index] * depth, depth)
            piece = total[pl.ds(start, depth), :].astype(bf16)
            (send_ref if index % 2 else keep_ref)[index // 2, i] = piece


def weights(place, half, lefts, rights, w):
    depth = w.shape[0]
    chans = rights[0].shape[1]
    size = place.shape[0]
    piece = shape((size // 2, len(lefts), depth // size, chans), bf16)
    outs = [piece, piece, shape((8, depth), f32)]
    return pl.pallas_call(
        functools.partial(weights_kernel, len(lefts), half),
        grid_spec=pltpu.PrefetchScalarGridSpec(
            num_scalar_prefetch=1,
            grid=(1,),
            in_specs=[full(a) for a in (*lefts, *rights, w)],
            out_specs=[full(a) for a in outs],
            scratch_shapes=[pltpu.VMEM((depth, chans), f32)],
        ),
        out_shape=outs,
        compiler_params=params(),
        cost_estimate=cost(3 * len(lefts)),
        name="weights",
    )(place, *lefts, *rights, w)


def last_kernel(tokens, grad, normed_grad, gain, out_ref):
    values = tokens[...].astype(f32)
    inverse = lax.rsqrt(jnp.mean(values * values, axis=-1, keepdims=True) + epsilon)
    hat = values * inverse
    scaled = normed_grad[...].astype(f32) * gain[...]
    out_ref[...] = grad[...].astype(f32) + inverse * (
        scaled - hat * jnp.mean(scaled * hat, axis=-1, keepdims=True)
    )


def last(tokens, grad, normed_grad, gain):
    total, depth = tokens.shape
    rows = min(128, total)
    row = pl.BlockSpec((rows, depth), lambda i: (i, 0))
    return pl.pallas_call(
        last_kernel,
        grid=(total // rows,),
        in_specs=[row, row, row, full(gain)],
        out_specs=row,
        out_shape=shape((total, depth), f32),
        compiler_params=params(),
        cost_estimate=cost(2),
        name="last",
    )(tokens, grad, normed_grad, gain)


def exchange(values, axis, size, bits):
    return lax.ppermute(values, axis, [(i, i ^ bits) for i in range(size)])


def even_pieces(values, axis, size):
    return [values] + [exchange(values, axis, size, m) for m in range(2, size, 2)]


def all_pieces(even, axis, size):
    odd = [exchange(piece, axis, size, 1) for piece in even]
    return [piece for pair in zip(even, odd) for piece in pair]


def pair_sum(keep, send, axis, size):
    return keep + exchange(send, axis, size, 1)


def chip_terms(summed, axis, size):
    return [summed[0]] + [exchange(summed[m], axis, size, 2 * m) for m in range(1, size // 2)]


def total(terms):
    return sum(term.astype(f32) for term in terms)


def sum_all(values, send, axis, size, beside):
    bits = 1
    while bits < size:
        got = exchange(send, axis, size, 2 * bits - 1)
        if bits == 1:
            got, beside = lax.optimization_barrier((got, beside))
        bits *= 2
        if bits < size:
            values = values + got.astype(f32)
            send = values.astype(bf16)
    return values, got, beside


def shards(
    fsdp, tp, tokens, lengths, norm_gain, in_weight, conv_weight, conv_bias, x_weight, dt_weight,
    dt_bias, a_log, d_skip, out_weight, cotangent,
):
    fs_me = lax.axis_index("fsdp")
    place = (fs_me ^ jnp.arange(fsdp)).astype(jnp.int32)
    depth = tokens.shape[2]
    part = conv_weight.shape[1]
    chans = part * fsdp
    lay = Rows(x_weight.shape[1], a_log.shape[0], conv_weight.shape[0])
    maps, width, taps, rank, first = lay.maps, lay.width, lay.taps, lay.rank, lay.first

    whole = lax.all_gather(tokens[0], "tp", axis=0, tiled=True)
    even = even_pieces(in_weight.reshape(in_weight.shape[0], 2 * chans), "fsdp", fsdp)
    even, x_weight = lax.optimization_barrier((even, x_weight))
    w = jnp.stack(all_pieces(even, "fsdp", fsdp))[place].reshape(depth, 2 * chans)
    pieces = all_pieces(even_pieces(out_weight, "fsdp", fsdp), "fsdp", fsdp)
    out_w = jnp.stack(pieces)[place].transpose(1, 0, 2).reshape(chans, depth)
    packed = jnp.concatenate(
        [
            x_weight.T,
            a_log,
            conv_weight,
            conv_bias[None],
            dt_bias[None],
            d_skip[None],
            jnp.zeros((lay.count - first - taps - 3, part), bf16),
            dt_weight.reshape(-1, part),
            norm_gain.reshape(-1, part),
        ],
        0,
    )
    gathered = lax.all_gather(packed, "fsdp", axis=0)
    small = gathered[:, : lay.count].transpose(1, 0, 2).reshape(lay.count, chans)
    dt_rows = dt_weight.size // part
    dt_w = gathered[:, lay.count : lay.count + dt_rows].reshape(rank, chans)
    gain = gathered[:, lay.count + dt_rows :].reshape(1, depth).astype(f32)

    whole, out_w = lax.optimization_barrier((whole, out_w))
    normed, conv_in, gate, conv_sum, low, map_part, map_send = front(lay, whole, gain, small, w)
    map_send, held = lax.optimization_barrier((map_send, cotangent[0]))
    grad_whole = lax.all_gather(held, "tp", axis=0, tiled=True)
    own, got, _ = sum_all(map_part, map_send, "tp", tp, ())
    mixed, before, step, h, sent = forward(
        lay, lengths, own, got, low, gate, dt_w, small, out_w
    )
    block_sum = lax.psum_scatter(sent, "tp", scatter_dimension=0, tiled=True)

    map_part, map_send, conv_grad, gate_grad, rate_grad, dt_w_grad, bias_grad = backward(
        lay, lengths, own, got, low, gate, before, step, grad_whole, h, dt_w, small, out_w
    )
    *out_one, _ = weights(place, 0, (grad_whole,), (mixed,), w)
    own_grad, got_grad, (held, out_one) = sum_all(
        map_part, map_send, "tp", tp, (gate_grad, out_one)
    )
    *gate_one, gain_two = weights(place, 1, (normed,), (held,), w)
    block_out = (tokens.astype(f32) + block_sum[None].astype(f32)).astype(bf16)
    out_pairs = pair_sum(*out_one, "fsdp", fsdp)
    own_grad, got_grad, gate_one, out_pairs = lax.optimization_barrier(
        (own_grad, got_grad, gate_one, out_pairs)
    )
    normed_part, input_grad, x_w_grad, taps_grad = back(
        lay, own_grad, got_grad, small, conv_grad, conv_sum, conv_in, low, gate_grad, w
    )
    normed_grad = lax.psum_scatter(normed_part, "tp", scatter_dimension=0, tiled=True)
    *one, gain_one = weights(place, 0, (normed,), (input_grad,), w)
    out_terms = chip_terms(out_pairs, "fsdp", fsdp)
    gate_terms = chip_terms(pair_sum(*gate_one, "fsdp", fsdp), "fsdp", fsdp)
    x_w_grad, taps_grad, out_terms, gate_terms = lax.optimization_barrier(
        (x_w_grad, taps_grad, out_terms, gate_terms)
    )
    conv_terms = chip_terms(pair_sum(*one, "fsdp", fsdp), "fsdp", fsdp)
    out_weight_grad, gate_half, conv_half = (
        total(terms)[0] for terms in (out_terms, gate_terms, conv_terms)
    )
    in_weight_grad = jnp.stack([conv_half, gate_half], 1)
    out_weight_grad = out_weight_grad.T
    gain_grad = gain_one[:1] + gain_two[:1]
    bits = 1
    while bits < tp:
        gain_grad = gain_grad + exchange(gain_grad, "tp", tp, 2 * bits - 1)
        bits *= 2
    rows = jnp.concatenate(
        [x_w_grad, rate_grad * LN2, taps_grad[: taps + 1], bias_grad[:2]], 0
    ).astype(bf16)
    top = rows.shape[0]
    packed = jnp.concatenate(
        [
            rows.reshape(top, fsdp, part).transpose(1, 0, 2),
            dt_w_grad.astype(bf16).reshape(fsdp, -1, part),
            gain_grad.astype(bf16).reshape(fsdp, -1, part),
        ],
        1,
    )[place]
    pairs = pair_sum(packed[0::2], packed[1::2], "fsdp", fsdp)
    small_grad = total(chip_terms(pairs, "fsdp", fsdp))
    gain_out = small_grad[top + dt_rows :].reshape(-1) / norm_gain.astype(f32)

    input_grads = last(tokens[0], cotangent[0], normed_grad, gain)[None]
    return (
        block_out,
        input_grads,
        gain_out,
        in_weight_grad,
        small_grad[first : first + taps],
        small_grad[first + taps],
        small_grad[:maps].T,
        small_grad[top : top + dt_rows].reshape(-1, chans),
        small_grad[first + taps + 1],
        small_grad[maps:first],
        small_grad[first + taps + 2],
        out_weight_grad,
    )


def solution(mesh):
    sizes = dict(mesh.shape)
    return jax.shard_map(
        functools.partial(shards, sizes["fsdp"], sizes["tp"]),
        mesh=mesh,
        in_specs=(
            P("fsdp", "tp", None),
            P("fsdp"),
            P("fsdp"),
            P("fsdp", None, "tp"),
            P(None, ("tp", "fsdp")),
            P(("tp", "fsdp")),
            P(("tp", "fsdp"), None),
            P("fsdp", "tp"),
            P(("tp", "fsdp")),
            P(None, ("tp", "fsdp")),
            P(("tp", "fsdp")),
            P("tp", "fsdp"),
            P("fsdp", "tp", None),
        ),
        out_specs=(
            P("fsdp", "tp", None),
            P("fsdp", "tp", None),
            P("fsdp"),
            P("fsdp", None, "tp"),
            P(None, ("tp", "fsdp")),
            P(("tp", "fsdp")),
            P(("tp", "fsdp"), None),
            P("fsdp", "tp"),
            P(("tp", "fsdp")),
            P(None, ("tp", "fsdp")),
            P(("tp", "fsdp")),
            P("tp", "fsdp"),
        ),
        check_vma=False,
    )
```

```python
import functools

import jax
import jax.numpy as jnp
from jax import lax
from jax.experimental import pallas as pl
from jax.experimental.pallas import tpu as pltpu
from jax.sharding import PartitionSpec as P

bf16 = jnp.bfloat16
f32 = jnp.float32
LOG2E = 1.4426950408889634
LN2 = 0.6931471805599453
ROWS = 256
STEPS = 16
LANES = 128
SCALE = 1.0
NT = (((1,), (1,)), ((), ()))
TN = (((0,), (0,)), ((), ()))
epsilon = 1e-05
VMEM_LIMIT = 56 * 2**20


def dot(a, b, dims=(((1,), (0,)), ((), ()))):
    return lax.dot_general(a, b, dims, preferred_element_type=f32)


def shape(dims, kind):
    return jax.ShapeDtypeStruct(dims, kind)


def iota(dims, axis):
    return lax.broadcasted_iota(jnp.int32, dims, axis)


def params():
    return pltpu.CompilerParams(vmem_limit_bytes=VMEM_LIMIT)


def cost(micros):
    return pl.CostEstimate(
        flops=int(micros * SCALE * 1e9), bytes_accessed=int(micros * SCALE * 3e6), transcendentals=0
    )


def halves(values):
    high = values.astype(bf16)
    return high, (values - high.astype(f32)).astype(bf16)


def spread(columns):
    width, rows = columns.shape
    wide = STEPS * width
    pick = (iota((width, wide), 1) % width == iota((width, wide), 0)).astype(bf16)
    keep = iota((rows, wide), 1) // width == iota((rows, wide), 0) % STEPS
    return jnp.where(keep, dot(columns, pick, TN), 0.0).astype(bf16)


def to_lanes(target, columns):
    width, rows = columns.shape
    wide = STEPS * width
    parts = [spread(part) for part in halves(columns)]
    ones = jnp.ones((2 * STEPS, LANES), bf16)
    for index in range(rows // STEPS):
        s = slice(index * STEPS, (index + 1) * STEPS)
        both = jnp.concatenate([part[s] for part in parts], 0)
        target[index * wide : (index + 1) * wide, :] = dot(both, ones, TN)


def across(values, chans):
    return jnp.concatenate([values] * (chans // LANES), 1)


def row_of(ref, index, count):
    return ref[pl.ds(index, count, stride=0), :]


def twice(values):
    return jnp.concatenate([values, values], 0).astype(bf16)


def fold(values):
    return sum(values[:, i : i + LANES] for i in range(0, values.shape[1], LANES))


def lane_sums(values, width):
    rows = values.shape[0] // width
    if rows > LANES:
        step = LANES * width
        parts = [values[i : i + step] for i in range(0, values.shape[0], step)]
        return jnp.concatenate([lane_sums(part, width) for part in parts], 1)
    sums = dot(values, jnp.ones((LANES, rows), bf16))
    lane = iota((width, rows), 1)
    kept = [jnp.zeros((width, rows), f32)] * 4
    for t in range(rows):
        kept[t % 4] = jnp.where(lane == t, sums[t * width : (t + 1) * width], kept[t % 4])
    return (kept[0] + kept[1]) + (kept[2] + kept[3])


def live_rows(length, first, rows):
    return (iota((rows, 1), 0) + first < length).astype(f32)


def full(array):
    return pl.BlockSpec(array.shape, lambda *_: (0,) * len(array.shape))


class Rows:
    def __init__(self, maps, width, taps):
        self.maps = maps
        self.width = width
        self.taps = taps
        self.rank = maps - 2 * width
        self.first = maps + width
        self.count = -(-(self.first + taps + 3) // 16) * 16

    def x_w(self, ref):
        return ref[: self.maps, :]

    def a_log(self, ref):
        return ref[self.maps : self.first, :].astype(f32)

    def rest(self, ref):
        return ref[self.first :, :].astype(f32)


def front_kernel(
    lay, tokens, gain, small, w,
    normed_ref, input_ref, gate_ref, sum_ref, low_ref, map_ref, send_ref, halo,
):
    rows = tokens.shape[0]
    chans = small.shape[1]
    taps = lay.taps

    @pl.when(pl.program_id(0) == 0)
    def _():
        halo[:8] = jnp.zeros_like(halo[:8])

    values = tokens[...].astype(f32)
    inverse = lax.rsqrt(jnp.mean(values * values, axis=-1, keepdims=True) + epsilon)
    normed = (values * inverse * gain[...]).astype(bf16)
    normed_ref[...] = normed
    projected = dot(normed, w[...])
    conv_in = projected[:, :chans]
    input_ref[...] = conv_in
    gate_ref[...] = projected[:, chans:]
    halo[8:] = conv_in
    rest = lay.rest(small)
    total = rest[taps : taps + 1]
    for tap in range(taps):
        first = 8 - taps + 1 + tap
        total = total + rest[tap : tap + 1] * halo[first : first + rows]
    halo[:8] = conv_in[rows - 8 :]
    sum_ref[...] = total
    low = (total * jax.nn.sigmoid(total)).astype(bf16)
    low_ref[...] = low
    mapped = dot(lay.x_w(small), low, NT)
    map_ref[...] = mapped
    send_ref[...] = mapped.astype(bf16)


def front(lay, tokens, gain, small, w):
    total, depth = tokens.shape
    rows = 256
    chans = small.shape[1]
    row = lambda w: pl.BlockSpec((rows, w), lambda i: (i, 0))
    column = lambda w: pl.BlockSpec((w, rows), lambda i: (0, i))
    return pl.pallas_call(
        functools.partial(front_kernel, lay),
        grid=(total // rows,),
        in_specs=[row(depth)] + [full(a) for a in (gain, small, w)],
        out_specs=[row(depth)] + [row(chans)] * 4 + [column(lay.maps)] * 2,
        out_shape=[
            shape((total, depth), bf16),
            shape((total, chans), f32),
            shape((total, chans), f32),
            shape((total, chans), f32),
            shape((total, chans), bf16),
            shape((lay.maps, total), f32),
            shape((lay.maps, total), bf16),
        ],
        scratch_shapes=[pltpu.VMEM((rows + 8, chans), f32)],
        compiler_params=params(),
        cost_estimate=cost(9),
        name="front",
    )(tokens, gain, small, w)


def forward_kernel(
    lay, length, own, got, low, gate, dt_w, small, out_w,
    mixed_ref, before_ref, step_ref, h_ref, sent_ref, state, drive, lanes, step_rows, drive_rows,
):
    rows, chans = low.shape
    width, rank, taps = lay.width, lay.rank, lay.taps
    half = width // 2
    wide = STEPS * width

    @pl.when(pl.program_id(0) == 0)
    def _():
        state[...] = jnp.zeros_like(state)

    live = live_rows(length[0], pl.program_id(0) * rows, rows)
    mapped = own[...] + got[...].astype(f32)
    rest = lay.rest(small)
    step_pre = dot(mapped[:rank].astype(bf16), dt_w[...], TN) + rest[taps + 1 : taps + 2]
    step = jax.nn.softplus(step_pre) * live
    step_ref[...] = step
    conv_out = low[...].astype(f32)
    drive[...] = step * conv_out
    to_lanes(lanes, mapped[rank : rank + width])
    rate = -jnp.exp(lay.a_log(small)) * LOG2E
    rate_0, rate_1 = rate[:half], rate[half:]

    def body(block, carried):
        h_0, h_1 = carried
        s = pl.ds(pl.multiple_of(block * STEPS, STEPS), STEPS)
        step_rows[...] = step_ref[s, :]
        drive_rows[...] = drive[s, :]
        for k in range(STEPS):
            steps = row_of(step_rows, k, half)
            drives = row_of(drive_rows, k, half)
            base = pl.multiple_of(block * wide, wide) + k * width
            b_0 = across(lanes[pl.ds(base, half), :], chans)
            b_1 = across(lanes[pl.ds(base + half, half), :], chans)
            h_0 = jnp.exp2(steps * rate_0) * h_0 + drives * b_0
            h_1 = jnp.exp2(steps * rate_1) * h_1 + drives * b_1
            h_ref[pl.ds(base, width), :] = jnp.concatenate([h_0, h_1], 0).astype(bf16)
        return h_0, h_1

    h_0, h_1 = lax.fori_loop(0, rows // STEPS, body, (state[:half], state[half:]))
    state[:half] = h_0
    state[half:] = h_1
    outs = spread(mapped[rank + width :].astype(bf16))
    scan = [
        dot(outs[i * STEPS : (i + 1) * STEPS], h_ref[i * wide : (i + 1) * wide, :])
        for i in range(rows // STEPS)
    ]
    before = jnp.concatenate(scan, 0) + rest[taps + 2 : taps + 3] * conv_out
    before_ref[...] = before
    gates = gate[...]
    mixed = (before * (gates * jax.nn.sigmoid(gates)) * live).astype(bf16)
    mixed_ref[...] = mixed
    sent_ref[...] = dot(mixed, out_w[...]).astype(bf16)


def forward(lay, length, own, got, low, gate, dt_w, small, out_w):
    total, chans = low.shape
    depth = out_w.shape[1]
    width = lay.width
    row = lambda w: pl.BlockSpec((ROWS, w), lambda i, *_: (i, 0))
    column = lambda w: pl.BlockSpec((w, ROWS), lambda i, *_: (0, i))
    return pl.pallas_call(
        functools.partial(forward_kernel, lay),
        grid_spec=pltpu.PrefetchScalarGridSpec(
            num_scalar_prefetch=1,
            grid=(total // ROWS,),
            in_specs=[column(lay.maps), column(lay.maps), row(chans), row(chans)]
            + [full(a) for a in (dt_w, small, out_w)],
            out_specs=[
                row(chans),
                row(chans),
                row(chans),
                pl.BlockSpec((ROWS * width, chans), lambda i, *_: (i, 0)),
                row(depth),
            ],
            scratch_shapes=[
                pltpu.VMEM((width, chans), f32),
                pltpu.VMEM((ROWS, chans), f32),
                pltpu.VMEM((ROWS * width, LANES), f32),
                pltpu.VMEM((STEPS, chans), f32),
                pltpu.VMEM((STEPS, chans), f32),
            ],
        ),
        out_shape=[
            shape((total, chans), bf16),
            shape((total, chans), f32),
            shape((total, chans), f32),
            shape((total * width, chans), bf16),
            shape((total, depth), bf16),
        ],
        compiler_params=params(),
        cost_estimate=cost(24),
        name="forward",
    )(length, own, got, low, gate, dt_w, small, out_w)


def backward_kernel(
    lay, length, own, got, low, gate, before_ref, step_ref, grad, h_ref, last_ref, dt_w, small, out_w_t,
    map_ref, send_ref, out_ref, gate_ref, rate_ref, dt_w_ref, bias_ref,
    carry, grads, terms, drive, scan_grad, lanes, cross_b, cross_c, step_rows, drive_rows, grad_rows,
):
    rows, chans = low.shape
    width, rank, taps = lay.width, lay.rank, lay.taps
    half = width // 2
    wide = STEPS * width
    turn = pl.program_id(0)
    turns = pl.num_programs(0)

    @pl.when(turn == 0)
    def _():
        for ref in (carry, rate_ref, dt_w_ref, bias_ref):
            ref[...] = jnp.zeros_like(ref)

    live = live_rows(length[0], (turns - 1 - turn) * rows, rows)
    rest = lay.rest(small)
    conv_out = low[...].astype(f32)
    masked = dot(grad[...], out_w_t[...]) * live
    gates = gate[...]
    sigma = jax.nn.sigmoid(gates)
    gate_ref[...] = (
        masked * before_ref[...] * (sigma * (1.0 + gates * (1.0 - sigma)))
    ).astype(bf16)
    out_scan = masked * (gates * sigma)
    scan_grad[...] = out_scan
    bias_ref[1:2] += jnp.sum(out_scan * conv_out, axis=0, keepdims=True)
    mapped = own[...] + got[...].astype(f32)
    to_lanes(lanes, mapped[rank + width :])
    drive[...] = step_ref[...] * conv_out
    rate = -jnp.exp(lay.a_log(small)) * LOG2E
    rate_0, rate_1 = rate[:half], rate[half:]
    rate_low = rate.astype(bf16)
    first = jnp.where(turn == turns - 1, jnp.zeros_like(last_ref[...]), last_ref[...])

    def body(back, carried):
        q_0, q_1, total, h = carried
        block = rows // STEPS - 1 - back
        s = pl.ds(pl.multiple_of(block * STEPS, STEPS), STEPS)
        step_rows[...] = step_ref[s, :]
        drive_rows[...] = drive[s, :]
        grad_rows[...] = scan_grad[s, :]
        part = jnp.zeros((width, chans), bf16)
        for k in reversed(range(STEPS)):
            steps = row_of(step_rows, k, half)
            drives = row_of(drive_rows, k, half)
            outs = row_of(grad_rows, k, half)
            base = pl.multiple_of(block * wide, wide) + k * width
            g_0 = outs * across(lanes[pl.ds(base, half), :], chans) + q_0
            g_1 = outs * across(lanes[pl.ds(base + half, half), :], chans) + q_1
            g = jnp.concatenate([g_0, g_1], 0).astype(bf16)
            grads[pl.ds(base, width), :] = g
            cross_b[pl.ds(base, width), :] = fold(g * twice(drives))
            cross_c[pl.ds(base, width), :] = fold(h * twice(outs))
            q_0 = jnp.exp2(steps * rate_0) * g_0
            q_1 = jnp.exp2(steps * rate_1) * g_1
            if k == 0:
                start = pl.multiple_of(jnp.maximum(base - width, 0), width)
                h = jnp.where(block == 0, first, h_ref[pl.ds(start, width), :])
            else:
                h = h_ref[pl.ds(base - width, width), :]
            term = jnp.concatenate([q_0, q_1], 0).astype(bf16) * h * rate_low
            terms[pl.ds(base, width), :] = term
            part = part + twice(steps) * term
        return q_0, q_1, total + part.astype(f32), h

    start = (carry[:half], carry[half:], rate_ref[...], h_ref[(rows - 1) * width :, :])
    q_0, q_1, total, _ = lax.fori_loop(0, rows // STEPS, body, start)
    carry[:half] = q_0
    carry[half:] = q_1
    rate_ref[...] = total
    ins = spread(mapped[rank : rank + width].astype(bf16))
    ones = (iota((STEPS, wide), 1) // width == iota((STEPS, wide), 0)).astype(bf16)
    weighted, stepped = [], []
    for i in range(rows // STEPS):
        big = slice(i * wide, (i + 1) * wide)
        weighted.append(dot(ins[i * STEPS : (i + 1) * STEPS], grads[big, :]))
        stepped.append(dot(ones, terms[big, :]))
    weighted = jnp.concatenate(weighted, 0)
    step_grad = jnp.concatenate(stepped, 0) * LN2 + conv_out * weighted
    map_low = mapped[:rank].astype(bf16)
    step_pre = dot(map_low, dt_w[...], TN) + rest[taps + 1 : taps + 2]
    pre_grad = (step_grad * live * jax.nn.sigmoid(step_pre)).astype(bf16)
    bias_ref[0:1] += jnp.sum(pre_grad.astype(f32), axis=0, keepdims=True)
    dt_w_ref[...] += dot(map_low, pre_grad)
    map_grad = jnp.concatenate(
        [dot(dt_w[...], pre_grad, NT), lane_sums(cross_b[...], width), lane_sums(cross_c[...], width)],
        0,
    )
    map_ref[...] = map_grad
    send_ref[...] = map_grad.astype(bf16)
    out_ref[...] = out_scan * rest[taps + 2 : taps + 3] + step_ref[...] * weighted


def backward(lay, length, own, got, low, gate, before, step, grad, h, dt_w, small, out_w_t):
    total, chans = low.shape
    width = lay.width
    turns = total // ROWS
    at = lambda i: turns - 1 - i
    row = lambda w: pl.BlockSpec((ROWS, w), lambda i, *_: (at(i), 0))
    column = lambda w: pl.BlockSpec((w, ROWS), lambda i, *_: (0, at(i)))
    outs = [
        shape((lay.maps, total), f32),
        shape((lay.maps, total), bf16),
        shape((total, chans), f32),
        shape((total, chans), bf16),
        shape((width, chans), f32),
        shape(dt_w.shape, f32),
        shape((8, chans), f32),
    ]
    return pl.pallas_call(
        functools.partial(backward_kernel, lay),
        grid_spec=pltpu.PrefetchScalarGridSpec(
            num_scalar_prefetch=1,
            grid=(turns,),
            in_specs=[
                column(lay.maps),
                column(lay.maps),
                row(chans),
                row(chans),
                row(chans),
                row(chans),
                row(grad.shape[1]),
                pl.BlockSpec((ROWS * width, chans), lambda i, *_: (at(i), 0)),
                pl.BlockSpec((width, chans), lambda i, *_: (jnp.maximum(at(i) * ROWS - 1, 0), 0)),
            ]
            + [full(a) for a in (dt_w, small, out_w_t)],
            out_specs=[column(lay.maps), column(lay.maps), row(chans), row(chans)]
            + [full(a) for a in outs[4:]],
            scratch_shapes=[
                pltpu.VMEM((width, chans), f32),
                pltpu.VMEM((ROWS * width, chans), bf16),
                pltpu.VMEM((ROWS * width, chans), bf16),
                pltpu.VMEM((ROWS, chans), f32),
                pltpu.VMEM((ROWS, chans), f32),
                pltpu.VMEM((ROWS * width, LANES), f32),
                pltpu.VMEM((ROWS * width, LANES), bf16),
                pltpu.VMEM((ROWS * width, LANES), bf16),
                pltpu.VMEM((STEPS, chans), f32),
                pltpu.VMEM((STEPS, chans), f32),
                pltpu.VMEM((STEPS, chans), f32),
            ],
        ),
        out_shape=outs,
        compiler_params=params(),
        cost_estimate=cost(40),
        name="backward",
    )(length, own, got, low, gate, before, step, grad, h, h, dt_w, small, out_w_t)


def back_kernel(
    lay, own, got, small, out_grad, conv_sum, conv_in, low, gate_grad, w,
    part_ref, input_ref, x_ref, conv_ref, halo,
):
    rows, chans = low.shape
    taps = lay.taps
    turn = pl.program_id(0)

    @pl.when(turn == 0)
    def _():
        halo[rows:] = jnp.zeros_like(halo[rows:])
        for ref in (x_ref, conv_ref):
            ref[...] = jnp.zeros_like(ref)

    rest = lay.rest(small)
    map_grad = (own[...] + got[...].astype(f32)).astype(bf16)
    x_ref[...] += dot(map_grad, low[...])
    values = conv_sum[...]
    sigma = jax.nn.sigmoid(values)
    sum_grad = (out_grad[...] + dot(map_grad, lay.x_w(small), TN)) * (
        sigma * (1.0 + values * (1.0 - sigma))
    )
    conv_ref[taps : taps + 1] += jnp.sum(sum_grad, axis=0, keepdims=True)
    halo[:rows] = sum_grad
    inputs = conv_in[...]
    input_grad = jnp.zeros_like(inputs)
    for tap in range(taps):
        first = taps - 1 - tap
        moved = halo[first : first + rows]
        input_grad = input_grad + rest[tap : tap + 1] * moved
        conv_ref[tap : tap + 1] += jnp.sum(inputs * moved, axis=0, keepdims=True)
    halo[rows:] = sum_grad[:8]
    input_grad = input_grad.astype(bf16)
    input_ref[...] = input_grad
    part = dot(jnp.concatenate([input_grad, gate_grad[...]], 1), w[...], NT)
    part_ref[...] = part.astype(bf16)


def back(lay, own, got, small, out_grad, conv_sum, conv_in, low, gate_grad, w):
    total, chans = low.shape
    depth = w.shape[0]
    rows = 256
    count = total // rows
    at = lambda i: count - 1 - i
    row = lambda a: pl.BlockSpec((rows, a.shape[1]), lambda i: (at(i), 0))
    column = lambda a: pl.BlockSpec((a.shape[0], rows), lambda i: (0, at(i)))
    outs = [
        shape((total, depth), bf16),
        shape((total, chans), bf16),
        shape((lay.maps, chans), f32),
        shape((8, chans), f32),
    ]
    return pl.pallas_call(
        functools.partial(back_kernel, lay),
        grid=(count,),
        in_specs=[
            column(own),
            column(got),
            full(small),
            row(out_grad),
            row(conv_sum),
            row(conv_in),
            row(low),
            row(gate_grad),
            full(w),
        ],
        out_specs=[row(outs[0]), row(outs[1]), full(outs[2]), full(outs[3])],
        out_shape=outs,
        scratch_shapes=[pltpu.VMEM((rows + 8, chans), f32)],
        compiler_params=params(),
        cost_estimate=cost(11),
        name="back",
    )(own, got, small, out_grad, conv_sum, conv_in, low, gate_grad, w)


def weights_kernel(pairs, half, place, *refs):
    lefts, rights = refs[:pairs], refs[pairs : 2 * pairs]
    w, keep_ref, send_ref, gain_ref, total = refs[2 * pairs :]
    chans = rights[0].shape[1]
    depth = keep_ref.shape[2]
    for i in range(pairs):
        values = dot(lefts[i][...], rights[i][...], TN)
        total[...] = values
        if i == 0:
            product = values * w[:, half * chans : (half + 1) * chans].astype(f32)
            gain_ref[...] = dot(jnp.ones((8, chans), bf16), product.astype(bf16), NT)
        for index in range(2 * keep_ref.shape[0]):
            start = pl.multiple_of(place[index] * depth, depth)
            piece = total[pl.ds(start, depth), :].astype(bf16)
            (send_ref if index % 2 else keep_ref)[index // 2, i] = piece


def weights(place, half, lefts, rights, w):
    depth = w.shape[0]
    chans = rights[0].shape[1]
    size = place.shape[0]
    piece = shape((size // 2, len(lefts), depth // size, chans), bf16)
    outs = [piece, piece, shape((8, depth), f32)]
    return pl.pallas_call(
        functools.partial(weights_kernel, len(lefts), half),
        grid_spec=pltpu.PrefetchScalarGridSpec(
            num_scalar_prefetch=1,
            grid=(1,),
            in_specs=[full(a) for a in (*lefts, *rights, w)],
            out_specs=[full(a) for a in outs],
            scratch_shapes=[pltpu.VMEM((depth, chans), f32)],
        ),
        out_shape=outs,
        compiler_params=params(),
        cost_estimate=cost(3 * len(lefts)),
        name="weights",
    )(place, *lefts, *rights, w)


def last_kernel(tokens, grad, normed_grad, gain, out_ref):
    values = tokens[...].astype(f32)
    inverse = lax.rsqrt(jnp.mean(values * values, axis=-1, keepdims=True) + epsilon)
    hat = values * inverse
    scaled = normed_grad[...].astype(f32) * gain[...]
    out_ref[...] = grad[...].astype(f32) + inverse * (
        scaled - hat * jnp.mean(scaled * hat, axis=-1, keepdims=True)
    )


def last(tokens, grad, normed_grad, gain):
    total, depth = tokens.shape
    rows = min(128, total)
    row = pl.BlockSpec((rows, depth), lambda i: (i, 0))
    return pl.pallas_call(
        last_kernel,
        grid=(total // rows,),
        in_specs=[row, row, row, full(gain)],
        out_specs=row,
        out_shape=shape((total, depth), f32),
        compiler_params=params(),
        cost_estimate=cost(2),
        name="last",
    )(tokens, grad, normed_grad, gain)


def exchange(values, axis, size, bits):
    return lax.ppermute(values, axis, [(i, i ^ bits) for i in range(size)])


def even_pieces(values, axis, size):
    return [values] + [exchange(values, axis, size, m) for m in range(2, size, 2)]


def all_pieces(even, axis, size):
    odd = [exchange(piece, axis, size, 1) for piece in even]
    return [piece for pair in zip(even, odd) for piece in pair]


def pair_sum(keep, send, axis, size):
    return keep + exchange(send, axis, size, 1)


def chip_terms(summed, axis, size):
    return [summed[0]] + [exchange(summed[m], axis, size, 2 * m) for m in range(1, size // 2)]


def total(terms):
    return sum(term.astype(f32) for term in terms)


def sum_all(values, send, axis, size, beside):
    bits = 1
    while bits < size:
        got = exchange(send, axis, size, 2 * bits - 1)
        if bits == 1:
            got, beside = lax.optimization_barrier((got, beside))
        bits *= 2
        if bits < size:
            values = values + got.astype(f32)
            send = values.astype(bf16)
    return values, got, beside


def shards(
    fsdp, tp, tokens, lengths, norm_gain, in_weight, conv_weight, conv_bias, x_weight, dt_weight,
    dt_bias, a_log, d_skip, out_weight, cotangent,
):
    fs_me = lax.axis_index("fsdp")
    place = (fs_me ^ jnp.arange(fsdp)).astype(jnp.int32)
    depth = tokens.shape[2]
    part = conv_weight.shape[1]
    chans = part * fsdp
    lay = Rows(x_weight.shape[1], a_log.shape[0], conv_weight.shape[0])
    maps, width, taps, rank, first = lay.maps, lay.width, lay.taps, lay.rank, lay.first

    whole = lax.all_gather(tokens[0], "tp", axis=0, tiled=True)
    even = even_pieces(in_weight.reshape(in_weight.shape[0], 2 * chans), "fsdp", fsdp)
    even, x_weight = lax.optimization_barrier((even, x_weight))
    w = jnp.stack(all_pieces(even, "fsdp", fsdp))[place].reshape(depth, 2 * chans)
    pieces = all_pieces(even_pieces(out_weight, "fsdp", fsdp), "fsdp", fsdp)
    ordered = jnp.stack(pieces)[place]
    out_w = ordered.transpose(1, 0, 2).reshape(chans, depth)
    out_w_t = ordered.transpose(0, 2, 1).reshape(depth, chans)
    packed = jnp.concatenate(
        [
            x_weight.T,
            a_log,
            conv_weight,
            conv_bias[None],
            dt_bias[None],
            d_skip[None],
            jnp.zeros((lay.count - first - taps - 3, part), bf16),
            dt_weight.reshape(-1, part),
            norm_gain.reshape(-1, part),
        ],
        0,
    )
    gathered = lax.all_gather(packed, "fsdp", axis=0)
    small = gathered[:, : lay.count].transpose(1, 0, 2).reshape(lay.count, chans)
    dt_rows = dt_weight.size // part
    dt_w = gathered[:, lay.count : lay.count + dt_rows].reshape(rank, chans)
    gain = gathered[:, lay.count + dt_rows :].reshape(1, depth).astype(f32)

    whole, out_w, out_w_t = lax.optimization_barrier((whole, out_w, out_w_t))
    normed, conv_in, gate, conv_sum, low, map_part, map_send = front(lay, whole, gain, small, w)
    own, got, held = sum_all(map_part, map_send, "tp", tp, cotangent[0])
    grad_whole = lax.all_gather(held, "tp", axis=0, tiled=True)
    mixed, before, step, h, sent = forward(
        lay, lengths, own, got, low, gate, dt_w, small, out_w
    )
    block_sum = lax.psum_scatter(sent, "tp", scatter_dimension=0, tiled=True)

    map_part, map_send, conv_grad, gate_grad, rate_grad, dt_w_grad, bias_grad = backward(
        lay, lengths, own, got, low, gate, before, step, grad_whole, h, dt_w, small, out_w_t
    )
    *out_one, _ = weights(place, 0, (grad_whole,), (mixed,), w)
    own_grad, got_grad, (held, out_one) = sum_all(
        map_part, map_send, "tp", tp, (gate_grad, out_one)
    )
    *gate_one, gain_two = weights(place, 1, (normed,), (held,), w)
    out_pairs = pair_sum(*out_one, "fsdp", fsdp)
    own_grad, got_grad, gate_one, out_pairs = lax.optimization_barrier(
        (own_grad, got_grad, gate_one, out_pairs)
    )
    normed_part, input_grad, x_w_grad, taps_grad = back(
        lay, own_grad, got_grad, small, conv_grad, conv_sum, conv_in, low, gate_grad, w
    )
    normed_grad = lax.psum_scatter(normed_part, "tp", scatter_dimension=0, tiled=True)
    *one, gain_one = weights(place, 0, (normed,), (input_grad,), w)
    out_terms = chip_terms(out_pairs, "fsdp", fsdp)
    gate_terms = chip_terms(pair_sum(*gate_one, "fsdp", fsdp), "fsdp", fsdp)
    x_w_grad, taps_grad, out_terms, gate_terms = lax.optimization_barrier(
        (x_w_grad, taps_grad, out_terms, gate_terms)
    )
    conv_terms = chip_terms(pair_sum(*one, "fsdp", fsdp), "fsdp", fsdp)
    gain_grad = gain_one[:1] + gain_two[:1]
    bits = 1
    while bits < tp:
        gain_grad = gain_grad + exchange(gain_grad, "tp", tp, 2 * bits - 1)
        bits *= 2
    rows = jnp.concatenate(
        [x_w_grad, rate_grad * LN2, taps_grad[: taps + 1], bias_grad[:2]], 0
    ).astype(bf16)
    top = rows.shape[0]
    packed = jnp.concatenate(
        [
            rows.reshape(top, fsdp, part).transpose(1, 0, 2),
            dt_w_grad.astype(bf16).reshape(fsdp, -1, part),
            gain_grad.astype(bf16).reshape(fsdp, -1, part),
        ],
        1,
    )[place]
    pairs = pair_sum(packed[0::2], packed[1::2], "fsdp", fsdp)
    small_terms = chip_terms(pairs, "fsdp", fsdp)
    out_terms, gate_terms, conv_terms, small_terms, block_sum = lax.optimization_barrier(
        (out_terms, gate_terms, conv_terms, small_terms, block_sum)
    )
    small_grad = total(small_terms)
    out_weight_grad = total(out_terms)[0].T
    in_weight_grad = jnp.stack([total(conv_terms)[0], total(gate_terms)[0]], 1)
    block_out = (tokens.astype(f32) + block_sum[None].astype(f32)).astype(bf16)
    gain_out = small_grad[top + dt_rows :].reshape(-1) / norm_gain.astype(f32)

    input_grads = last(tokens[0], cotangent[0], normed_grad, gain)[None]
    return (
        block_out,
        input_grads,
        gain_out,
        in_weight_grad,
        small_grad[first : first + taps],
        small_grad[first + taps],
        small_grad[:maps].T,
        small_grad[top : top + dt_rows].reshape(-1, chans),
        small_grad[first + taps + 1],
        small_grad[maps:first],
        small_grad[first + taps + 2],
        out_weight_grad,
    )


def solution(mesh):
    sizes = dict(mesh.shape)
    return jax.shard_map(
        functools.partial(shards, sizes["fsdp"], sizes["tp"]),
        mesh=mesh,
        in_specs=(
            P("fsdp", "tp", None),
            P("fsdp"),
            P("fsdp"),
            P("fsdp", None, "tp"),
            P(None, ("tp", "fsdp")),
            P(("tp", "fsdp")),
            P(("tp", "fsdp"), None),
            P("fsdp", "tp"),
            P(("tp", "fsdp")),
            P(None, ("tp", "fsdp")),
            P(("tp", "fsdp")),
            P("tp", "fsdp"),
            P("fsdp", "tp", None),
        ),
        out_specs=(
            P("fsdp", "tp", None),
            P("fsdp", "tp", None),
            P("fsdp"),
            P("fsdp", None, "tp"),
            P(None, ("tp", "fsdp")),
            P(("tp", "fsdp")),
            P(("tp", "fsdp"), None),
            P("fsdp", "tp"),
            P(("tp", "fsdp")),
            P(None, ("tp", "fsdp")),
            P(("tp", "fsdp")),
            P("tp", "fsdp"),
        ),
        check_vma=False,
    )
```

```python
import functools

import jax
import jax.numpy as jnp
from jax import lax
from jax.experimental import pallas as pl
from jax.experimental.pallas import tpu as pltpu
from jax.sharding import PartitionSpec as P

bf16 = jnp.bfloat16
f32 = jnp.float32
LOG2E = 1.4426950408889634
LN2 = 0.6931471805599453
ROWS = 256
STEPS = 16
LANES = 128
SCALE = 1.0
NT = (((1,), (1,)), ((), ()))
TN = (((0,), (0,)), ((), ()))
epsilon = 1e-05
VMEM_LIMIT = 56 * 2**20


def dot(a, b, dims=(((1,), (0,)), ((), ()))):
    return lax.dot_general(a, b, dims, preferred_element_type=f32)


def shape(dims, kind):
    return jax.ShapeDtypeStruct(dims, kind)


def iota(dims, axis):
    return lax.broadcasted_iota(jnp.int32, dims, axis)


def params():
    return pltpu.CompilerParams(vmem_limit_bytes=VMEM_LIMIT)


def cost(micros):
    return pl.CostEstimate(
        flops=int(micros * SCALE * 1e9), bytes_accessed=int(micros * SCALE * 3e6), transcendentals=0
    )


def halves(values):
    high = values.astype(bf16)
    return high, (values - high.astype(f32)).astype(bf16)


def spread(columns):
    width, rows = columns.shape
    wide = STEPS * width
    pick = (iota((width, wide), 1) % width == iota((width, wide), 0)).astype(bf16)
    keep = iota((rows, wide), 1) // width == iota((rows, wide), 0) % STEPS
    return jnp.where(keep, dot(columns, pick, TN), 0.0).astype(bf16)


def to_lanes(target, columns):
    width, rows = columns.shape
    wide = STEPS * width
    parts = [spread(part) for part in halves(columns)]
    ones = jnp.ones((2 * STEPS, LANES), bf16)
    for index in range(rows // STEPS):
        s = slice(index * STEPS, (index + 1) * STEPS)
        both = jnp.concatenate([part[s] for part in parts], 0)
        target[index * wide : (index + 1) * wide, :] = dot(both, ones, TN)


def across(values, chans):
    return jnp.concatenate([values] * (chans // LANES), 1)


def row_of(ref, index, count):
    return ref[pl.ds(index, count, stride=0), :]


def twice(values):
    return jnp.concatenate([values, values], 0).astype(bf16)


def fold(values):
    return sum(values[:, i : i + LANES] for i in range(0, values.shape[1], LANES))


def lane_sums(values, width):
    rows = values.shape[0] // width
    if rows > LANES:
        step = LANES * width
        parts = [values[i : i + step] for i in range(0, values.shape[0], step)]
        return jnp.concatenate([lane_sums(part, width) for part in parts], 1)
    sums = dot(values, jnp.ones((LANES, rows), bf16))
    lane = iota((width, rows), 1)
    kept = [jnp.zeros((width, rows), f32)] * 4
    for t in range(rows):
        kept[t % 4] = jnp.where(lane == t, sums[t * width : (t + 1) * width], kept[t % 4])
    return (kept[0] + kept[1]) + (kept[2] + kept[3])


def live_rows(length, first, rows):
    return (iota((rows, 1), 0) + first < length).astype(f32)


def full(array):
    return pl.BlockSpec(array.shape, lambda *_: (0,) * len(array.shape))


class Rows:
    def __init__(self, maps, width, taps):
        self.maps = maps
        self.width = width
        self.taps = taps
        self.rank = maps - 2 * width
        self.first = maps + width
        self.count = -(-(self.first + taps + 3) // 16) * 16

    def x_w(self, ref):
        return ref[: self.maps, :]

    def a_log(self, ref):
        return ref[self.maps : self.first, :].astype(f32)

    def rest(self, ref):
        return ref[self.first :, :].astype(f32)


def front_kernel(lay, shards, pieces, order, place, tokens, gain, small, *refs):
    shard_refs = refs[:shards]
    piece_refs = refs[shards : shards + pieces]
    (
        normed_ref, w, input_ref, gate_ref, sum_ref, low_ref, map_ref, send_ref, halo, values,
    ) = refs[shards + pieces :]
    rows = normed_ref.shape[0]
    cut = tokens.shape[0]
    chans = small.shape[1]
    taps = lay.taps
    turn = pl.program_id(0)

    @pl.when(turn == 0)
    def _():
        for index in range(pieces):
            depth = piece_refs[index].shape[0]
            start = pl.multiple_of(place[index] * depth, depth)
            w[pl.ds(start, depth), :] = piece_refs[index][...]
        halo[:8] = jnp.zeros_like(halo[:8])

    for index in range(shards):

        @pl.when(order[turn] == index)
        def _(index=index):
            values[cut:] = shard_refs[index][...].astype(f32)

    values[:cut] = tokens[...].astype(f32)
    values = values[...]
    inverse = lax.rsqrt(jnp.mean(values * values, axis=-1, keepdims=True) + epsilon)
    normed = (values * inverse * gain[...]).astype(bf16)
    normed_ref[...] = normed
    projected = dot(normed, w[...])
    conv_in = projected[:, :chans]
    input_ref[...] = conv_in
    gate_ref[...] = projected[:, chans:]
    halo[8:] = conv_in
    rest = lay.rest(small)
    total = rest[taps : taps + 1]
    for tap in range(taps):
        first = 8 - taps + 1 + tap
        total = total + rest[tap : tap + 1] * halo[first : first + rows]
    halo[:8] = conv_in[rows - 8 :]
    sum_ref[...] = total
    low = (total * jax.nn.sigmoid(total)).astype(bf16)
    low_ref[...] = low
    mapped = dot(lay.x_w(small), low, NT)
    map_ref[...] = mapped
    send_ref[...] = mapped.astype(bf16)


def front(lay, order, place, tokens, shards, gain, small, pieces):
    count = len(shards)
    cut = tokens.shape[0] // count
    rows = cut + shards[0].shape[0]
    depth = tokens.shape[1]
    total = count * rows
    chans = small.shape[1]
    both = pieces[0].shape[1]
    row = lambda w: pl.BlockSpec((rows, w), lambda i, *_: (i, 0))
    column = lambda w: pl.BlockSpec((w, rows), lambda i, *_: (0, i))
    return pl.pallas_call(
        functools.partial(front_kernel, lay, count, len(pieces)),
        grid_spec=pltpu.PrefetchScalarGridSpec(
            num_scalar_prefetch=2,
            grid=(count,),
            in_specs=[pl.BlockSpec((cut, depth), lambda i, *_: (i, 0))]
            + [full(a) for a in (gain, small, *shards, *pieces)],
            out_specs=[row(depth), pl.BlockSpec((depth, both), lambda i, *_: (0, 0))]
            + [row(chans)] * 4
            + [column(lay.maps)] * 2,
            scratch_shapes=[pltpu.VMEM((rows + 8, chans), f32), pltpu.VMEM((rows, depth), f32)],
        ),
        out_shape=[
            shape((total, depth), bf16),
            shape((depth, both), bf16),
            shape((total, chans), f32),
            shape((total, chans), f32),
            shape((total, chans), f32),
            shape((total, chans), bf16),
            shape((lay.maps, total), f32),
            shape((lay.maps, total), bf16),
        ],
        compiler_params=params(),
        cost_estimate=cost(9),
        name="front",
    )(order, place, tokens, gain, small, *shards, *pieces)


def forward_kernel(
    lay, length, own, got, low, gate, dt_w, small, out_w,
    mixed_ref, before_ref, step_ref, h_ref, sent_ref, state, drive, lanes, step_rows, drive_rows,
):
    rows, chans = low.shape
    width, rank, taps = lay.width, lay.rank, lay.taps
    half = width // 2
    wide = STEPS * width

    @pl.when(pl.program_id(0) == 0)
    def _():
        state[...] = jnp.zeros_like(state)

    live = live_rows(length[0], pl.program_id(0) * rows, rows)
    mapped = own[...] + got[...].astype(f32)
    rest = lay.rest(small)
    step_pre = dot(mapped[:rank].astype(bf16), dt_w[...], TN) + rest[taps + 1 : taps + 2]
    step = jax.nn.softplus(step_pre) * live
    step_ref[...] = step
    conv_out = low[...].astype(f32)
    drive[...] = step * conv_out
    to_lanes(lanes, mapped[rank : rank + width])
    rate = -jnp.exp(lay.a_log(small)) * LOG2E
    rate_0, rate_1 = rate[:half], rate[half:]

    def body(block, carried):
        h_0, h_1 = carried
        s = pl.ds(pl.multiple_of(block * STEPS, STEPS), STEPS)
        step_rows[...] = step_ref[s, :]
        drive_rows[...] = drive[s, :]
        for k in range(STEPS):
            steps = row_of(step_rows, k, half)
            drives = row_of(drive_rows, k, half)
            base = pl.multiple_of(block * wide, wide) + k * width
            b_0 = across(lanes[pl.ds(base, half), :], chans)
            b_1 = across(lanes[pl.ds(base + half, half), :], chans)
            h_0 = jnp.exp2(steps * rate_0) * h_0 + drives * b_0
            h_1 = jnp.exp2(steps * rate_1) * h_1 + drives * b_1
            h_ref[pl.ds(base, width), :] = jnp.concatenate([h_0, h_1], 0).astype(bf16)
        return h_0, h_1

    h_0, h_1 = lax.fori_loop(0, rows // STEPS, body, (state[:half], state[half:]))
    state[:half] = h_0
    state[half:] = h_1
    outs = spread(mapped[rank + width :].astype(bf16))
    scan = [
        dot(outs[i * STEPS : (i + 1) * STEPS], h_ref[i * wide : (i + 1) * wide, :])
        for i in range(rows // STEPS)
    ]
    before = jnp.concatenate(scan, 0) + rest[taps + 2 : taps + 3] * conv_out
    before_ref[...] = before
    gates = gate[...]
    mixed = (before * (gates * jax.nn.sigmoid(gates)) * live).astype(bf16)
    mixed_ref[...] = mixed
    sent_ref[...] = dot(mixed, out_w[...]).astype(bf16)


def forward(lay, length, own, got, low, gate, dt_w, small, out_w):
    total, chans = low.shape
    depth = out_w.shape[1]
    width = lay.width
    row = lambda w: pl.BlockSpec((ROWS, w), lambda i, *_: (i, 0))
    column = lambda w: pl.BlockSpec((w, ROWS), lambda i, *_: (0, i))
    return pl.pallas_call(
        functools.partial(forward_kernel, lay),
        grid_spec=pltpu.PrefetchScalarGridSpec(
            num_scalar_prefetch=1,
            grid=(total // ROWS,),
            in_specs=[column(lay.maps), column(lay.maps), row(chans), row(chans)]
            + [full(a) for a in (dt_w, small, out_w)],
            out_specs=[
                row(chans),
                row(chans),
                row(chans),
                pl.BlockSpec((ROWS * width, chans), lambda i, *_: (i, 0)),
                row(depth),
            ],
            scratch_shapes=[
                pltpu.VMEM((width, chans), f32),
                pltpu.VMEM((ROWS, chans), f32),
                pltpu.VMEM((ROWS * width, LANES), f32),
                pltpu.VMEM((STEPS, chans), f32),
                pltpu.VMEM((STEPS, chans), f32),
            ],
        ),
        out_shape=[
            shape((total, chans), bf16),
            shape((total, chans), f32),
            shape((total, chans), f32),
            shape((total * width, chans), bf16),
            shape((total, depth), bf16),
        ],
        compiler_params=params(),
        cost_estimate=cost(24),
        name="forward",
    )(length, own, got, low, gate, dt_w, small, out_w)


def backward_kernel(
    lay, length, own, got, low, gate, before_ref, step_ref, grad, h_ref, last_ref, dt_w, small, out_w_t,
    map_ref, send_ref, out_ref, gate_ref, rate_ref, dt_w_ref, bias_ref,
    carry, grads, terms, drive, scan_grad, lanes, cross_b, cross_c, step_rows, drive_rows, grad_rows,
):
    rows, chans = low.shape
    width, rank, taps = lay.width, lay.rank, lay.taps
    half = width // 2
    wide = STEPS * width
    turn = pl.program_id(0)
    turns = pl.num_programs(0)

    @pl.when(turn == 0)
    def _():
        for ref in (carry, rate_ref, dt_w_ref, bias_ref):
            ref[...] = jnp.zeros_like(ref)

    live = live_rows(length[0], (turns - 1 - turn) * rows, rows)
    rest = lay.rest(small)
    conv_out = low[...].astype(f32)
    masked = dot(grad[...], out_w_t[...]) * live
    gates = gate[...]
    sigma = jax.nn.sigmoid(gates)
    gate_ref[...] = (
        masked * before_ref[...] * (sigma * (1.0 + gates * (1.0 - sigma)))
    ).astype(bf16)
    out_scan = masked * (gates * sigma)
    scan_grad[...] = out_scan
    bias_ref[1:2] += jnp.sum(out_scan * conv_out, axis=0, keepdims=True)
    mapped = own[...] + got[...].astype(f32)
    to_lanes(lanes, mapped[rank + width :])
    drive[...] = step_ref[...] * conv_out
    rate = -jnp.exp(lay.a_log(small)) * LOG2E
    rate_0, rate_1 = rate[:half], rate[half:]
    rate_low = rate.astype(bf16)
    first = jnp.where(turn == turns - 1, jnp.zeros_like(last_ref[...]), last_ref[...])

    def body(back, carried):
        q_0, q_1, total, h = carried
        block = rows // STEPS - 1 - back
        s = pl.ds(pl.multiple_of(block * STEPS, STEPS), STEPS)
        step_rows[...] = step_ref[s, :]
        drive_rows[...] = drive[s, :]
        grad_rows[...] = scan_grad[s, :]
        part = jnp.zeros((width, chans), bf16)
        for k in reversed(range(STEPS)):
            steps = row_of(step_rows, k, half)
            drives = row_of(drive_rows, k, half)
            outs = row_of(grad_rows, k, half)
            base = pl.multiple_of(block * wide, wide) + k * width
            g_0 = outs * across(lanes[pl.ds(base, half), :], chans) + q_0
            g_1 = outs * across(lanes[pl.ds(base + half, half), :], chans) + q_1
            g = jnp.concatenate([g_0, g_1], 0).astype(bf16)
            grads[pl.ds(base, width), :] = g
            cross_b[pl.ds(base, width), :] = fold(g * twice(drives))
            cross_c[pl.ds(base, width), :] = fold(h * twice(outs))
            q_0 = jnp.exp2(steps * rate_0) * g_0
            q_1 = jnp.exp2(steps * rate_1) * g_1
            if k == 0:
                start = pl.multiple_of(jnp.maximum(base - width, 0), width)
                h = jnp.where(block == 0, first, h_ref[pl.ds(start, width), :])
            else:
                h = h_ref[pl.ds(base - width, width), :]
            term = jnp.concatenate([q_0, q_1], 0).astype(bf16) * h * rate_low
            terms[pl.ds(base, width), :] = term
            part = part + twice(steps) * term
        return q_0, q_1, total + part.astype(f32), h

    start = (carry[:half], carry[half:], rate_ref[...], h_ref[(rows - 1) * width :, :])
    q_0, q_1, total, _ = lax.fori_loop(0, rows // STEPS, body, start)
    carry[:half] = q_0
    carry[half:] = q_1
    rate_ref[...] = total
    ins = spread(mapped[rank : rank + width].astype(bf16))
    ones = (iota((STEPS, wide), 1) // width == iota((STEPS, wide), 0)).astype(bf16)
    weighted, stepped = [], []
    for i in range(rows // STEPS):
        big = slice(i * wide, (i + 1) * wide)
        weighted.append(dot(ins[i * STEPS : (i + 1) * STEPS], grads[big, :]))
        stepped.append(dot(ones, terms[big, :]))
    weighted = jnp.concatenate(weighted, 0)
    step_grad = jnp.concatenate(stepped, 0) * LN2 + conv_out * weighted
    map_low = mapped[:rank].astype(bf16)
    step_pre = dot(map_low, dt_w[...], TN) + rest[taps + 1 : taps + 2]
    pre_grad = (step_grad * live * jax.nn.sigmoid(step_pre)).astype(bf16)
    bias_ref[0:1] += jnp.sum(pre_grad.astype(f32), axis=0, keepdims=True)
    dt_w_ref[...] += dot(map_low, pre_grad)
    map_grad = jnp.concatenate(
        [dot(dt_w[...], pre_grad, NT), lane_sums(cross_b[...], width), lane_sums(cross_c[...], width)],
        0,
    )
    map_ref[...] = map_grad
    send_ref[...] = map_grad.astype(bf16)
    out_ref[...] = out_scan * rest[taps + 2 : taps + 3] + step_ref[...] * weighted


def backward(lay, length, own, got, low, gate, before, step, grad, h, dt_w, small, out_w_t):
    total, chans = low.shape
    width = lay.width
    turns = total // ROWS
    at = lambda i: turns - 1 - i
    row = lambda w: pl.BlockSpec((ROWS, w), lambda i, *_: (at(i), 0))
    column = lambda w: pl.BlockSpec((w, ROWS), lambda i, *_: (0, at(i)))
    outs = [
        shape((lay.maps, total), f32),
        shape((lay.maps, total), bf16),
        shape((total, chans), f32),
        shape((total, chans), bf16),
        shape((width, chans), f32),
        shape(dt_w.shape, f32),
        shape((8, chans), f32),
    ]
    return pl.pallas_call(
        functools.partial(backward_kernel, lay),
        grid_spec=pltpu.PrefetchScalarGridSpec(
            num_scalar_prefetch=1,
            grid=(turns,),
            in_specs=[
                column(lay.maps),
                column(lay.maps),
                row(chans),
                row(chans),
                row(chans),
                row(chans),
                row(grad.shape[1]),
                pl.BlockSpec((ROWS * width, chans), lambda i, *_: (at(i), 0)),
                pl.BlockSpec((width, chans), lambda i, *_: (jnp.maximum(at(i) * ROWS - 1, 0), 0)),
            ]
            + [full(a) for a in (dt_w, small, out_w_t)],
            out_specs=[column(lay.maps), column(lay.maps), row(chans), row(chans)]
            + [full(a) for a in outs[4:]],
            scratch_shapes=[
                pltpu.VMEM((width, chans), f32),
                pltpu.VMEM((ROWS * width, chans), bf16),
                pltpu.VMEM((ROWS * width, chans), bf16),
                pltpu.VMEM((ROWS, chans), f32),
                pltpu.VMEM((ROWS, chans), f32),
                pltpu.VMEM((ROWS * width, LANES), f32),
                pltpu.VMEM((ROWS * width, LANES), bf16),
                pltpu.VMEM((ROWS * width, LANES), bf16),
                pltpu.VMEM((STEPS, chans), f32),
                pltpu.VMEM((STEPS, chans), f32),
                pltpu.VMEM((STEPS, chans), f32),
            ],
        ),
        out_shape=outs,
        compiler_params=params(),
        cost_estimate=cost(40),
        name="backward",
    )(length, own, got, low, gate, before, step, grad, h, h, dt_w, small, out_w_t)


def back_kernel(
    lay, own, got, small, out_grad, conv_sum, conv_in, low, gate_grad, w,
    part_ref, input_ref, x_ref, conv_ref, halo,
):
    rows, chans = low.shape
    taps = lay.taps
    turn = pl.program_id(0)

    @pl.when(turn == 0)
    def _():
        halo[rows:] = jnp.zeros_like(halo[rows:])
        for ref in (x_ref, conv_ref):
            ref[...] = jnp.zeros_like(ref)

    rest = lay.rest(small)
    map_grad = (own[...] + got[...].astype(f32)).astype(bf16)
    x_ref[...] += dot(map_grad, low[...])
    values = conv_sum[...]
    sigma = jax.nn.sigmoid(values)
    sum_grad = (out_grad[...] + dot(map_grad, lay.x_w(small), TN)) * (
        sigma * (1.0 + values * (1.0 - sigma))
    )
    conv_ref[taps : taps + 1] += jnp.sum(sum_grad, axis=0, keepdims=True)
    halo[:rows] = sum_grad
    inputs = conv_in[...]
    input_grad = jnp.zeros_like(inputs)
    for tap in range(taps):
        first = taps - 1 - tap
        moved = halo[first : first + rows]
        input_grad = input_grad + rest[tap : tap + 1] * moved
        conv_ref[tap : tap + 1] += jnp.sum(inputs * moved, axis=0, keepdims=True)
    halo[rows:] = sum_grad[:8]
    input_grad = input_grad.astype(bf16)
    input_ref[...] = input_grad
    part = dot(jnp.concatenate([input_grad, gate_grad[...]], 1), w[...], NT)
    part_ref[...] = part.astype(bf16)


def back(lay, own, got, small, out_grad, conv_sum, conv_in, low, gate_grad, w):
    total, chans = low.shape
    depth = w.shape[0]
    rows = 256
    count = total // rows
    at = lambda i: count - 1 - i
    row = lambda a: pl.BlockSpec((rows, a.shape[1]), lambda i: (at(i), 0))
    column = lambda a: pl.BlockSpec((a.shape[0], rows), lambda i: (0, at(i)))
    outs = [
        shape((total, depth), bf16),
        shape((total, chans), bf16),
        shape((lay.maps, chans), f32),
        shape((8, chans), f32),
    ]
    return pl.pallas_call(
        functools.partial(back_kernel, lay),
        grid=(count,),
        in_specs=[
            column(own),
            column(got),
            full(small),
            row(out_grad),
            row(conv_sum),
            row(conv_in),
            row(low),
            row(gate_grad),
            full(w),
        ],
        out_specs=[row(outs[0]), row(outs[1]), full(outs[2]), full(outs[3])],
        out_shape=outs,
        scratch_shapes=[pltpu.VMEM((rows + 8, chans), f32)],
        compiler_params=params(),
        cost_estimate=cost(11),
        name="back",
    )(own, got, small, out_grad, conv_sum, conv_in, low, gate_grad, w)


def weights_kernel(pairs, half, place, *refs):
    lefts, rights = refs[:pairs], refs[pairs : 2 * pairs]
    w, keep_ref, send_ref, gain_ref, total = refs[2 * pairs :]
    chans = rights[0].shape[1]
    depth = keep_ref.shape[2]
    for i in range(pairs):
        values = dot(lefts[i][...], rights[i][...], TN)
        total[...] = values
        if i == 0:
            product = values * w[:, half * chans : (half + 1) * chans].astype(f32)
            gain_ref[...] = dot(jnp.ones((8, chans), bf16), product.astype(bf16), NT)
        for index in range(2 * keep_ref.shape[0]):
            start = pl.multiple_of(place[index] * depth, depth)
            piece = total[pl.ds(start, depth), :].astype(bf16)
            (send_ref if index % 2 else keep_ref)[index // 2, i] = piece


def weights(place, half, lefts, rights, w):
    depth = w.shape[0]
    chans = rights[0].shape[1]
    size = place.shape[0]
    piece = shape((size // 2, len(lefts), depth // size, chans), bf16)
    outs = [piece, piece, shape((8, depth), f32)]
    return pl.pallas_call(
        functools.partial(weights_kernel, len(lefts), half),
        grid_spec=pltpu.PrefetchScalarGridSpec(
            num_scalar_prefetch=1,
            grid=(1,),
            in_specs=[full(a) for a in (*lefts, *rights, w)],
            out_specs=[full(a) for a in outs],
            scratch_shapes=[pltpu.VMEM((depth, chans), f32)],
        ),
        out_shape=outs,
        compiler_params=params(),
        cost_estimate=cost(3 * len(lefts)),
        name="weights",
    )(place, *lefts, *rights, w)


def last_kernel(tokens, grad, normed_grad, gain, out_ref):
    values = tokens[...].astype(f32)
    inverse = lax.rsqrt(jnp.mean(values * values, axis=-1, keepdims=True) + epsilon)
    hat = values * inverse
    scaled = normed_grad[...].astype(f32) * gain[...]
    out_ref[...] = grad[...].astype(f32) + inverse * (
        scaled - hat * jnp.mean(scaled * hat, axis=-1, keepdims=True)
    )


def last(tokens, grad, normed_grad, gain):
    total, depth = tokens.shape
    rows = min(128, total)
    row = pl.BlockSpec((rows, depth), lambda i: (i, 0))
    return pl.pallas_call(
        last_kernel,
        grid=(total // rows,),
        in_specs=[row, row, row, full(gain)],
        out_specs=row,
        out_shape=shape((total, depth), f32),
        compiler_params=params(),
        cost_estimate=cost(2),
        name="last",
    )(tokens, grad, normed_grad, gain)


def exchange(values, axis, size, bits):
    return lax.ppermute(values, axis, [(i, i ^ bits) for i in range(size)])


def even_pieces(values, axis, size):
    return [values] + [exchange(values, axis, size, m) for m in range(2, size, 2)]


def all_pieces(even, axis, size):
    odd = [exchange(piece, axis, size, 1) for piece in even]
    return [piece for pair in zip(even, odd) for piece in pair]


def pair_sum(keep, send, axis, size):
    return keep + exchange(send, axis, size, 1)


def chip_terms(summed, axis, size):
    return [summed[0]] + [exchange(summed[m], axis, size, 2 * m) for m in range(1, size // 2)]


def total(terms):
    return sum(term.astype(f32) for term in terms)


def sum_all(values, send, axis, size, beside):
    bits = 1
    while bits < size:
        got = exchange(send, axis, size, 2 * bits - 1)
        if bits == 1:
            got, beside = lax.optimization_barrier((got, beside))
        bits *= 2
        if bits < size:
            values = values + got.astype(f32)
            send = values.astype(bf16)
    return values, got, beside


def shards(
    fsdp, tp, tokens, lengths, norm_gain, in_weight, conv_weight, conv_bias, x_weight, dt_weight,
    dt_bias, a_log, d_skip, out_weight, cotangent,
):
    fs_me = lax.axis_index("fsdp")
    place = (fs_me ^ jnp.arange(fsdp)).astype(jnp.int32)
    depth = tokens.shape[2]
    part = conv_weight.shape[1]
    chans = part * fsdp
    lay = Rows(x_weight.shape[1], a_log.shape[0], conv_weight.shape[0])
    maps, width, taps, rank, first = lay.maps, lay.width, lay.taps, lay.rank, lay.first

    cut = tokens.shape[1] * 3 // 4
    whole = lax.all_gather(tokens[0, :cut], "tp", axis=0, tiled=True)
    order = ((lax.axis_index("tp") - jnp.arange(tp)) % tp).astype(jnp.int32)
    direct = [tokens[0, cut:]] + [
        lax.ppermute(tokens[0, cut:], "tp", [(i, (i + k) % tp) for i in range(tp)])
        for k in range(1, tp)
    ]
    even = even_pieces(in_weight.reshape(in_weight.shape[0], 2 * chans), "fsdp", fsdp)
    even, direct, x_weight, a_log, conv_weight, conv_bias, dt_bias, d_skip, dt_weight, gain_part = (
        lax.optimization_barrier(
            (
                even, direct, x_weight, a_log, conv_weight, conv_bias, dt_bias, d_skip, dt_weight,
                norm_gain,
            )
        )
    )
    pieces = all_pieces(even_pieces(out_weight, "fsdp", fsdp), "fsdp", fsdp)
    ordered = jnp.stack(pieces)[place]
    out_w = ordered.transpose(1, 0, 2).reshape(chans, depth)
    out_w_t = ordered.transpose(0, 2, 1).reshape(depth, chans)
    packed = jnp.concatenate(
        [
            x_weight.T,
            a_log,
            conv_weight,
            conv_bias[None],
            dt_bias[None],
            d_skip[None],
            jnp.zeros((lay.count - first - taps - 3, part), bf16),
            dt_weight.reshape(-1, part),
            gain_part.reshape(-1, part),
        ],
        0,
    )
    gathered = lax.all_gather(packed, "fsdp", axis=0)
    w_pieces = all_pieces(even, "fsdp", fsdp)
    gathered, w_pieces = lax.optimization_barrier((gathered, w_pieces))
    small = gathered[:, : lay.count].transpose(1, 0, 2).reshape(lay.count, chans)
    dt_rows = dt_weight.size // part
    dt_w = gathered[:, lay.count : lay.count + dt_rows].reshape(rank, chans)
    gain = gathered[:, lay.count + dt_rows :].reshape(1, depth).astype(f32)

    normed, w, conv_in, gate, conv_sum, low, map_part, map_send = front(
        lay, order, place, whole, direct, gain, small, w_pieces
    )
    own, got, (held, out_w, out_w_t) = sum_all(
        map_part, map_send, "tp", tp, (cotangent[0], out_w, out_w_t)
    )
    grad_whole = lax.all_gather(held, "tp", axis=0, tiled=True)
    mixed, before, step, h, sent = forward(
        lay, lengths, own, got, low, gate, dt_w, small, out_w
    )
    block_sum = lax.psum_scatter(sent, "tp", scatter_dimension=0, tiled=True)

    map_part, map_send, conv_grad, gate_grad, rate_grad, dt_w_grad, bias_grad = backward(
        lay, lengths, own, got, low, gate, before, step, grad_whole, h, dt_w, small, out_w_t
    )
    *out_one, _ = weights(place, 0, (grad_whole,), (mixed,), w)
    own_grad, got_grad, (held, out_one) = sum_all(
        map_part, map_send, "tp", tp, (gate_grad, out_one)
    )
    *gate_one, gain_two = weights(place, 1, (normed,), (held,), w)
    out_pairs = pair_sum(*out_one, "fsdp", fsdp)
    own_grad, got_grad, gate_one, out_pairs = lax.optimization_barrier(
        (own_grad, got_grad, gate_one, out_pairs)
    )
    normed_part, input_grad, x_w_grad, taps_grad = back(
        lay, own_grad, got_grad, small, conv_grad, conv_sum, conv_in, low, gate_grad, w
    )
    normed_grad = lax.psum_scatter(normed_part, "tp", scatter_dimension=0, tiled=True)
    *one, gain_one = weights(place, 0, (normed,), (input_grad,), w)
    out_terms = chip_terms(out_pairs, "fsdp", fsdp)
    gate_terms = chip_terms(pair_sum(*gate_one, "fsdp", fsdp), "fsdp", fsdp)
    x_w_grad, taps_grad, out_terms, gate_terms = lax.optimization_barrier(
        (x_w_grad, taps_grad, out_terms, gate_terms)
    )
    conv_terms = chip_terms(pair_sum(*one, "fsdp", fsdp), "fsdp", fsdp)
    gain_grad = gain_one[:1] + gain_two[:1]
    bits = 1
    while bits < tp:
        gain_grad = gain_grad + exchange(gain_grad, "tp", tp, 2 * bits - 1)
        bits *= 2
    rows = jnp.concatenate(
        [x_w_grad, rate_grad * LN2, taps_grad[: taps + 1], bias_grad[:2]], 0
    ).astype(bf16)
    top = rows.shape[0]
    packed = jnp.concatenate(
        [
            rows.reshape(top, fsdp, part).transpose(1, 0, 2),
            dt_w_grad.astype(bf16).reshape(fsdp, -1, part),
            gain_grad.astype(bf16).reshape(fsdp, -1, part),
        ],
        1,
    )[place]
    pairs = pair_sum(packed[0::2], packed[1::2], "fsdp", fsdp)
    small_terms = chip_terms(pairs, "fsdp", fsdp)
    out_terms, gate_terms, conv_terms, small_terms, block_sum = lax.optimization_barrier(
        (out_terms, gate_terms, conv_terms, small_terms, block_sum)
    )
    small_grad = total(small_terms)
    out_weight_grad = total(out_terms)[0].T
    in_weight_grad = jnp.stack([total(conv_terms)[0], total(gate_terms)[0]], 1)
    block_out = (tokens.astype(f32) + block_sum[None].astype(f32)).astype(bf16)
    gain_out = small_grad[top + dt_rows :].reshape(-1) / norm_gain.astype(f32)

    input_grads = last(tokens[0], cotangent[0], normed_grad, gain)[None]
    return (
        block_out,
        input_grads,
        gain_out,
        in_weight_grad,
        small_grad[first : first + taps],
        small_grad[first + taps],
        small_grad[:maps].T,
        small_grad[top : top + dt_rows].reshape(-1, chans),
        small_grad[first + taps + 1],
        small_grad[maps:first],
        small_grad[first + taps + 2],
        out_weight_grad,
    )


def solution(mesh):
    sizes = dict(mesh.shape)
    return jax.shard_map(
        functools.partial(shards, sizes["fsdp"], sizes["tp"]),
        mesh=mesh,
        in_specs=(
            P("fsdp", "tp", None),
            P("fsdp"),
            P("fsdp"),
            P("fsdp", None, "tp"),
            P(None, ("tp", "fsdp")),
            P(("tp", "fsdp")),
            P(("tp", "fsdp"), None),
            P("fsdp", "tp"),
            P(("tp", "fsdp")),
            P(None, ("tp", "fsdp")),
            P(("tp", "fsdp")),
            P("tp", "fsdp"),
            P("fsdp", "tp", None),
        ),
        out_specs=(
            P("fsdp", "tp", None),
            P("fsdp", "tp", None),
            P("fsdp"),
            P("fsdp", None, "tp"),
            P(None, ("tp", "fsdp")),
            P(("tp", "fsdp")),
            P(("tp", "fsdp"), None),
            P("fsdp", "tp"),
            P(("tp", "fsdp")),
            P(None, ("tp", "fsdp")),
            P(("tp", "fsdp")),
            P("tp", "fsdp"),
        ),
        check_vma=False,
    )
```

```python
import functools

import jax
import jax.numpy as jnp
from jax import lax
from jax.experimental import pallas as pl
from jax.experimental.pallas import tpu as pltpu
from jax.sharding import PartitionSpec as P

bf16 = jnp.bfloat16
f32 = jnp.float32
LOG2E = 1.4426950408889634
LN2 = 0.6931471805599453
ROWS = 256
STEPS = 16
LANES = 128
SCALE = 1.0
NT = (((1,), (1,)), ((), ()))
TN = (((0,), (0,)), ((), ()))
epsilon = 1e-05
VMEM_LIMIT = 56 * 2**20


def dot(a, b, dims=(((1,), (0,)), ((), ()))):
    return lax.dot_general(a, b, dims, preferred_element_type=f32)


def shape(dims, kind):
    return jax.ShapeDtypeStruct(dims, kind)


def iota(dims, axis):
    return lax.broadcasted_iota(jnp.int32, dims, axis)


def params():
    return pltpu.CompilerParams(vmem_limit_bytes=VMEM_LIMIT)


def cost(micros):
    return pl.CostEstimate(
        flops=int(micros * SCALE * 1e9), bytes_accessed=int(micros * SCALE * 3e6), transcendentals=0
    )


def halves(values):
    high = values.astype(bf16)
    return high, (values - high.astype(f32)).astype(bf16)


def spread(columns):
    width, rows = columns.shape
    wide = STEPS * width
    pick = (iota((width, wide), 1) % width == iota((width, wide), 0)).astype(bf16)
    keep = iota((rows, wide), 1) // width == iota((rows, wide), 0) % STEPS
    return jnp.where(keep, dot(columns, pick, TN), 0.0).astype(bf16)


def to_lanes(target, columns):
    width, rows = columns.shape
    wide = STEPS * width
    parts = [spread(part) for part in halves(columns)]
    ones = jnp.ones((2 * STEPS, LANES), bf16)
    for index in range(rows // STEPS):
        s = slice(index * STEPS, (index + 1) * STEPS)
        both = jnp.concatenate([part[s] for part in parts], 0)
        target[index * wide : (index + 1) * wide, :] = dot(both, ones, TN)


def across(values, chans):
    return jnp.concatenate([values] * (chans // LANES), 1)


def row_of(ref, index, count):
    return ref[pl.ds(index, count, stride=0), :]


def twice(values):
    return jnp.concatenate([values, values], 0).astype(bf16)


def fold(values):
    return sum(values[:, i : i + LANES] for i in range(0, values.shape[1], LANES))


def lane_sums(values, width):
    rows = values.shape[0] // width
    if rows > LANES:
        step = LANES * width
        parts = [values[i : i + step] for i in range(0, values.shape[0], step)]
        return jnp.concatenate([lane_sums(part, width) for part in parts], 1)
    sums = dot(values, jnp.ones((LANES, rows), bf16))
    lane = iota((width, rows), 1)
    kept = [jnp.zeros((width, rows), f32)] * 4
    for t in range(rows):
        kept[t % 4] = jnp.where(lane == t, sums[t * width : (t + 1) * width], kept[t % 4])
    return (kept[0] + kept[1]) + (kept[2] + kept[3])


def live_rows(length, first, rows):
    return (iota((rows, 1), 0) + first < length).astype(f32)


def full(array):
    return pl.BlockSpec(array.shape, lambda *_: (0,) * len(array.shape))


class Rows:
    def __init__(self, maps, width, taps):
        self.maps = maps
        self.width = width
        self.taps = taps
        self.rank = maps - 2 * width
        self.first = maps + width
        self.count = -(-(self.first + taps + 3) // 16) * 16

    def x_w(self, ref):
        return ref[: self.maps, :]

    def a_log(self, ref):
        return ref[self.maps : self.first, :].astype(f32)

    def rest(self, ref):
        return ref[self.first :, :].astype(f32)


def front_kernel(lay, shards, pieces, order, place, tokens, gain, small, *refs):
    shard_refs = refs[:shards]
    piece_refs = refs[shards : shards + pieces]
    (
        normed_ref, w, input_ref, gate_ref, sum_ref, low_ref, map_ref, send_ref, halo, values,
    ) = refs[shards + pieces :]
    rows = normed_ref.shape[0]
    cut = tokens.shape[0]
    chans = small.shape[1]
    taps = lay.taps
    turn = pl.program_id(0)

    @pl.when(turn == 0)
    def _():
        for index in range(pieces):
            depth = piece_refs[index].shape[0]
            start = pl.multiple_of(place[index] * depth, depth)
            w[pl.ds(start, depth), :] = piece_refs[index][...]
        halo[:8] = jnp.zeros_like(halo[:8])

    for index in range(shards):

        @pl.when(order[turn] == index)
        def _(index=index):
            values[cut:] = shard_refs[index][...].astype(f32)

    values[:cut] = tokens[...].astype(f32)
    values = values[...]
    inverse = lax.rsqrt(jnp.mean(values * values, axis=-1, keepdims=True) + epsilon)
    normed = (values * inverse * gain[...]).astype(bf16)
    normed_ref[...] = normed
    projected = dot(normed, w[...])
    conv_in = projected[:, :chans]
    input_ref[...] = conv_in
    gate_ref[...] = projected[:, chans:]
    halo[8:] = conv_in
    rest = lay.rest(small)
    total = rest[taps : taps + 1]
    for tap in range(taps):
        first = 8 - taps + 1 + tap
        total = total + rest[tap : tap + 1] * halo[first : first + rows]
    halo[:8] = conv_in[rows - 8 :]
    sum_ref[...] = total
    low = (total * jax.nn.sigmoid(total)).astype(bf16)
    low_ref[...] = low
    mapped = dot(lay.x_w(small), low, NT)
    map_ref[...] = mapped
    send_ref[...] = mapped.astype(bf16)


def front(lay, order, place, tokens, shards, gain, small, pieces):
    count = len(shards)
    cut = tokens.shape[0] // count
    rows = cut + shards[0].shape[0]
    depth = tokens.shape[1]
    total = count * rows
    chans = small.shape[1]
    both = pieces[0].shape[1]
    row = lambda w: pl.BlockSpec((rows, w), lambda i, *_: (i, 0))
    column = lambda w: pl.BlockSpec((w, rows), lambda i, *_: (0, i))
    return pl.pallas_call(
        functools.partial(front_kernel, lay, count, len(pieces)),
        grid_spec=pltpu.PrefetchScalarGridSpec(
            num_scalar_prefetch=2,
            grid=(count,),
            in_specs=[pl.BlockSpec((cut, depth), lambda i, *_: (i, 0))]
            + [full(a) for a in (gain, small, *shards, *pieces)],
            out_specs=[row(depth), pl.BlockSpec((depth, both), lambda i, *_: (0, 0))]
            + [row(chans)] * 4
            + [column(lay.maps)] * 2,
            scratch_shapes=[pltpu.VMEM((rows + 8, chans), f32), pltpu.VMEM((rows, depth), f32)],
        ),
        out_shape=[
            shape((total, depth), bf16),
            shape((depth, both), bf16),
            shape((total, chans), f32),
            shape((total, chans), f32),
            shape((total, chans), f32),
            shape((total, chans), bf16),
            shape((lay.maps, total), f32),
            shape((lay.maps, total), bf16),
        ],
        compiler_params=params(),
        cost_estimate=cost(9),
        name="front",
    )(order, place, tokens, gain, small, *shards, *pieces)


def forward_kernel(
    lay, length, own, got, low, gate, dt_w, small, out_w,
    mixed_ref, before_ref, step_ref, h_ref, sent_ref, state, drive, lanes, step_rows, drive_rows,
):
    rows, chans = low.shape
    width, rank, taps = lay.width, lay.rank, lay.taps
    half = width // 2
    wide = STEPS * width

    @pl.when(pl.program_id(0) == 0)
    def _():
        state[...] = jnp.zeros_like(state)

    live = live_rows(length[0], pl.program_id(0) * rows, rows)
    mapped = own[...] + got[...].astype(f32)
    rest = lay.rest(small)
    step_pre = dot(mapped[:rank].astype(bf16), dt_w[...], TN) + rest[taps + 1 : taps + 2]
    step = jax.nn.softplus(step_pre) * live
    step_ref[...] = step
    conv_out = low[...].astype(f32)
    drive[...] = step * conv_out
    to_lanes(lanes, mapped[rank : rank + width])
    rate = -jnp.exp(lay.a_log(small)) * LOG2E
    rate_0, rate_1 = rate[:half], rate[half:]

    def body(block, carried):
        h_0, h_1 = carried
        s = pl.ds(pl.multiple_of(block * STEPS, STEPS), STEPS)
        step_rows[...] = step_ref[s, :]
        drive_rows[...] = drive[s, :]
        for k in range(STEPS):
            steps = row_of(step_rows, k, half)
            drives = row_of(drive_rows, k, half)
            base = pl.multiple_of(block * wide, wide) + k * width
            b_0 = across(lanes[pl.ds(base, half), :], chans)
            b_1 = across(lanes[pl.ds(base + half, half), :], chans)
            h_0 = jnp.exp2(steps * rate_0) * h_0 + drives * b_0
            h_1 = jnp.exp2(steps * rate_1) * h_1 + drives * b_1
            h_ref[pl.ds(base, width), :] = jnp.concatenate([h_0, h_1], 0).astype(bf16)
        return h_0, h_1

    h_0, h_1 = lax.fori_loop(0, rows // STEPS, body, (state[:half], state[half:]))
    state[:half] = h_0
    state[half:] = h_1
    outs = spread(mapped[rank + width :].astype(bf16))
    scan = [
        dot(outs[i * STEPS : (i + 1) * STEPS], h_ref[i * wide : (i + 1) * wide, :])
        for i in range(rows // STEPS)
    ]
    before = jnp.concatenate(scan, 0) + rest[taps + 2 : taps + 3] * conv_out
    before_ref[...] = before
    gates = gate[...]
    mixed = (before * (gates * jax.nn.sigmoid(gates)) * live).astype(bf16)
    mixed_ref[...] = mixed
    sent_ref[...] = dot(mixed, out_w[...]).astype(bf16)


def forward(lay, length, own, got, low, gate, dt_w, small, out_w):
    total, chans = low.shape
    depth = out_w.shape[1]
    width = lay.width
    row = lambda w: pl.BlockSpec((ROWS, w), lambda i, *_: (i, 0))
    column = lambda w: pl.BlockSpec((w, ROWS), lambda i, *_: (0, i))
    return pl.pallas_call(
        functools.partial(forward_kernel, lay),
        grid_spec=pltpu.PrefetchScalarGridSpec(
            num_scalar_prefetch=1,
            grid=(total // ROWS,),
            in_specs=[column(lay.maps), column(lay.maps), row(chans), row(chans)]
            + [full(a) for a in (dt_w, small, out_w)],
            out_specs=[
                row(chans),
                row(chans),
                row(chans),
                pl.BlockSpec((ROWS * width, chans), lambda i, *_: (i, 0)),
                row(depth),
            ],
            scratch_shapes=[
                pltpu.VMEM((width, chans), f32),
                pltpu.VMEM((ROWS, chans), f32),
                pltpu.VMEM((ROWS * width, LANES), f32),
                pltpu.VMEM((STEPS, chans), f32),
                pltpu.VMEM((STEPS, chans), f32),
            ],
        ),
        out_shape=[
            shape((total, chans), bf16),
            shape((total, chans), f32),
            shape((total, chans), f32),
            shape((total * width, chans), bf16),
            shape((total, depth), bf16),
        ],
        compiler_params=params(),
        cost_estimate=cost(24),
        name="forward",
    )(length, own, got, low, gate, dt_w, small, out_w)


def backward_kernel(
    lay, length, own, got, low, gate, before_ref, step_ref, grad, h_ref, last_ref, dt_w, small, out_w_t,
    map_ref, send_ref, out_ref, gate_ref, rate_ref, dt_w_ref, bias_ref,
    carry, grads, terms, drive, scan_grad, lanes, cross_b, cross_c, step_rows, drive_rows, grad_rows,
):
    rows, chans = low.shape
    width, rank, taps = lay.width, lay.rank, lay.taps
    half = width // 2
    wide = STEPS * width
    turn = pl.program_id(0)
    turns = pl.num_programs(0)

    @pl.when(turn == 0)
    def _():
        for ref in (carry, rate_ref, dt_w_ref, bias_ref):
            ref[...] = jnp.zeros_like(ref)

    live = live_rows(length[0], (turns - 1 - turn) * rows, rows)
    rest = lay.rest(small)
    conv_out = low[...].astype(f32)
    masked = dot(grad[...], out_w_t[...]) * live
    gates = gate[...]
    sigma = jax.nn.sigmoid(gates)
    gate_ref[...] = (
        masked * before_ref[...] * (sigma * (1.0 + gates * (1.0 - sigma)))
    ).astype(bf16)
    out_scan = masked * (gates * sigma)
    scan_grad[...] = out_scan
    bias_ref[1:2] += jnp.sum(out_scan * conv_out, axis=0, keepdims=True)
    mapped = own[...] + got[...].astype(f32)
    to_lanes(lanes, mapped[rank + width :])
    drive[...] = step_ref[...] * conv_out
    rate = -jnp.exp(lay.a_log(small)) * LOG2E
    rate_0, rate_1 = rate[:half], rate[half:]
    rate_low = rate.astype(bf16)
    first = jnp.where(turn == turns - 1, jnp.zeros_like(last_ref[...]), last_ref[...])

    def body(back, carried):
        q_0, q_1, total, h = carried
        block = rows // STEPS - 1 - back
        s = pl.ds(pl.multiple_of(block * STEPS, STEPS), STEPS)
        step_rows[...] = step_ref[s, :]
        drive_rows[...] = drive[s, :]
        grad_rows[...] = scan_grad[s, :]
        part = jnp.zeros((width, chans), bf16)
        for k in reversed(range(STEPS)):
            steps = row_of(step_rows, k, half)
            drives = row_of(drive_rows, k, half)
            outs = row_of(grad_rows, k, half)
            base = pl.multiple_of(block * wide, wide) + k * width
            g_0 = outs * across(lanes[pl.ds(base, half), :], chans) + q_0
            g_1 = outs * across(lanes[pl.ds(base + half, half), :], chans) + q_1
            g = jnp.concatenate([g_0, g_1], 0).astype(bf16)
            grads[pl.ds(base, width), :] = g
            cross_b[pl.ds(base, width), :] = fold(g * twice(drives))
            cross_c[pl.ds(base, width), :] = fold(h * twice(outs))
            q_0 = jnp.exp2(steps * rate_0) * g_0
            q_1 = jnp.exp2(steps * rate_1) * g_1
            if k == 0:
                start = pl.multiple_of(jnp.maximum(base - width, 0), width)
                h = jnp.where(block == 0, first, h_ref[pl.ds(start, width), :])
            else:
                h = h_ref[pl.ds(base - width, width), :]
            term = jnp.concatenate([q_0, q_1], 0).astype(bf16) * h * rate_low
            terms[pl.ds(base, width), :] = term
            part = part + twice(steps) * term
        return q_0, q_1, total + part.astype(f32), h

    start = (carry[:half], carry[half:], rate_ref[...], h_ref[(rows - 1) * width :, :])
    q_0, q_1, total, _ = lax.fori_loop(0, rows // STEPS, body, start)
    carry[:half] = q_0
    carry[half:] = q_1
    rate_ref[...] = total
    ins = spread(mapped[rank : rank + width].astype(bf16))
    ones = (iota((STEPS, wide), 1) // width == iota((STEPS, wide), 0)).astype(bf16)
    weighted, stepped = [], []
    for i in range(rows // STEPS):
        big = slice(i * wide, (i + 1) * wide)
        weighted.append(dot(ins[i * STEPS : (i + 1) * STEPS], grads[big, :]))
        stepped.append(dot(ones, terms[big, :]))
    weighted = jnp.concatenate(weighted, 0)
    step_grad = jnp.concatenate(stepped, 0) * LN2 + conv_out * weighted
    map_low = mapped[:rank].astype(bf16)
    step_pre = dot(map_low, dt_w[...], TN) + rest[taps + 1 : taps + 2]
    pre_grad = (step_grad * live * jax.nn.sigmoid(step_pre)).astype(bf16)
    bias_ref[0:1] += jnp.sum(pre_grad.astype(f32), axis=0, keepdims=True)
    dt_w_ref[...] += dot(map_low, pre_grad)
    map_grad = jnp.concatenate(
        [dot(dt_w[...], pre_grad, NT), lane_sums(cross_b[...], width), lane_sums(cross_c[...], width)],
        0,
    )
    map_ref[...] = map_grad
    send_ref[...] = map_grad.astype(bf16)
    out_ref[...] = out_scan * rest[taps + 2 : taps + 3] + step_ref[...] * weighted


def backward(lay, length, own, got, low, gate, before, step, grad, h, dt_w, small, out_w_t):
    total, chans = low.shape
    width = lay.width
    turns = total // ROWS
    at = lambda i: turns - 1 - i
    row = lambda w: pl.BlockSpec((ROWS, w), lambda i, *_: (at(i), 0))
    column = lambda w: pl.BlockSpec((w, ROWS), lambda i, *_: (0, at(i)))
    outs = [
        shape((lay.maps, total), f32),
        shape((lay.maps, total), bf16),
        shape((total, chans), f32),
        shape((total, chans), bf16),
        shape((width, chans), f32),
        shape(dt_w.shape, f32),
        shape((8, chans), f32),
    ]
    return pl.pallas_call(
        functools.partial(backward_kernel, lay),
        grid_spec=pltpu.PrefetchScalarGridSpec(
            num_scalar_prefetch=1,
            grid=(turns,),
            in_specs=[
                column(lay.maps),
                column(lay.maps),
                row(chans),
                row(chans),
                row(chans),
                row(chans),
                row(grad.shape[1]),
                pl.BlockSpec((ROWS * width, chans), lambda i, *_: (at(i), 0)),
                pl.BlockSpec((width, chans), lambda i, *_: (jnp.maximum(at(i) * ROWS - 1, 0), 0)),
            ]
            + [full(a) for a in (dt_w, small, out_w_t)],
            out_specs=[column(lay.maps), column(lay.maps), row(chans), row(chans)]
            + [full(a) for a in outs[4:]],
            scratch_shapes=[
                pltpu.VMEM((width, chans), f32),
                pltpu.VMEM((ROWS * width, chans), bf16),
                pltpu.VMEM((ROWS * width, chans), bf16),
                pltpu.VMEM((ROWS, chans), f32),
                pltpu.VMEM((ROWS, chans), f32),
                pltpu.VMEM((ROWS * width, LANES), f32),
                pltpu.VMEM((ROWS * width, LANES), bf16),
                pltpu.VMEM((ROWS * width, LANES), bf16),
                pltpu.VMEM((STEPS, chans), f32),
                pltpu.VMEM((STEPS, chans), f32),
                pltpu.VMEM((STEPS, chans), f32),
            ],
        ),
        out_shape=outs,
        compiler_params=params(),
        cost_estimate=cost(40),
        name="backward",
    )(length, own, got, low, gate, before, step, grad, h, h, dt_w, small, out_w_t)


def back_kernel(
    lay, own, got, small, out_grad, conv_sum, conv_in, low, gate_grad, w,
    part_ref, input_ref, x_ref, conv_ref, halo,
):
    rows, chans = low.shape
    taps = lay.taps
    turn = pl.program_id(0)

    @pl.when(turn == 0)
    def _():
        halo[rows:] = jnp.zeros_like(halo[rows:])
        for ref in (x_ref, conv_ref):
            ref[...] = jnp.zeros_like(ref)

    rest = lay.rest(small)
    map_grad = (own[...] + got[...].astype(f32)).astype(bf16)
    x_ref[...] += dot(map_grad, low[...])
    values = conv_sum[...]
    sigma = jax.nn.sigmoid(values)
    sum_grad = (out_grad[...] + dot(map_grad, lay.x_w(small), TN)) * (
        sigma * (1.0 + values * (1.0 - sigma))
    )
    conv_ref[taps : taps + 1] += jnp.sum(sum_grad, axis=0, keepdims=True)
    halo[:rows] = sum_grad
    inputs = conv_in[...]
    input_grad = jnp.zeros_like(inputs)
    for tap in range(taps):
        first = taps - 1 - tap
        moved = halo[first : first + rows]
        input_grad = input_grad + rest[tap : tap + 1] * moved
        conv_ref[tap : tap + 1] += jnp.sum(inputs * moved, axis=0, keepdims=True)
    halo[rows:] = sum_grad[:8]
    input_grad = input_grad.astype(bf16)
    input_ref[...] = input_grad
    part = dot(jnp.concatenate([input_grad, gate_grad[...]], 1), w[...], NT)
    part_ref[...] = part.astype(bf16)


def back(lay, own, got, small, out_grad, conv_sum, conv_in, low, gate_grad, w):
    total, chans = low.shape
    depth = w.shape[0]
    rows = 256
    count = total // rows
    at = lambda i: count - 1 - i
    row = lambda a: pl.BlockSpec((rows, a.shape[1]), lambda i: (at(i), 0))
    column = lambda a: pl.BlockSpec((a.shape[0], rows), lambda i: (0, at(i)))
    outs = [
        shape((total, depth), bf16),
        shape((total, chans), bf16),
        shape((lay.maps, chans), f32),
        shape((8, chans), f32),
    ]
    return pl.pallas_call(
        functools.partial(back_kernel, lay),
        grid=(count,),
        in_specs=[
            column(own),
            column(got),
            full(small),
            row(out_grad),
            row(conv_sum),
            row(conv_in),
            row(low),
            row(gate_grad),
            full(w),
        ],
        out_specs=[row(outs[0]), row(outs[1]), full(outs[2]), full(outs[3])],
        out_shape=outs,
        scratch_shapes=[pltpu.VMEM((rows + 8, chans), f32)],
        compiler_params=params(),
        cost_estimate=cost(11),
        name="back",
    )(own, got, small, out_grad, conv_sum, conv_in, low, gate_grad, w)


def weights_kernel(pairs, half, place, *refs):
    lefts, rights = refs[:pairs], refs[pairs : 2 * pairs]
    w, keep_ref, send_ref, gain_ref, total = refs[2 * pairs :]
    chans = rights[0].shape[1]
    depth = keep_ref.shape[2]
    for i in range(pairs):
        values = dot(lefts[i][...], rights[i][...], TN)
        total[...] = values
        if i == 0:
            product = values * w[:, half * chans : (half + 1) * chans].astype(f32)
            gain_ref[...] = dot(jnp.ones((8, chans), bf16), product.astype(bf16), NT)
        for index in range(2 * keep_ref.shape[0]):
            start = pl.multiple_of(place[index] * depth, depth)
            piece = total[pl.ds(start, depth), :].astype(bf16)
            (send_ref if index % 2 else keep_ref)[index // 2, i] = piece


def weights(place, half, lefts, rights, w):
    depth = w.shape[0]
    chans = rights[0].shape[1]
    size = place.shape[0]
    piece = shape((size // 2, len(lefts), depth // size, chans), bf16)
    outs = [piece, piece, shape((8, depth), f32)]
    return pl.pallas_call(
        functools.partial(weights_kernel, len(lefts), half),
        grid_spec=pltpu.PrefetchScalarGridSpec(
            num_scalar_prefetch=1,
            grid=(1,),
            in_specs=[full(a) for a in (*lefts, *rights, w)],
            out_specs=[full(a) for a in outs],
            scratch_shapes=[pltpu.VMEM((depth, chans), f32)],
        ),
        out_shape=outs,
        compiler_params=params(),
        cost_estimate=cost(3 * len(lefts)),
        name="weights",
    )(place, *lefts, *rights, w)


def last_kernel(tokens, grad, normed_grad, gain, out_ref):
    values = tokens[...].astype(f32)
    inverse = lax.rsqrt(jnp.mean(values * values, axis=-1, keepdims=True) + epsilon)
    hat = values * inverse
    scaled = normed_grad[...].astype(f32) * gain[...]
    out_ref[...] = grad[...].astype(f32) + inverse * (
        scaled - hat * jnp.mean(scaled * hat, axis=-1, keepdims=True)
    )


def last(tokens, grad, normed_grad, gain):
    total, depth = tokens.shape
    rows = min(128, total)
    row = pl.BlockSpec((rows, depth), lambda i: (i, 0))
    return pl.pallas_call(
        last_kernel,
        grid=(total // rows,),
        in_specs=[row, row, row, full(gain)],
        out_specs=row,
        out_shape=shape((total, depth), f32),
        compiler_params=params(),
        cost_estimate=cost(2),
        name="last",
    )(tokens, grad, normed_grad, gain)


def exchange(values, axis, size, bits):
    return lax.ppermute(values, axis, [(i, i ^ bits) for i in range(size)])


def even_pieces(values, axis, size):
    return [values] + [exchange(values, axis, size, m) for m in range(2, size, 2)]


def all_pieces(even, axis, size):
    odd = [exchange(piece, axis, size, 1) for piece in even]
    return [piece for pair in zip(even, odd) for piece in pair]


def pair_sum(keep, send, axis, size):
    return keep + exchange(send, axis, size, 1)


def chip_terms(summed, axis, size):
    return [summed[0]] + [exchange(summed[m], axis, size, 2 * m) for m in range(1, size // 2)]


def total(terms):
    return sum(term.astype(f32) for term in terms)


def sum_all(values, send, axis, size, beside):
    bits = 1
    while bits < size:
        got = exchange(send, axis, size, 2 * bits - 1)
        if bits == 1:
            got, beside = lax.optimization_barrier((got, beside))
        bits *= 2
        if bits < size:
            values = values + got.astype(f32)
            send = values.astype(bf16)
    return values, got, beside


def shards(
    fsdp, tp, tokens, lengths, norm_gain, in_weight, conv_weight, conv_bias, x_weight, dt_weight,
    dt_bias, a_log, d_skip, out_weight, cotangent,
):
    fs_me = lax.axis_index("fsdp")
    place = (fs_me ^ jnp.arange(fsdp)).astype(jnp.int32)
    depth = tokens.shape[2]
    part = conv_weight.shape[1]
    chans = part * fsdp
    lay = Rows(x_weight.shape[1], a_log.shape[0], conv_weight.shape[0])
    maps, width, taps, rank, first = lay.maps, lay.width, lay.taps, lay.rank, lay.first

    cut = tokens.shape[1] * 3 // 4
    whole = lax.all_gather(tokens[0, :cut], "tp", axis=0, tiled=True)
    order = ((lax.axis_index("tp") - jnp.arange(tp)) % tp).astype(jnp.int32)
    direct = [tokens[0, cut:]] + [
        lax.ppermute(tokens[0, cut:], "tp", [(i, (i + k) % tp) for i in range(tp)])
        for k in range(1, tp)
    ]
    even = even_pieces(in_weight.reshape(in_weight.shape[0], 2 * chans), "fsdp", fsdp)
    even, direct, x_weight, a_log, conv_weight, conv_bias, dt_bias, d_skip, dt_weight, gain_part, out_weight = (
        lax.optimization_barrier(
            (
                even, direct, x_weight, a_log, conv_weight, conv_bias, dt_bias, d_skip, dt_weight,
                norm_gain, out_weight,
            )
        )
    )
    pieces = all_pieces(even_pieces(out_weight, "fsdp", fsdp), "fsdp", fsdp)
    ordered = jnp.stack(pieces)[place]
    out_w = ordered.transpose(1, 0, 2).reshape(chans, depth)
    out_w_t = ordered.transpose(0, 2, 1).reshape(depth, chans)
    packed = jnp.concatenate(
        [
            x_weight.T,
            a_log,
            conv_weight,
            conv_bias[None],
            dt_bias[None],
            d_skip[None],
            jnp.zeros((lay.count - first - taps - 3, part), bf16),
            dt_weight.reshape(-1, part),
            gain_part.reshape(-1, part),
        ],
        0,
    )
    gathered = lax.all_gather(packed, "fsdp", axis=0)
    w_pieces = all_pieces(even, "fsdp", fsdp)
    gathered, w_pieces = lax.optimization_barrier((gathered, w_pieces))
    small = gathered[:, : lay.count].transpose(1, 0, 2).reshape(lay.count, chans)
    dt_rows = dt_weight.size // part
    dt_w = gathered[:, lay.count : lay.count + dt_rows].reshape(rank, chans)
    gain = gathered[:, lay.count + dt_rows :].reshape(1, depth).astype(f32)

    normed, w, conv_in, gate, conv_sum, low, map_part, map_send = front(
        lay, order, place, whole, direct, gain, small, w_pieces
    )
    own, got, (held, out_w, out_w_t) = sum_all(
        map_part, map_send, "tp", tp, (cotangent[0], out_w, out_w_t)
    )
    grad_whole = lax.all_gather(held, "tp", axis=0, tiled=True)
    mixed, before, step, h, sent = forward(
        lay, lengths, own, got, low, gate, dt_w, small, out_w
    )
    block_sum = lax.psum_scatter(sent, "tp", scatter_dimension=0, tiled=True)

    map_part, map_send, conv_grad, gate_grad, rate_grad, dt_w_grad, bias_grad = backward(
        lay, lengths, own, got, low, gate, before, step, grad_whole, h, dt_w, small, out_w_t
    )
    *out_one, _ = weights(place, 0, (grad_whole,), (mixed,), w)
    own_grad, got_grad, (held, out_one) = sum_all(
        map_part, map_send, "tp", tp, (gate_grad, out_one)
    )
    *gate_one, gain_two = weights(place, 1, (normed,), (held,), w)
    out_pairs = pair_sum(*out_one, "fsdp", fsdp)
    own_grad, got_grad, gate_one, out_pairs = lax.optimization_barrier(
        (own_grad, got_grad, gate_one, out_pairs)
    )
    normed_part, input_grad, x_w_grad, taps_grad = back(
        lay, own_grad, got_grad, small, conv_grad, conv_sum, conv_in, low, gate_grad, w
    )
    normed_grad = lax.psum_scatter(normed_part, "tp", scatter_dimension=0, tiled=True)
    *one, gain_one = weights(place, 0, (normed,), (input_grad,), w)
    out_terms = chip_terms(out_pairs, "fsdp", fsdp)
    gate_terms = chip_terms(pair_sum(*gate_one, "fsdp", fsdp), "fsdp", fsdp)
    x_w_grad, taps_grad, out_terms, gate_terms = lax.optimization_barrier(
        (x_w_grad, taps_grad, out_terms, gate_terms)
    )
    conv_terms = chip_terms(pair_sum(*one, "fsdp", fsdp), "fsdp", fsdp)
    gain_grad = gain_one[:1] + gain_two[:1]
    bits = 1
    while bits < tp:
        gain_grad = gain_grad + exchange(gain_grad, "tp", tp, 2 * bits - 1)
        bits *= 2
    rows = jnp.concatenate(
        [x_w_grad, rate_grad * LN2, taps_grad[: taps + 1], bias_grad[:2]], 0
    ).astype(bf16)
    top = rows.shape[0]
    packed = jnp.concatenate(
        [
            rows.reshape(top, fsdp, part).transpose(1, 0, 2),
            dt_w_grad.astype(bf16).reshape(fsdp, -1, part),
            gain_grad.astype(bf16).reshape(fsdp, -1, part),
        ],
        1,
    )[place]
    pairs = pair_sum(packed[0::2], packed[1::2], "fsdp", fsdp)
    small_terms = chip_terms(pairs, "fsdp", fsdp)
    out_terms, gate_terms, conv_terms, small_terms, block_sum = lax.optimization_barrier(
        (out_terms, gate_terms, conv_terms, small_terms, block_sum)
    )
    small_grad = total(small_terms)
    out_weight_grad = total(out_terms)[0].T
    in_weight_grad = jnp.stack([total(conv_terms)[0], total(gate_terms)[0]], 1)
    block_out = (tokens.astype(f32) + block_sum[None].astype(f32)).astype(bf16)
    gain_out = small_grad[top + dt_rows :].reshape(-1) / norm_gain.astype(f32)

    input_grads = last(tokens[0], cotangent[0], normed_grad, gain)[None]
    return (
        block_out,
        input_grads,
        gain_out,
        in_weight_grad,
        small_grad[first : first + taps],
        small_grad[first + taps],
        small_grad[:maps].T,
        small_grad[top : top + dt_rows].reshape(-1, chans),
        small_grad[first + taps + 1],
        small_grad[maps:first],
        small_grad[first + taps + 2],
        out_weight_grad,
    )


def solution(mesh):
    sizes = dict(mesh.shape)
    return jax.shard_map(
        functools.partial(shards, sizes["fsdp"], sizes["tp"]),
        mesh=mesh,
        in_specs=(
            P("fsdp", "tp", None),
            P("fsdp"),
            P("fsdp"),
            P("fsdp", None, "tp"),
            P(None, ("tp", "fsdp")),
            P(("tp", "fsdp")),
            P(("tp", "fsdp"), None),
            P("fsdp", "tp"),
            P(("tp", "fsdp")),
            P(None, ("tp", "fsdp")),
            P(("tp", "fsdp")),
            P("tp", "fsdp"),
            P("fsdp", "tp", None),
        ),
        out_specs=(
            P("fsdp", "tp", None),
            P("fsdp", "tp", None),
            P("fsdp"),
            P("fsdp", None, "tp"),
            P(None, ("tp", "fsdp")),
            P(("tp", "fsdp")),
            P(("tp", "fsdp"), None),
            P("fsdp", "tp"),
            P(("tp", "fsdp")),
            P(None, ("tp", "fsdp")),
            P(("tp", "fsdp")),
            P("tp", "fsdp"),
        ),
        check_vma=False,
    )
```
